32 devices in a mesh: dp: 1 (over z), ep: 32 (over y, x, core).
Axes of the slice: x: 4, y: 4, z: 1, core: 2. Of those that a mesh axis runs over, the one named last changes fastest.
The devices are a block of a 4x4x8 slice.
Arguments:
- grad_y: bfloat16 [8192, 1024], P(('dp', 'ep'))
- gate_vals: float32 [8192, 8], P(('dp', 'ep'))
- topk_idx: int32 [8192, 8], P(('dp', 'ep'))
- slot_ids: int32 [8192, 8], P(('dp', 'ep'))
- pair_counts: int32 [32, 32], P(('dp', 'ep'))
- y_routed: bfloat16 [8192, 8, 1024], P(('dp', 'ep'))
- x_disp: bfloat16 [32, 4096, 1024], P(('dp', 'ep'))
- h_gate: bfloat16 [32, 4096, 512], P(('dp', 'ep'))
- h_up: bfloat16 [32, 4096, 512], P(('dp', 'ep'))
- w_gate: bfloat16 [32, 1024, 512], P('ep')
- w_up: bfloat16 [32, 1024, 512], P('ep')
- w_down: bfloat16 [32, 512, 1024], P('ep')
Outputs:
- output 1: bfloat16 [8192, 1024], P(('dp', 'ep'))
- output 2: float32 [8192, 8], P(('dp', 'ep'))
- output 3: float32 [32, 1024, 512], P(('dp', 'ep'))
- output 4: float32 [32, 1024, 512], P(('dp', 'ep'))
- output 5: float32 [32, 512, 1024], P(('dp', 'ep'))
All inputs are finite; a program needn't handle non-finite values.
Results may differ from the reference program's by a relative error of at most 0.0149524.
Values are sent between devices in bfloat16 or wider.
A program may use at most 768 MiB of HBM per device.

```python
import jax
import jax.numpy as jnp
from jax import lax

GROUP_DEV = 32
TOKENS_DEV = 256
EXPERTS = 32
TOP_K = 8
MODEL_DIM = 1024
FFN_DIM = 512
CAPACITY = 128
N_TOKENS = GROUP_DEV * TOKENS_DEV
EXPERT_ROWS = GROUP_DEV * CAPACITY


def setup_inputs(seed: int = 0, part: int = 0) -> dict:
    base_key = jax.random.fold_in(jax.random.key(seed), part)
    key_list = jax.random.split(base_key, 8)
    weight_keys = jax.random.split(jax.random.key(seed + 1), 3)
    key_noise, key_bias, key_hot = jax.random.split(key_list[0], 3)
    expert_iota = jnp.arange(EXPERTS, dtype=jnp.int32)
    token_iota = jnp.arange(TOKENS_DEV, dtype=jnp.int32)
    noise_int = jax.random.randint(key_noise, (GROUP_DEV, TOKENS_DEV, EXPERTS), 0, 4 * EXPERTS)
    bias_base = jax.random.randint(key_bias, (EXPERTS,), 0, 2 * EXPERTS)
    bias_int = (bias_base * bias_base) // (4 * EXPERTS)
    hot_expert = jax.random.randint(key_hot, (GROUP_DEV,), 0, EXPERTS)
    hot_bonus = jnp.where((token_iota[None, :, None] < CAPACITY) & (expert_iota[None, None, :] == hot_expert[:, None, None]), 8 * EXPERTS, 0)
    scores = (noise_int + bias_int[None, None, :] + hot_bonus) * EXPERTS + expert_iota[None, None, :]
    expert_ids = lax.top_k(scores, TOP_K)[1].astype(jnp.int32)

    def rank_one(ids_dev):
        flat_ids = ids_dev.reshape(-1)
        onehot = (flat_ids[:, None] == expert_iota[None, :]).astype(jnp.int32)
        before = jnp.cumsum(onehot, axis=0) - onehot
        rank_pos = jnp.sum(before * onehot, axis=1)
        return rank_pos.reshape(TOKENS_DEV, TOP_K), jnp.sum(onehot, axis=0)

    rank_pos, n_total = lax.map(rank_one, expert_ids)
    slot_dev = jnp.where(rank_pos < CAPACITY, rank_pos, -1).astype(jnp.int32)
    pair_counts = jnp.minimum(n_total, CAPACITY).astype(jnp.int32)
    is_kept = slot_dev >= 0
    slot_safe = jnp.where(is_kept, slot_dev, CAPACITY)
    slot_clip = jnp.where(is_kept, slot_dev, 0)
    src_dev = jnp.broadcast_to(jnp.arange(GROUP_DEV, dtype=jnp.int32)[:, None, None], expert_ids.shape)

    w_gate = (jax.random.normal(weight_keys[0], (EXPERTS, MODEL_DIM, FFN_DIM), jnp.float32) * MODEL_DIM ** -0.5).astype(jnp.bfloat16)
    w_up = (jax.random.normal(weight_keys[1], (EXPERTS, MODEL_DIM, FFN_DIM), jnp.float32) * MODEL_DIM ** -0.5).astype(jnp.bfloat16)
    w_down = (jax.random.normal(weight_keys[2], (EXPERTS, FFN_DIM, MODEL_DIM), jnp.float32) * FFN_DIM ** -0.5).astype(jnp.bfloat16)
    x_tok = jax.random.normal(key_list[1], (GROUP_DEV, TOKENS_DEV, MODEL_DIM), jnp.float32).astype(jnp.bfloat16)
    stale_rows = jax.random.normal(key_list[2], (EXPERTS, GROUP_DEV, CAPACITY, MODEL_DIM), jnp.float32).astype(jnp.bfloat16)
    x_vals = jnp.broadcast_to(x_tok[:, :, None, :], (GROUP_DEV, TOKENS_DEV, TOP_K, MODEL_DIM))
    x_disp = stale_rows.at[expert_ids, src_dev, slot_safe].set(x_vals, mode="drop").reshape(EXPERTS, EXPERT_ROWS, MODEL_DIM)

    def forward_one(operands):
        x_rows, w_gate_e, w_up_e, w_down_e = operands
        h_g = jnp.dot(x_rows, w_gate_e, preferred_element_type=jnp.float32).astype(jnp.bfloat16)
        h_u = jnp.dot(x_rows, w_up_e, preferred_element_type=jnp.float32).astype(jnp.bfloat16)
        gate_f = h_g.astype(jnp.float32)
        hidden_act = (gate_f * jax.nn.sigmoid(gate_f) * h_u.astype(jnp.float32)).astype(jnp.bfloat16)
        y_rows = jnp.dot(hidden_act, w_down_e, preferred_element_type=jnp.float32).astype(jnp.bfloat16)
        return h_g, h_u, y_rows

    h_gate, h_up, y_exp = lax.map(forward_one, (x_disp, w_gate, w_up, w_down))
    y_pick = y_exp.reshape(EXPERTS, GROUP_DEV, CAPACITY, MODEL_DIM)[expert_ids, src_dev, slot_clip]
    y_routed = jnp.where(is_kept[..., None], y_pick, jnp.zeros((), jnp.bfloat16)).reshape(N_TOKENS, TOP_K, MODEL_DIM)
    grad_y = jax.random.normal(key_list[3], (N_TOKENS, MODEL_DIM), jnp.float32).astype(jnp.bfloat16)
    gate_vals = jax.random.uniform(key_list[4], (N_TOKENS, TOP_K), jnp.float32, 0.25, 1.0)
    return {"grad_y": grad_y, "gate_vals": gate_vals, "topk_idx": expert_ids.reshape(N_TOKENS, TOP_K), "slot_ids": slot_dev.reshape(N_TOKENS, TOP_K), "pair_counts": pair_counts, "y_routed": y_routed, "x_disp": x_disp, "h_gate": h_gate, "h_up": h_up, "w_gate": w_gate, "w_up": w_up, "w_down": w_down}


def reference(grad_y, gate_vals, topk_idx, slot_ids, pair_counts, y_routed, x_disp, h_gate, h_up, w_gate, w_up, w_down):
    grad_gate = jnp.einsum("td,tkd->tk", grad_y.astype(jnp.float32), y_routed.astype(jnp.float32))
    is_kept = slot_ids >= 0
    src_dev = jnp.broadcast_to((jnp.arange(N_TOKENS, dtype=jnp.int32) // TOKENS_DEV)[:, None], topk_idx.shape)
    slot_safe = jnp.where(is_kept, slot_ids, CAPACITY)
    slot_clip = jnp.where(is_kept, slot_ids, 0)
    gated_rows = (gate_vals[:, :, None] * grad_y.astype(jnp.float32)[:, None, :]).astype(jnp.bfloat16)
    disp_rows = jnp.zeros((EXPERTS, GROUP_DEV, CAPACITY, MODEL_DIM), jnp.bfloat16).at[topk_idx, src_dev, slot_safe].set(gated_rows, mode="drop")
    keep_row = jnp.arange(CAPACITY)[None, None, :] < jnp.transpose(pair_counts)[:, :, None]
    disp_rows = jnp.where(keep_row[..., None], disp_rows, jnp.zeros((), jnp.bfloat16)).reshape(EXPERTS, EXPERT_ROWS, MODEL_DIM)

    def expert_one(operands):
        grad_rows, x_rows, hg_rows, hu_rows, w_gate_e, w_up_e, w_down_e = operands
        grad_hidden = jnp.dot(grad_rows, w_down_e.T, preferred_element_type=jnp.float32).astype(jnp.bfloat16)
        gate_f = hg_rows.astype(jnp.float32)
        up_f = hu_rows.astype(jnp.float32)
        gate_sig = jax.nn.sigmoid(gate_f)
        gate_act = gate_f * gate_sig
        hidden_act = (gate_act * up_f).astype(jnp.bfloat16)
        grad_h = grad_hidden.astype(jnp.float32)
        grad_hgate = (grad_h * up_f * gate_sig * (1.0 + gate_f * (1.0 - gate_sig))).astype(jnp.bfloat16)
        grad_hup = (grad_h * gate_act).astype(jnp.bfloat16)
        grad_wdown = jnp.dot(hidden_act.T, grad_rows, preferred_element_type=jnp.float32)
        grad_wgate = jnp.dot(x_rows.T, grad_hgate, preferred_element_type=jnp.float32)
        grad_wup = jnp.dot(x_rows.T, grad_hup, preferred_element_type=jnp.float32)
        grad_disp = (jnp.dot(grad_hgate, w_gate_e.T, preferred_element_type=jnp.float32) + jnp.dot(grad_hup, w_up_e.T, preferred_element_type=jnp.float32)).astype(jnp.bfloat16)
        return grad_disp, grad_wgate, grad_wup, grad_wdown

    grad_disp, grad_w_gate, grad_w_up, grad_w_down = lax.map(expert_one, (disp_rows, x_disp, h_gate, h_up, w_gate, w_up, w_down))
    back_rows = grad_disp.reshape(EXPERTS, GROUP_DEV, CAPACITY, MODEL_DIM)[topk_idx, src_dev, slot_clip]
    grad_x = jnp.sum(jnp.where(is_kept[..., None], back_rows.astype(jnp.float32), 0.0), axis=1).astype(jnp.bfloat16)
    return grad_x, grad_gate, grad_w_gate, grad_w_up, grad_w_down
```

```python
import functools
import math

import jax
import jax.numpy as jnp
from jax import lax
from jax.experimental import pallas as pl
from jax.experimental.pallas import tpu as pltpu
from jax.sharding import PartitionSpec as P

MESH = pl.DeviceIdType.MESH
CORES = 2
BF16, F32 = jnp.bfloat16, jnp.float32

ORDER = ((0, 0), (-1, 0), (1, 0), (0, -1), (0, 1), (2, 0), (0, 2), (-1, -1), (1, 1), (-1, 1), (1, -1), (2, -1), (-1, 2), (2, 1), (1, 2), (2, 2))

NN = (((1,), (0,)), ((), ()))
NT = (((1,), (1,)), ((), ()))
TN = (((0,), (0,)), ((), ()))


def dot(a, b, dims):
    return lax.dot_general(a, b, dims, preferred_element_type=F32)


def lut(k, vals):
    out = vals[0]
    for i, v in enumerate(vals):
        if i:
            out = jnp.where(k == i, v, out)
    return out


def kernel(n_dev, side, gy_ref, tab_ref, own_ref, x_ref, hg_ref, hu_ref, wg_ref, wu_ref, wd_ref,
           gx_ref, gwg_ref, gwu_ref, gwd_ref,
           tokens, tabs, rbuf, ret, wgu, wd, xb, hgb, hub, gacc,
           tok_sem, tab_sem, ret_sem, ag_send, pair_send, tab_send, ret_send, load_sem, w_sem, loc_sem):
    me = lax.axis_index("ep")
    core = me % CORES
    mx = (me // CORES) % side
    my = me // (CORES * side)
    tok_dev, model_dim = gy_ref.shape
    ffn = wg_ref.shape[1]
    cap = rbuf.shape[1]
    half = tok_dev // 2
    n_chip = side * side
    crow = CORES * cap

    def plane(a, b):
        x = (mx + (1 - core) * a + core * b + 2 * side) % side
        y = (my + core * a + (1 - core) * b + 2 * side) % side
        return (y * side + x) * CORES + core

    partner = me + 1 - 2 * core

    barrier = pltpu.get_barrier_semaphore()

    def signal_one(i, carry):
        pl.semaphore_signal(barrier, inc=1, device_id={"ep": (me + 1 + i) % n_dev}, device_id_type=MESH)
        return carry

    lax.fori_loop(0, n_dev - 1, signal_one, 0)

    wcopies = [
        pltpu.make_async_copy(wd_ref, wd, w_sem.at[0]),
        pltpu.make_async_copy(wg_ref, wgu.at[:, pl.ds(0, ffn)], w_sem.at[1]),
        pltpu.make_async_copy(wu_ref, wgu.at[:, pl.ds(ffn, ffn)], w_sem.at[2]),
    ]
    for c in wcopies:
        c.start()
    own_copy = pltpu.make_async_copy(gy_ref, tokens.at[me], tok_sem.at[me, 0])
    own_copy.start()
    tab_copy = pltpu.make_async_copy(tab_ref.at[me], tabs.at[me], tab_sem.at[me])
    tab_copy.start()

    def chip_at(k, sign):
        dx = lut(k, [o[0] for o in ORDER])
        dy = lut(k, [o[1] for o in ORDER])
        x = (mx + sign * dx + 2 * side) % side
        y = (my + sign * dy + 2 * side) % side
        return y * side + x

    def loads(k):
        q = chip_at(k, 1)
        slot = k % 2
        rows = pl.ds(pl.multiple_of(q * crow, crow), crow)
        return [
            pltpu.make_async_copy(x_ref.at[rows], xb.at[slot], load_sem.at[0, slot]),
            pltpu.make_async_copy(hg_ref.at[rows], hgb.at[slot], load_sem.at[1, slot]),
            pltpu.make_async_copy(hu_ref.at[rows], hub.at[slot], load_sem.at[2, slot]),
        ]

    for c in loads(0):
        c.start()
    gwg_ref[...] = jnp.zeros_like(gwg_ref)
    gwu_ref[...] = jnp.zeros_like(gwu_ref)
    gwd_ref[...] = jnp.zeros_like(gwd_ref)
    gacc[...] = jnp.zeros_like(gacc)
    pl.semaphore_wait(barrier, n_dev - 1)

    def tab_msg(i):
        to = (me + 1 + i) % n_dev
        return pltpu.make_async_remote_copy(src_ref=tab_ref.at[to], dst_ref=tabs.at[me], send_sem=tab_send.at[i], recv_sem=tab_sem.at[me], device_id={"ep": to}, device_id_type=MESH)

    def tab_start(i, carry):
        tab_msg(i).start()
        return carry

    lax.fori_loop(0, n_dev - 1, tab_start, 0)

    sends, pairs = [], []

    def block(src, part):
        if part == "full":
            return tokens.at[src]
        return tokens.at[src, pl.ds(part * half, half)]

    def forward_msg(n, i, j, part, a, b):
        src = plane(i, j)
        ref = gy_ref if i == 0 and j == 0 else block(src, part)
        return pltpu.make_async_remote_copy(src_ref=ref, dst_ref=block(src, part), send_sem=ag_send.at[n], recv_sem=tok_sem.at[src, 1 if part == 1 else 0], device_id={"ep": plane(a, b)}, device_id_type=MESH)

    def forward(*what):
        what = (len(sends), *what)
        sends.append(what)
        forward_msg(*what).start()

    def pair_msg(n, i, j):
        src = plane(i, j)
        ref = gy_ref if i == 0 and j == 0 else tokens.at[src]
        return pltpu.make_async_remote_copy(src_ref=ref, dst_ref=tokens.at[src], send_sem=pair_send.at[n], recv_sem=tok_sem.at[src, 0], device_id={"ep": partner}, device_id_type=MESH)

    def to_partner(i, j):
        what = (len(pairs), i, j)
        pairs.append(what)
        pair_msg(*what).start()

    def arrived(src, part):
        ref = block(src, part)
        pltpu.make_async_copy(ref, ref, tok_sem.at[src, 1 if part == 1 else 0]).wait()

    to_partner(0, 0)
    for a, b in ((1, 0), (-1, 0), (0, 1), (0, -1)):
        forward(0, 0, "full", a, b)
    own_copy.wait()

    def event(i, j):
        src = plane(i, j)
        if i == 2 and j == 0 or j == 2:
            arrived(src, 0)
            arrived(src, 1)
        else:
            arrived(src, "full")
        if j == 0:
            if i == -1:
                forward(i, j, 0, 1, 0)
            if i == 1:
                forward(i, j, 1, -1, 0)
            forward(i, j, "full", 0, 1)
            forward(i, j, "full", 0, -1)
        elif j == -1:
            forward(i, j, 0, 0, 1)
        elif j == 1:
            forward(i, j, 1, 0, -1)
        to_partner(i, j)

    events = {
        1: ((-1, 0), (1, 0), (0, -1), (0, 1)),
        3: ((2, 0), (0, 2)),
        5: ((-1, -1), (-1, 1), (1, -1), (1, 1)),
        7: ((2, -1), (2, 1)),
        9: ((-1, 2), (1, 2)),
        10: ((2, 2),),
    }

    def ret_msg(k, cc):
        q = chip_at(k, 1)
        to = q * CORES + cc
        return pltpu.make_async_remote_copy(src_ref=rbuf.at[to], dst_ref=ret.at[me], send_sem=ret_send.at[to], recv_sem=ret_sem.at[me], device_id={"ep": to}, device_id_type=MESH)

    def local_ret():
        return pltpu.make_async_copy(rbuf.at[me], ret.at[me], ret_sem.at[me])

    def send_chunk(k):
        @pl.when(k == 0)
        def _():
            local_ret().start()
            to = partner
            pltpu.make_async_remote_copy(src_ref=rbuf.at[to], dst_ref=ret.at[me], send_sem=ret_send.at[to], recv_sem=ret_sem.at[me], device_id={"ep": to}, device_id_type=MESH).start()

        @pl.when(k > 0)
        def _():
            for cc in range(CORES):
                ret_msg(k, cc).start()

    slot_iota = lax.broadcasted_iota(jnp.int32, (cap, tok_dev), 0).astype(F32)
    for c in wcopies:
        c.wait()

    def chunk(k, carry):
        for at, evs in events.items():
            @pl.when(k == at)
            def _(evs=evs):
                for i, j in evs:
                    event(i, j)

        @pl.when(k > 0)
        def _():
            send_chunk(k - 1)

        slot = k % 2
        for c in loads(k):
            c.wait()

        @pl.when(k + 1 < n_chip)
        def _():
            for c in loads(k + 1):
                c.start()

        q = chip_at(k, 1)
        @pl.when(k > 0)
        def _():
            src = q * CORES + 1 - core
            arrived(src, "full")

        @pl.when(k == 0)
        def _():
            arrived(partner, "full")

        d_parts = []
        for cc in range(CORES):
            home = q * CORES + cc
            pltpu.make_async_copy(tabs.at[home], tabs.at[home], tab_sem.at[home]).wait()
            tab = tabs[home]
            pick = tab[0:1, :] == slot_iota
            gate = jnp.sum(jnp.where(pick, tab[1:2, :], 0.0), axis=1, keepdims=True)
            rows = dot(pick.astype(F32).astype(BF16), tokens[home], NN)
            d_parts.append((gate * rows).astype(BF16))
        d = jnp.concatenate(d_parts, axis=0)
        da = dot(d, wd[...], NT).astype(BF16).astype(F32)
        h1 = hgb[slot].astype(F32)
        h3 = hub[slot].astype(F32)
        g = jax.nn.sigmoid(h1)
        s = h1 * g
        act = (s * h3).astype(BF16)
        dh1 = (da * h3 * g * (1.0 + h1 * (1.0 - g))).astype(BF16)
        dh3 = (da * s).astype(BF16)
        dh = jnp.concatenate([dh1, dh3], axis=1)
        r = dot(dh, wgu[...], NT).astype(BF16)
        for cc in range(CORES):
            rbuf[q * CORES + cc] = r[cc * cap:(cc + 1) * cap]
        x = xb[slot]
        gwg_ref[...] += dot(x, dh1, TN)
        gwu_ref[...] += dot(x, dh3, TN)
        gwd_ref[...] += dot(act, d, TN)
        return carry

    lax.fori_loop(0, n_chip, chunk, 0)
    send_chunk(jnp.int32(n_chip - 1))

    def combine(k, carry):
        q = chip_at(k, -1)
        picks = []
        for cc in range(CORES):
            e = q * CORES + cc
            pltpu.make_async_copy(ret.at[e], ret.at[e], ret_sem.at[e]).wait()
            picks.append((own_ref[e] == slot_iota).astype(F32).astype(BF16))
        pick = jnp.concatenate(picks, axis=0)
        rows = jnp.concatenate([ret[q * CORES + cc] for cc in range(CORES)], axis=0)
        gacc[...] += dot(pick, rows, TN)
        return carry

    lax.fori_loop(0, n_chip, combine, 0)
    gx_ref[...] = gacc[...].astype(gx_ref.dtype)

    for what in sends:
        forward_msg(*what).wait_send()
    for what in pairs:
        pair_msg(*what).wait_send()

    def tab_done(i, carry):
        tab_msg(i).wait_send()
        return carry

    lax.fori_loop(0, n_dev - 1, tab_done, 0)

    def ret_done(i, carry):
        to = (me + 1 + i) % n_dev
        pltpu.make_async_remote_copy(src_ref=rbuf.at[to], dst_ref=ret.at[me], send_sem=ret_send.at[to], recv_sem=ret_sem.at[me], device_id={"ep": to}, device_id_type=MESH).wait_send()
        return carry

    lax.fori_loop(0, n_dev - 1, ret_done, 0)


def routing_tables(gate_vals, topk_idx, slot_ids, pair_counts, n_exp):
    ids = topk_idx.T
    slots = slot_ids.T
    gates = gate_vals.T
    expert = lax.broadcasted_iota(jnp.int32, (n_exp, ids.shape[1]), 0)
    slot_of = jnp.full((n_exp, ids.shape[1]), -1, jnp.int32)
    gate_of = jnp.zeros((n_exp, ids.shape[1]), F32)
    for j in range(ids.shape[0]):
        hit = ids[j][None, :] == expert
        slot_of = jnp.where(hit, slots[j][None, :], slot_of)
        gate_of = jnp.where(hit, gates[j][None, :], gate_of)
    real = slot_of < pair_counts.reshape(n_exp, 1)
    slot_d = jnp.where(real, slot_of, -1)
    return jnp.stack([slot_d.astype(F32), gate_of], axis=1), slot_of.astype(F32)[:, None, :]


def solution(mesh):
    n_dev = mesh.shape["ep"]
    side = math.isqrt(n_dev // CORES)
    rows_spec = P(("dp", "ep"), None)
    cube_spec = P(("dp", "ep"), None, None)
    weight_spec = P("ep", None, None)

    def local_step(grad_y, gate_vals, topk_idx, slot_ids, pair_counts, y_routed, x_disp, h_gate, h_up, w_gate, w_up, w_down):
        assert w_gate.shape[0] == 1
        assert side * side * CORES == n_dev and len(ORDER) == side * side
        cap = x_disp.shape[1] // n_dev
        tok_dev, model_dim = grad_y.shape
        ffn = w_gate.shape[2]
        crow = CORES * cap
        n_chip = side * side
        grad_gate = jnp.einsum("td,tkd->tk", grad_y, y_routed, preferred_element_type=F32)
        tab, own = routing_tables(gate_vals, topk_idx, slot_ids, pair_counts, n_dev)
        vmem = pl.BlockSpec(memory_space=pltpu.VMEM)
        anym = pl.BlockSpec(memory_space=pl.ANY)
        dma = pltpu.SemaphoreType.DMA
        gx, gwg, gwu, gwd = pl.pallas_call(
            functools.partial(kernel, n_dev, side),
            out_shape=(
                jax.ShapeDtypeStruct((tok_dev, model_dim), BF16),
                jax.ShapeDtypeStruct((model_dim, ffn), F32),
                jax.ShapeDtypeStruct((model_dim, ffn), F32),
                jax.ShapeDtypeStruct((ffn, model_dim), F32),
            ),
            in_specs=[vmem, vmem, vmem, anym, anym, anym, anym, anym, anym],
            out_specs=(vmem, vmem, vmem, vmem),
            scratch_shapes=[
                pltpu.VMEM((n_dev, tok_dev, model_dim), BF16),
                pltpu.VMEM((n_dev, 2, tok_dev), F32),
                pltpu.VMEM((n_dev, cap, model_dim), BF16),
                pltpu.VMEM((n_dev, cap, model_dim), BF16),
                pltpu.VMEM((model_dim, 2 * ffn), BF16),
                pltpu.VMEM((ffn, model_dim), BF16),
                pltpu.VMEM((2, crow, model_dim), BF16),
                pltpu.VMEM((2, crow, ffn), BF16),
                pltpu.VMEM((2, crow, ffn), BF16),
                pltpu.VMEM((tok_dev, model_dim), F32),
                dma((n_dev, 2)),
                dma((n_dev,)),
                dma((n_dev,)),
                dma((32,)),
                dma((n_chip,)),
                dma((n_dev,)),
                dma((n_dev,)),
                dma((3, 2)),
                dma((3,)),
                dma((1,)),
            ],
            compiler_params=pltpu.CompilerParams(collective_id=0, has_side_effects=True, vmem_limit_bytes=67043328),
            name="moe_bwd",
        )(grad_y, tab, own, x_disp[0], h_gate[0], h_up[0], w_gate[0], w_up[0], w_down[0])
        return gx, grad_gate, gwg[None], gwu[None], gwd[None]

    return jax.shard_map(local_step, mesh=mesh, in_specs=(rows_spec, rows_spec, rows_spec, rows_spec, rows_spec, cube_spec, cube_spec, cube_spec, cube_spec, weight_spec, weight_spec, weight_spec), out_specs=(rows_spec, rows_spec, cube_spec, cube_spec, cube_spec), check_vma=False)
```

```python
import functools
import math

import jax
import jax.numpy as jnp
from jax import lax
from jax.experimental import pallas as pl
from jax.experimental.pallas import tpu as pltpu
from jax.sharding import PartitionSpec as P

MESH = pl.DeviceIdType.MESH
CORES = 2
BF16, F32 = jnp.bfloat16, jnp.float32

ORDER = ((0, 0), (-1, 0), (1, 0), (0, -1), (0, 1), (2, 0), (0, 2), (-1, -1), (1, 1), (-1, 1), (1, -1), (2, -1), (-1, 2), (2, 1), (1, 2), (2, 2))

EVENTS = {
    1: ((-1, 0), (1, 0), (0, -1), (0, 1)),
    3: ((2, 0), (0, 2)),
    5: ((-1, -1), (-1, 1), (1, -1), (1, 1)),
    7: ((2, -1), (2, 1)),
    9: ((-1, 2), (1, 2)),
    10: ((2, 2),),
}
LAG = 3

NN = (((1,), (0,)), ((), ()))
NT = (((1,), (1,)), ((), ()))
TN = (((0,), (0,)), ((), ()))


def dot(a, b, dims):
    return lax.dot_general(a, b, dims, preferred_element_type=F32)


def lut(k, vals):
    out = vals[0]
    for i, v in enumerate(vals):
        if i:
            out = jnp.where(k == i, v, out)
    return out


def kernel(n_dev, side, gy_ref, ids_ref, slots_ref, gates_ref, pc_ref, y_ref, x_ref, hg_ref, hu_ref, wg_ref, wu_ref, wd_ref,
           gx_ref, gg_ref, gwg_ref, gwu_ref, gwd_ref,
           tokens, stab, tabs, mids, mslots, rbuf, ret, relay, part, hop_in, fin, wgu, wd, xb, hgb, hub,
           tok_sem, tab_sem, meta_sem, ret_sem, relay_sem, hop_sem, fin_sem,
           ag_send, pair_send, tab_send, meta_send, ret_send, relay_send, part_send, load_sem, w_sem):
    me = lax.axis_index("ep")
    core = me % CORES
    mx = (me // CORES) % side
    my = me // (CORES * side)
    my_a = (1 - core) * mx + core * my
    my_b = (1 - core) * my + core * mx
    tok_dev, model_dim = gy_ref.shape
    top_k = ids_ref.shape[0]
    ffn = wg_ref.shape[1]
    cap = rbuf.shape[1]
    half = tok_dev // 2
    n_chip = side * side
    crow = CORES * cap
    partner = me + 1 - 2 * core

    def wrap(v):
        return (v + 2 * side) % side

    def device(x, y, c):
        return (wrap(y) * side + wrap(x)) * CORES + c

    def plane(a, b):
        return device(mx + (1 - core) * a + core * b, my + core * a + (1 - core) * b, core)

    def remote(src, dst, send_sem, recv_sem, to):
        return pltpu.make_async_remote_copy(src_ref=src, dst_ref=dst, send_sem=send_sem, recv_sem=recv_sem, device_id={"ep": to}, device_id_type=MESH)

    def landed(ref, sem):
        pltpu.make_async_copy(ref, ref, sem).wait()

    barrier = pltpu.get_barrier_semaphore()

    def signal_one(i, carry):
        pl.semaphore_signal(barrier, inc=1, device_id={"ep": (me + 1 + i) % n_dev}, device_id_type=MESH)
        return carry

    lax.fori_loop(0, n_dev - 1, signal_one, 0)

    wcopies = [
        pltpu.make_async_copy(wd_ref, wd, w_sem.at[0]),
        pltpu.make_async_copy(wg_ref, wgu.at[:, pl.ds(0, ffn)], w_sem.at[1]),
        pltpu.make_async_copy(wu_ref, wgu.at[:, pl.ds(ffn, ffn)], w_sem.at[2]),
    ]
    for c in wcopies:
        c.start()
    own_copies = [
        pltpu.make_async_copy(gy_ref, tokens.at[me], tok_sem.at[me, 0]),
        pltpu.make_async_copy(ids_ref, mids.at[my_b], meta_sem.at[my_b, 0]),
        pltpu.make_async_copy(slots_ref, mslots.at[my_b], meta_sem.at[my_b, 1]),
    ]
    for c in own_copies:
        c.start()

    def offset(k, axis):
        return lut(k, [o[axis] for o in ORDER])

    def chip_at(k):
        return wrap(my + offset(k, 1)) * side + wrap(mx + offset(k, 0))

    def loads(k):
        q = chip_at(k)
        slot = k % 2
        rows = pl.ds(pl.multiple_of(q * crow, crow), crow)
        return [
            pltpu.make_async_copy(x_ref.at[rows], xb.at[slot], load_sem.at[0, slot]),
            pltpu.make_async_copy(hg_ref.at[rows], hgb.at[slot], load_sem.at[1, slot]),
            pltpu.make_async_copy(hu_ref.at[rows], hub.at[slot], load_sem.at[2, slot]),
        ]

    for c in loads(0):
        c.start()

    ids = ids_ref[...]
    slots = slots_ref[...]
    gates = gates_ref[...]

    def table(e, carry):
        hit = ids == e
        slot = jnp.max(jnp.where(hit, slots, -1), axis=0, keepdims=True)
        slot = jnp.where(slot < pc_ref[0, e], slot, -1)
        gate = jnp.sum(jnp.where(hit, gates, 0.0), axis=0, keepdims=True)
        stab[e] = jnp.concatenate([slot.astype(F32), gate], axis=0)
        return carry

    lax.fori_loop(0, n_dev, table, 0)
    gwg_ref[...] = jnp.zeros_like(gwg_ref)
    gwu_ref[...] = jnp.zeros_like(gwu_ref)
    gwd_ref[...] = jnp.zeros_like(gwd_ref)
    pl.semaphore_wait(barrier, n_dev - 1)

    sends, pairs = [], []

    def block(src, part_no):
        if part_no == "full":
            return tokens.at[src]
        return tokens.at[src, pl.ds(part_no * half, half)]

    def forward_msg(n, i, j, part_no, a, b):
        src = plane(i, j)
        ref = gy_ref if i == 0 and j == 0 else block(src, part_no)
        return remote(ref, block(src, part_no), ag_send.at[n], tok_sem.at[src, 1 if part_no == 1 else 0], plane(a, b))

    def forward(*what):
        what = (len(sends), *what)
        sends.append(what)
        forward_msg(*what).start()

    def pair_msg(n, i, j):
        src = plane(i, j)
        ref = gy_ref if i == 0 and j == 0 else tokens.at[src]
        return remote(ref, tokens.at[src], pair_send.at[n], tok_sem.at[src, 0], partner)

    def to_partner(i, j):
        what = (len(pairs), i, j)
        pairs.append(what)
        pair_msg(*what).start()

    def arrived(src, part_no):
        landed(block(src, part_no), tok_sem.at[src, 1 if part_no == 1 else 0])

    to_partner(0, 0)

    def tab_msg(i):
        to = (me + 1 + i) % n_dev
        return remote(stab.at[to], tabs.at[me], tab_send.at[i], tab_sem.at[me], to)

    def tab_start(i, carry):
        tab_msg(i).start()
        return carry

    lax.fori_loop(0, n_dev - 1, tab_start, 0)
    tab_copy = pltpu.make_async_copy(stab.at[me], tabs.at[me], tab_sem.at[me])
    tab_copy.start()
    for a, b in ((1, 0), (-1, 0), (0, 1), (0, -1)):
        forward(0, 0, "full", a, b)

    def meta_msgs():
        out = []
        for n, j in enumerate((1, -1, 2)):
            out.append(remote(ids_ref, mids.at[my_b], meta_send.at[n, 0], meta_sem.at[my_b, 0], plane(0, j)))
            out.append(remote(slots_ref, mslots.at[my_b], meta_send.at[n, 1], meta_sem.at[my_b, 1], plane(0, j)))
        return out

    for c in meta_msgs():
        c.start()
    own_copies[0].wait()

    def event(i, j):
        src = plane(i, j)
        if i == 2 and j == 0 or j == 2:
            arrived(src, 0)
            arrived(src, 1)
        else:
            arrived(src, "full")
        if j == 0:
            if i == -1:
                forward(i, j, 0, 1, 0)
            if i == 1:
                forward(i, j, 1, -1, 0)
            forward(i, j, "full", 0, 1)
            forward(i, j, "full", 0, -1)
        elif j == -1:
            forward(i, j, 0, 0, 1)
        elif j == 1:
            forward(i, j, 1, 0, -1)
        to_partner(i, j)

    def r_block(k, cc):
        i, j = offset(k, cc), offset(k, 1 - cc)
        a, b = (mx, my) if cc == 0 else (my, mx)
        hb = wrap(b + j)
        home = chip_at(k) * CORES + cc
        step = jnp.where(i == 2, 1 - 2 * core, i)
        to = device(mx + step, my, cc) if cc == 0 else device(mx, my + step, cc)
        slot = (hb * side + a) * CORES + core
        hop = hb * 2 + core
        is_local = jnp.logical_and(i == 0, core == cc)
        return i, home, to, slot, hop, is_local

    def send_chunk(k):
        for cc in range(CORES):
            i, home, to, slot, hop, is_local = r_block(k, cc)

            @pl.when(is_local)
            def _():
                pltpu.make_async_copy(rbuf.at[home], ret.at[slot], ret_sem.at[slot]).start()

            @pl.when(i == 2)
            def _():
                remote(rbuf.at[home], relay.at[hop], ret_send.at[home], relay_sem.at[hop], to).start()

            @pl.when(jnp.logical_and(i != 2, jnp.logical_not(is_local)))
            def _():
                remote(rbuf.at[home], ret.at[slot], ret_send.at[home], ret_sem.at[slot], to).start()

    def relay_msg(j, way):
        hb = wrap(my_b + j)
        slot = (hb * side + wrap(my_a - 1 + 2 * way)) * CORES + way
        hop = hb * 2 + way
        return hop, remote(relay.at[hop], ret.at[slot], relay_send.at[hop], ret_sem.at[slot], plane(1 - 2 * way, 0))

    def hand_on(k):
        i = jnp.where(core == 0, offset(k, 0), offset(k, 1))
        j = jnp.where(core == 0, offset(k, 1), offset(k, 0))

        @pl.when(i == 2)
        def _():
            for way in range(2):
                hop, msg = relay_msg(j, way)
                landed(relay.at[hop], relay_sem.at[hop])
                msg.start()

    slot_iota = lax.broadcasted_iota(jnp.int32, (cap, tok_dev), 0)
    slot_iota_f = slot_iota.astype(F32)
    for c in wcopies:
        c.wait()

    def chunk(k, carry):
        for at, evs in EVENTS.items():
            @pl.when(k == at)
            def _(evs=evs):
                for i, j in evs:
                    event(i, j)

        @pl.when(k > 0)
        def _():
            send_chunk(k - 1)

        @pl.when(k >= LAG)
        def _():
            hand_on(k - LAG)

        slot = k % 2
        for c in loads(k):
            c.wait()

        @pl.when(k + 1 < n_chip)
        def _():
            for c in loads(k + 1):
                c.start()

        q = chip_at(k)
        arrived(q * CORES + 1 - core, "full")

        d_parts = []
        for cc in range(CORES):
            home = q * CORES + cc
            landed(tabs.at[home], tab_sem.at[home])
            tab = tabs[home]
            pick = tab[0:1, :] == slot_iota_f
            gate = jnp.sum(jnp.where(pick, tab[1:2, :], 0.0), axis=1, keepdims=True)
            rows = dot(pick.astype(F32).astype(BF16), tokens[home], NN)
            d_parts.append((gate * rows).astype(BF16))
        d = jnp.concatenate(d_parts, axis=0)
        da = dot(d, wd[...], NT).astype(BF16).astype(F32)
        h1 = hgb[slot].astype(F32)
        h3 = hub[slot].astype(F32)
        g = jax.nn.sigmoid(h1)
        s = h1 * g
        act = (s * h3).astype(BF16)
        dh1 = (da * h3 * g * (1.0 + h1 * (1.0 - g))).astype(BF16)
        dh3 = (da * s).astype(BF16)
        dh = jnp.concatenate([dh1, dh3], axis=1)
        r = dot(dh, wgu[...], NT).astype(BF16)
        for cc in range(CORES):
            rbuf[q * CORES + cc] = r[cc * cap:(cc + 1) * cap]
        x = xb[slot]
        gwg_ref[...] += dot(x, dh1, TN)
        gwu_ref[...] += dot(x, dh3, TN)
        gwd_ref[...] += dot(act, d, TN)
        return carry

    lax.fori_loop(0, n_chip, chunk, 0)
    send_chunk(jnp.int32(n_chip - 1))

    n_run = crow // top_k
    n_step = tok_dev // n_run

    def y_load(m):
        return pltpu.make_async_copy(y_ref.at[pl.ds(pl.multiple_of(m * crow, crow), crow)], xb.at[m % 2], load_sem.at[0, m % 2])

    y_load(0).start()
    lane = lax.broadcasted_iota(jnp.int32, (crow, tok_dev), 1)
    token_of = lax.broadcasted_iota(jnp.int32, (crow, tok_dev), 0) // top_k
    gg_ref[...] = jnp.zeros_like(gg_ref)

    def gate_grad(m, carry):
        y_load(m).wait()

        @pl.when(m + 1 < n_step)
        def _():
            y_load(m + 1).start()

        gy = gy_ref[pl.ds(pl.multiple_of(m * n_run, n_run), n_run), :].astype(F32)
        gy = jnp.broadcast_to(gy[:, None, :], (n_run, top_k, model_dim)).reshape(crow, model_dim)
        col = jnp.sum(xb[m % 2].astype(F32) * gy, axis=1, keepdims=True)
        put = jnp.where(lane == token_of + m * n_run, col, 0.0)
        gg_ref[...] += jnp.sum(put.reshape(n_run, top_k, tok_dev), axis=0)
        return carry

    for k in range(n_chip - LAG, n_chip):
        hand_on(jnp.int32(k))

    lax.fori_loop(0, n_step, gate_grad, 0)

    def add_rows(n, carry):
        j = lut(n, (2, 1, -1, 0))
        hb = wrap(my_b + j)
        landed(mids.at[hb], meta_sem.at[hb, 0])
        landed(mslots.at[hb], meta_sem.at[hb, 1])
        h_ids = mids[hb]
        h_slots = mslots[hb]
        picks = []
        for sa in range(side):
            for ce in range(CORES):
                slot = (hb * side + sa) * CORES + ce
                landed(ret.at[slot], ret_sem.at[slot])
                x = (1 - core) * sa + core * my_b
                y = (1 - core) * my_b + core * sa
                row = jnp.max(jnp.where(h_ids == (y * side + x) * CORES + ce, h_slots, -1), axis=0, keepdims=True)
                picks.append((row == slot_iota).astype(F32).astype(BF16))
        pick = jnp.concatenate(picks, axis=0)
        rows = ret[pl.ds(hb * side * CORES, side * CORES)].reshape(side * CORES * cap, model_dim)
        part[n] = dot(pick, rows, TN)

        @pl.when(n == 1)
        def _():
            for c in hop_msgs():
                c.start()

        return carry

    def hop_msgs():
        return [
            remote(part.at[0, pl.ds(0, half)], hop_in.at[0], part_send.at[0], hop_sem.at[0], plane(0, 1)),
            remote(part.at[0, pl.ds(half, half)], hop_in.at[1], part_send.at[1], hop_sem.at[1], plane(0, -1)),
        ]

    def fin_msgs():
        return [
            remote(part.at[1], fin.at[0], part_send.at[2], fin_sem.at[0], plane(0, 1)),
            remote(part.at[2], fin.at[1], part_send.at[3], fin_sem.at[1], plane(0, -1)),
        ]

    lax.fori_loop(0, 3, add_rows, 0)
    landed(hop_in.at[0], hop_sem.at[0])
    part[1, pl.ds(0, half)] += hop_in[0]
    landed(hop_in.at[1], hop_sem.at[1])
    part[2, pl.ds(half, half)] += hop_in[1]
    for what in sends:
        forward_msg(*what).wait_send()
    for what in pairs:
        pair_msg(*what).wait_send()
    fins = fin_msgs()
    fins[0].start()
    fins[1].start()
    lax.fori_loop(3, 4, add_rows, 0)


    def tab_done(i, carry):
        tab_msg(i).wait_send()
        return carry

    lax.fori_loop(0, n_dev - 1, tab_done, 0)
    for c in meta_msgs() + hop_msgs():
        c.wait_send()

    def ret_done(k, carry):
        for cc in range(CORES):
            i, home, to, slot, hop, is_local = r_block(k, cc)

            @pl.when(jnp.logical_not(is_local))
            def _():
                remote(rbuf.at[home], ret.at[slot], ret_send.at[home], ret_sem.at[slot], to).wait_send()
        return carry

    lax.fori_loop(0, n_chip, ret_done, 0)
    for j in (0, 1, -1, 2):
        for way in range(2):
            relay_msg(j, way)[1].wait_send()
    landed(fin.at[0], fin_sem.at[0])
    landed(fin.at[1], fin_sem.at[1])
    gx_ref[...] = (part[3] + fin[0] + fin[1]).astype(gx_ref.dtype)
    for c in fins:
        c.wait_send()


def solution(mesh):
    n_dev = mesh.shape["ep"]
    side = math.isqrt(n_dev // CORES)
    rows_spec = P(("dp", "ep"), None)
    cube_spec = P(("dp", "ep"), None, None)
    weight_spec = P("ep", None, None)

    def local_step(grad_y, gate_vals, topk_idx, slot_ids, pair_counts, y_routed, x_disp, h_gate, h_up, w_gate, w_up, w_down):
        assert w_gate.shape[0] == 1
        assert side * side * CORES == n_dev and len(ORDER) == side * side
        cap = x_disp.shape[1] // n_dev
        tok_dev, model_dim = grad_y.shape
        ffn = w_gate.shape[2]
        crow = CORES * cap
        n_chip = side * side
        top_k = topk_idx.shape[1]
        vmem = pl.BlockSpec(memory_space=pltpu.VMEM)
        smem = pl.BlockSpec(memory_space=pltpu.SMEM)
        anym = pl.BlockSpec(memory_space=pl.ANY)
        dma = pltpu.SemaphoreType.DMA
        gx, gg, gwg, gwu, gwd = pl.pallas_call(
            functools.partial(kernel, n_dev, side),
            out_shape=(
                jax.ShapeDtypeStruct((tok_dev, model_dim), BF16),
                jax.ShapeDtypeStruct((top_k, tok_dev), F32),
                jax.ShapeDtypeStruct((model_dim, ffn), F32),
                jax.ShapeDtypeStruct((model_dim, ffn), F32),
                jax.ShapeDtypeStruct((ffn, model_dim), F32),
            ),
            in_specs=[vmem, vmem, vmem, vmem, smem] + [anym] * 7,
            out_specs=(vmem,) * 5,
            scratch_shapes=[
                pltpu.VMEM((n_dev, tok_dev, model_dim), BF16),
                pltpu.VMEM((n_dev, 2, tok_dev), F32),
                pltpu.VMEM((n_dev, 2, tok_dev), F32),
                pltpu.VMEM((side, top_k, tok_dev), jnp.int32),
                pltpu.VMEM((side, top_k, tok_dev), jnp.int32),
                pltpu.VMEM((n_dev, cap, model_dim), BF16),
                pltpu.VMEM((n_dev, cap, model_dim), BF16),
                pltpu.VMEM((2 * side, cap, model_dim), BF16),
                pltpu.VMEM((4, tok_dev, model_dim), F32),
                pltpu.VMEM((2, tok_dev // 2, model_dim), F32),
                pltpu.VMEM((2, tok_dev, model_dim), F32),
                pltpu.VMEM((model_dim, 2 * ffn), BF16),
                pltpu.VMEM((ffn, model_dim), BF16),
                pltpu.VMEM((2, crow, model_dim), BF16),
                pltpu.VMEM((2, crow, ffn), BF16),
                pltpu.VMEM((2, crow, ffn), BF16),
                dma((n_dev, 2)),
                dma((n_dev,)),
                dma((side, 2)),
                dma((n_dev,)),
                dma((2 * side,)),
                dma((2,)),
                dma((2,)),
                dma((32,)),
                dma((n_chip,)),
                dma((n_dev,)),
                dma((3, 2)),
                dma((n_dev,)),
                dma((2 * side,)),
                dma((4,)),
                dma((3, 2)),
                dma((3,)),
            ],
            compiler_params=pltpu.CompilerParams(collective_id=0, has_side_effects=True, vmem_limit_bytes=67043328),
            name="moe_bwd",
        )(grad_y, topk_idx.T, slot_ids.T, gate_vals.T, pair_counts, y_routed.reshape(tok_dev * top_k, model_dim), x_disp[0], h_gate[0], h_up[0], w_gate[0], w_up[0], w_down[0])
        return gx, gg.T, gwg[None], gwu[None], gwd[None]

    return jax.shard_map(local_step, mesh=mesh, in_specs=(rows_spec, rows_spec, rows_spec, rows_spec, rows_spec, cube_spec, cube_spec, cube_spec, cube_spec, weight_spec, weight_spec, weight_spec), out_specs=(rows_spec, rows_spec, cube_spec, cube_spec, cube_spec), check_vma=False)
```

```python
import functools
import math

import jax
import jax.numpy as jnp
from jax import lax
from jax.experimental import pallas as pl
from jax.experimental.pallas import tpu as pltpu
from jax.sharding import PartitionSpec as P

MESH = pl.DeviceIdType.MESH
CORES = 2
BF16, F32 = jnp.bfloat16, jnp.float32

ORDER = ((0, 0), (-1, 0), (1, 0), (0, -1), (0, 1), (2, 0), (0, 2), (-1, -1), (1, 1), (-1, 1), (1, -1), (2, -1), (-1, 2), (2, 1), (1, 2), (2, 2))

EVENTS = {
    1: ((-1, 0), (1, 0), (0, -1), (0, 1)),
    3: ((2, 0), (0, 2)),
    5: ((-1, -1), (-1, 1), (1, -1), (1, 1)),
    7: ((2, -1), (2, 1)),
    9: ((-1, 2), (1, 2)),
    10: ((2, 2),),
}
LAG = 3

NN = (((1,), (0,)), ((), ()))
NT = (((1,), (1,)), ((), ()))
TN = (((0,), (0,)), ((), ()))


def dot(a, b, dims):
    return lax.dot_general(a, b, dims, preferred_element_type=F32)


def lut(k, vals):
    out = vals[0]
    for i, v in enumerate(vals):
        if i:
            out = jnp.where(k == i, v, out)
    return out


def kernel(n_dev, side, gy_ref, ids_ref, slots_ref, gates_ref, pc_ref, y_ref, x_ref, hg_ref, hu_ref, wg_ref, wu_ref, wd_ref,
           gx_ref, gg_ref, gwg_ref, gwu_ref, gwd_ref,
           tokens, stab, tabs, mids, mslots, rbuf, ret, relay, part, hop_in, fin, wgu, wd, xb, hgb, hub,
           tok_sem, tab_sem, meta_sem, ret_sem, relay_sem, hop_sem, fin_sem,
           ag_send, pair_send, tab_send, meta_send, ret_send, relay_send, part_send, load_sem, w_sem):
    me = lax.axis_index("ep")
    core = me % CORES
    mx = (me // CORES) % side
    my = me // (CORES * side)
    my_a = (1 - core) * mx + core * my
    my_b = (1 - core) * my + core * mx
    tok_dev, model_dim = gy_ref.shape
    top_k = ids_ref.shape[0]
    ffn = wg_ref.shape[1]
    cap = rbuf.shape[1]
    half = tok_dev // 2
    n_chip = side * side
    crow = CORES * cap
    partner = me + 1 - 2 * core

    def wrap(v):
        return (v + 2 * side) % side

    def device(x, y, c):
        return (wrap(y) * side + wrap(x)) * CORES + c

    def plane(a, b):
        return device(mx + (1 - core) * a + core * b, my + core * a + (1 - core) * b, core)

    def remote(src, dst, send_sem, recv_sem, to):
        return pltpu.make_async_remote_copy(src_ref=src, dst_ref=dst, send_sem=send_sem, recv_sem=recv_sem, device_id={"ep": to}, device_id_type=MESH)

    def landed(ref, sem):
        pltpu.make_async_copy(ref, ref, sem).wait()

    barrier = pltpu.get_barrier_semaphore()

    def signal_one(i, carry):
        pl.semaphore_signal(barrier, inc=1, device_id={"ep": (me + 1 + i) % n_dev}, device_id_type=MESH)
        return carry

    lax.fori_loop(0, n_dev - 1, signal_one, 0)

    wcopies = [
        pltpu.make_async_copy(wd_ref, wd, w_sem.at[0]),
        pltpu.make_async_copy(wg_ref, wgu.at[:, pl.ds(0, ffn)], w_sem.at[1]),
        pltpu.make_async_copy(wu_ref, wgu.at[:, pl.ds(ffn, ffn)], w_sem.at[2]),
    ]
    for c in wcopies:
        c.start()
    own_copies = [
        pltpu.make_async_copy(gy_ref, tokens.at[me], tok_sem.at[me, 0]),
        pltpu.make_async_copy(ids_ref, mids.at[my_b], meta_sem.at[my_b, 0]),
        pltpu.make_async_copy(slots_ref, mslots.at[my_b], meta_sem.at[my_b, 1]),
    ]
    for c in own_copies:
        c.start()

    def offset(k, axis):
        return lut(k, [o[axis] for o in ORDER])

    def chip_at(k):
        return wrap(my + offset(k, 1)) * side + wrap(mx + offset(k, 0))

    def loads(k):
        q = chip_at(k)
        slot = k % 2
        rows = pl.ds(pl.multiple_of(q * crow, crow), crow)
        return [
            pltpu.make_async_copy(x_ref.at[rows], xb.at[slot], load_sem.at[0, slot]),
            pltpu.make_async_copy(hg_ref.at[rows], hgb.at[slot], load_sem.at[1, slot]),
            pltpu.make_async_copy(hu_ref.at[rows], hub.at[slot], load_sem.at[2, slot]),
        ]

    for c in loads(0):
        c.start()

    ids = ids_ref[...]
    slots = slots_ref[...]
    gates = gates_ref[...]

    def table(e, carry):
        hit = ids == e
        slot = jnp.max(jnp.where(hit, slots, -1), axis=0, keepdims=True)
        slot = jnp.where(slot < pc_ref[0, e], slot, -1)
        gate = jnp.sum(jnp.where(hit, gates, 0.0), axis=0, keepdims=True)
        stab[e] = jnp.concatenate([slot.astype(F32), gate], axis=0)
        return carry

    lax.fori_loop(0, n_dev, table, 0)
    gwg_ref[...] = jnp.zeros_like(gwg_ref)
    gwu_ref[...] = jnp.zeros_like(gwu_ref)
    gwd_ref[...] = jnp.zeros_like(gwd_ref)
    pl.semaphore_wait(barrier, n_dev - 1)

    sends, pairs = [], []

    def block(src, part_no):
        if part_no == "full":
            return tokens.at[src]
        return tokens.at[src, pl.ds(part_no * half, half)]

    def forward_msg(n, i, j, part_no, a, b):
        src = plane(i, j)
        ref = gy_ref if i == 0 and j == 0 else block(src, part_no)
        return remote(ref, block(src, part_no), ag_send.at[n], tok_sem.at[src, 1 if part_no == 1 else 0], plane(a, b))

    def forward(*what):
        what = (len(sends), *what)
        sends.append(what)
        forward_msg(*what).start()

    def pair_msg(n, i, j):
        src = plane(i, j)
        ref = gy_ref if i == 0 and j == 0 else tokens.at[src]
        return remote(ref, tokens.at[src], pair_send.at[n], tok_sem.at[src, 0], partner)

    def to_partner(i, j):
        what = (len(pairs), i, j)
        pairs.append(what)
        pair_msg(*what).start()

    def arrived(src, part_no):
        landed(block(src, part_no), tok_sem.at[src, 1 if part_no == 1 else 0])

    to_partner(0, 0)

    def tab_msg(i):
        to = (me + 1 + i) % n_dev
        return remote(stab.at[to], tabs.at[me], tab_send.at[i], tab_sem.at[me], to)

    def tab_start(i, carry):
        tab_msg(i).start()
        return carry

    lax.fori_loop(0, n_dev - 1, tab_start, 0)
    tab_copy = pltpu.make_async_copy(stab.at[me], tabs.at[me], tab_sem.at[me])
    tab_copy.start()
    for a, b in ((1, 0), (-1, 0), (0, 1), (0, -1)):
        forward(0, 0, "full", a, b)

    def meta_msgs():
        out = []
        for n, j in enumerate((1, -1, 2)):
            out.append(remote(ids_ref, mids.at[my_b], meta_send.at[n, 0], meta_sem.at[my_b, 0], plane(0, j)))
            out.append(remote(slots_ref, mslots.at[my_b], meta_send.at[n, 1], meta_sem.at[my_b, 1], plane(0, j)))
        return out

    for c in meta_msgs():
        c.start()
    own_copies[0].wait()

    def event(i, j):
        src = plane(i, j)
        if i == 2 and j == 0 or j == 2:
            arrived(src, 0)
            arrived(src, 1)
        else:
            arrived(src, "full")
        if j == 0:
            if i == -1:
                forward(i, j, 0, 1, 0)
            if i == 1:
                forward(i, j, 1, -1, 0)
            forward(i, j, "full", 0, 1)
            forward(i, j, "full", 0, -1)
        elif j == -1:
            forward(i, j, 0, 0, 1)
        elif j == 1:
            forward(i, j, 1, 0, -1)
        to_partner(i, j)

    def r_block(k, cc):
        i, j = offset(k, cc), offset(k, 1 - cc)
        a, b = (mx, my) if cc == 0 else (my, mx)
        hb = wrap(b + j)
        home = chip_at(k) * CORES + cc
        step = jnp.where(i == 2, 1 - 2 * core, i)
        to = device(mx + step, my, cc) if cc == 0 else device(mx, my + step, cc)
        slot = (hb * side + a) * CORES + core
        hop = hb * 2 + core
        is_local = jnp.logical_and(i == 0, core == cc)
        return i, home, to, slot, hop, is_local

    def send_chunk(k):
        for cc in range(CORES):
            i, home, to, slot, hop, is_local = r_block(k, cc)

            @pl.when(is_local)
            def _():
                pltpu.make_async_copy(rbuf.at[home], ret.at[slot], ret_sem.at[slot]).start()

            @pl.when(i == 2)
            def _():
                remote(rbuf.at[home], relay.at[hop], ret_send.at[home], relay_sem.at[hop], to).start()

            @pl.when(jnp.logical_and(i != 2, jnp.logical_not(is_local)))
            def _():
                remote(rbuf.at[home], ret.at[slot], ret_send.at[home], ret_sem.at[slot], to).start()

    def relay_msg(j, way):
        hb = wrap(my_b + j)
        slot = (hb * side + wrap(my_a - 1 + 2 * way)) * CORES + way
        hop = hb * 2 + way
        return hop, remote(relay.at[hop], ret.at[slot], relay_send.at[hop], ret_sem.at[slot], plane(1 - 2 * way, 0))

    def hand_on(k):
        i = jnp.where(core == 0, offset(k, 0), offset(k, 1))
        j = jnp.where(core == 0, offset(k, 1), offset(k, 0))

        @pl.when(i == 2)
        def _():
            for way in range(2):
                hop, msg = relay_msg(j, way)
                landed(relay.at[hop], relay_sem.at[hop])
                msg.start()

    slot_iota = lax.broadcasted_iota(jnp.int32, (cap, tok_dev), 0)
    slot_iota_f = slot_iota.astype(F32)
    for c in wcopies:
        c.wait()

    def chunk(k, carry):
        for at, evs in EVENTS.items():
            @pl.when(k == at)
            def _(evs=evs):
                for i, j in evs:
                    event(i, j)

        @pl.when(k > 0)
        def _():
            send_chunk(k - 1)

        @pl.when(k >= LAG)
        def _():
            hand_on(k - LAG)

        slot = k % 2
        for c in loads(k):
            c.wait()

        @pl.when(k + 1 < n_chip)
        def _():
            for c in loads(k + 1):
                c.start()

        q = chip_at(k)
        arrived(q * CORES + 1 - core, "full")

        d_parts = []
        for cc in range(CORES):
            home = q * CORES + cc
            landed(tabs.at[home], tab_sem.at[home])
            tab = tabs[home]
            pick = tab[0:1, :] == slot_iota_f
            gate = jnp.sum(jnp.where(pick, tab[1:2, :], 0.0), axis=1, keepdims=True)
            rows = dot(pick.astype(F32).astype(BF16), tokens[home], NN)
            d_parts.append((gate * rows).astype(BF16))
        d = jnp.concatenate(d_parts, axis=0)
        da = dot(d, wd[...], NT).astype(BF16).astype(F32)
        h1 = hgb[slot].astype(F32)
        h3 = hub[slot].astype(F32)
        g = jax.nn.sigmoid(h1)
        s = h1 * g
        act = (s * h3).astype(BF16)
        dh1 = (da * h3 * g * (1.0 + h1 * (1.0 - g))).astype(BF16)
        dh3 = (da * s).astype(BF16)
        dh = jnp.concatenate([dh1, dh3], axis=1)
        r = dot(dh, wgu[...], NT).astype(BF16)
        for cc in range(CORES):
            rbuf[q * CORES + cc] = r[cc * cap:(cc + 1) * cap]
        x = xb[slot]
        gwg_ref[...] += dot(x, dh1, TN)
        gwu_ref[...] += dot(x, dh3, TN)
        gwd_ref[...] += dot(act, d, TN)
        return carry

    lax.fori_loop(0, n_chip, chunk, 0)
    send_chunk(jnp.int32(n_chip - 1))

    n_run = crow // top_k
    n_step = tok_dev // n_run

    def y_load(m):
        return pltpu.make_async_copy(y_ref.at[pl.ds(pl.multiple_of(m * crow, crow), crow)], xb.at[m % 2], load_sem.at[0, m % 2])

    y_load(0).start()
    lane = lax.broadcasted_iota(jnp.int32, (crow, tok_dev), 1)
    token_of = lax.broadcasted_iota(jnp.int32, (crow, tok_dev), 0) // top_k
    gg_ref[...] = jnp.zeros_like(gg_ref)

    def gate_grad(m, carry):
        y_load(m).wait()

        @pl.when(m + 1 < n_step)
        def _():
            y_load(m + 1).start()

        gy = gy_ref[pl.ds(pl.multiple_of(m * n_run, n_run), n_run), :].astype(F32)
        gy = jnp.broadcast_to(gy[:, None, :], (n_run, top_k, model_dim)).reshape(crow, model_dim)
        col = jnp.sum(xb[m % 2].astype(F32) * gy, axis=1, keepdims=True)
        put = jnp.where(lane == token_of + m * n_run, col, 0.0)
        gg_ref[...] += jnp.sum(put.reshape(n_run, top_k, tok_dev), axis=0)
        return carry

    for k in range(n_chip - LAG, n_chip):
        hand_on(jnp.int32(k))

    lax.fori_loop(0, n_step, gate_grad, 0)

    def add_rows(n, carry):
        j = lut(n, (2, 1, -1, 0))
        hb = wrap(my_b + j)
        landed(mids.at[hb], meta_sem.at[hb, 0])
        landed(mslots.at[hb], meta_sem.at[hb, 1])
        h_ids = mids[hb]
        h_slots = mslots[hb]
        picks = []
        for sa in range(side):
            for ce in range(CORES):
                slot = (hb * side + sa) * CORES + ce
                landed(ret.at[slot], ret_sem.at[slot])
                x = (1 - core) * sa + core * my_b
                y = (1 - core) * my_b + core * sa
                row = jnp.max(jnp.where(h_ids == (y * side + x) * CORES + ce, h_slots, -1), axis=0, keepdims=True)
                picks.append((row == slot_iota).astype(F32).astype(BF16))
        pick = jnp.concatenate(picks, axis=0)
        rows = ret[pl.ds(hb * side * CORES, side * CORES)].reshape(side * CORES * cap, model_dim)
        part[n] = dot(pick, rows, TN)

        @pl.when(n == 1)
        def _():
            for c in hop_msgs():
                c.start()

        return carry

    def hop_msgs():
        return [
            remote(part.at[0, pl.ds(0, half)], hop_in.at[0], part_send.at[0], hop_sem.at[0], plane(0, 1)),
            remote(part.at[0, pl.ds(half, half)], hop_in.at[1], part_send.at[1], hop_sem.at[1], plane(0, -1)),
        ]

    def fin_msgs():
        return [
            remote(part.at[1], fin.at[0], part_send.at[2], fin_sem.at[0], plane(0, 1)),
            remote(part.at[2], fin.at[1], part_send.at[3], fin_sem.at[1], plane(0, -1)),
        ]

    lax.fori_loop(0, 3, add_rows, 0)
    landed(hop_in.at[0], hop_sem.at[0])
    part[1, pl.ds(0, half)] += hop_in[0]
    landed(hop_in.at[1], hop_sem.at[1])
    part[2, pl.ds(half, half)] += hop_in[1]
    for what in sends:
        forward_msg(*what).wait_send()
    for what in pairs:
        pair_msg(*what).wait_send()
    fins = fin_msgs()
    fins[0].start()
    fins[1].start()
    lax.fori_loop(3, 4, add_rows, 0)


    def tab_done(i, carry):
        tab_msg(i).wait_send()
        return carry

    lax.fori_loop(0, n_dev - 1, tab_done, 0)
    for c in meta_msgs() + hop_msgs():
        c.wait_send()

    def ret_done(k, carry):
        for cc in range(CORES):
            i, home, to, slot, hop, is_local = r_block(k, cc)

            @pl.when(jnp.logical_not(is_local))
            def _():
                remote(rbuf.at[home], ret.at[slot], ret_send.at[home], ret_sem.at[slot], to).wait_send()
        return carry

    lax.fori_loop(0, n_chip, ret_done, 0)
    for j in (0, 1, -1, 2):
        for way in range(2):
            relay_msg(j, way)[1].wait_send()
    landed(fin.at[0], fin_sem.at[0])
    landed(fin.at[1], fin_sem.at[1])
    gx_ref[...] = (part[3] + fin[0] + fin[1]).astype(gx_ref.dtype)
    for c in fins:
        c.wait_send()


def solution(mesh):
    n_dev = mesh.shape["ep"]
    side = math.isqrt(n_dev // CORES)
    rows_spec = P(("dp", "ep"), None)
    cube_spec = P(("dp", "ep"), None, None)
    weight_spec = P("ep", None, None)

    def local_step(grad_y, gate_vals, topk_idx, slot_ids, pair_counts, y_routed, x_disp, h_gate, h_up, w_gate, w_up, w_down):
        assert w_gate.shape[0] == 1
        assert side * side * CORES == n_dev and len(ORDER) == side * side
        cap = x_disp.shape[1] // n_dev
        tok_dev, model_dim = grad_y.shape
        ffn = w_gate.shape[2]
        crow = CORES * cap
        n_chip = side * side
        top_k = topk_idx.shape[1]
        vmem = pl.BlockSpec(memory_space=pltpu.VMEM)
        smem = pl.BlockSpec(memory_space=pltpu.SMEM)
        anym = pl.BlockSpec(memory_space=pl.ANY)
        dma = pltpu.SemaphoreType.DMA
        gx, gg, gwg, gwu, gwd = pl.pallas_call(
            functools.partial(kernel, n_dev, side),
            out_shape=(
                pltpu.VMEM((tok_dev, model_dim), BF16),
                pltpu.VMEM((top_k, tok_dev), F32),
                pltpu.VMEM((model_dim, ffn), F32),
                pltpu.VMEM((model_dim, ffn), F32),
                pltpu.VMEM((ffn, model_dim), F32),
            ),
            in_specs=[vmem, vmem, vmem, vmem, smem] + [anym] * 7,
            out_specs=(vmem,) * 5,
            scratch_shapes=[
                pltpu.VMEM((n_dev, tok_dev, model_dim), BF16),
                pltpu.VMEM((n_dev, 2, tok_dev), F32),
                pltpu.VMEM((n_dev, 2, tok_dev), F32),
                pltpu.VMEM((side, top_k, tok_dev), jnp.int32),
                pltpu.VMEM((side, top_k, tok_dev), jnp.int32),
                pltpu.VMEM((n_dev, cap, model_dim), BF16),
                pltpu.VMEM((n_dev, cap, model_dim), BF16),
                pltpu.VMEM((2 * side, cap, model_dim), BF16),
                pltpu.VMEM((4, tok_dev, model_dim), F32),
                pltpu.VMEM((2, tok_dev // 2, model_dim), F32),
                pltpu.VMEM((2, tok_dev, model_dim), F32),
                pltpu.VMEM((model_dim, 2 * ffn), BF16),
                pltpu.VMEM((ffn, model_dim), BF16),
                pltpu.VMEM((2, crow, model_dim), BF16),
                pltpu.VMEM((2, crow, ffn), BF16),
                pltpu.VMEM((2, crow, ffn), BF16),
                dma((n_dev, 2)),
                dma((n_dev,)),
                dma((side, 2)),
                dma((n_dev,)),
                dma((2 * side,)),
                dma((2,)),
                dma((2,)),
                dma((32,)),
                dma((n_chip,)),
                dma((n_dev,)),
                dma((3, 2)),
                dma((n_dev,)),
                dma((2 * side,)),
                dma((4,)),
                dma((3, 2)),
                dma((3,)),
            ],
            compiler_params=pltpu.CompilerParams(collective_id=0, has_side_effects=True, vmem_limit_bytes=58720256),
            name="moe_bwd",
        )(grad_y, topk_idx.T, slot_ids.T, gate_vals.T, pair_counts, y_routed.reshape(tok_dev * top_k, model_dim), x_disp[0], h_gate[0], h_up[0], w_gate[0], w_up[0], w_down[0])
        return gx, gg.T, gwg[None], gwu[None], gwd[None]

    return jax.shard_map(local_step, mesh=mesh, in_specs=(rows_spec, rows_spec, rows_spec, rows_spec, rows_spec, cube_spec, cube_spec, cube_spec, cube_spec, weight_spec, weight_spec, weight_spec), out_specs=(rows_spec, rows_spec, cube_spec, cube_spec, cube_spec), check_vma=False)
```

```python
import functools
import math

import jax
import jax.numpy as jnp
from jax import lax
from jax.experimental import pallas as pl
from jax.experimental.pallas import tpu as pltpu
from jax.sharding import PartitionSpec as P

MESH = pl.DeviceIdType.MESH
CORES = 2
BF16, F32 = jnp.bfloat16, jnp.float32

ORDER = ((0, 1), (0, 0), (1, 0), (0, -1), (-1, 0), (2, 0), (0, 2), (1, -1), (-1, 1), (-1, -1), (1, 1), (2, 2), (-1, 2), (1, 2), (2, -1), (2, 1))
EVENTS = {
    0: ((0, -1), (1, 0), (0, 1), (-1, 0)),
    2: ((2, 0),),
    3: ((1, -1),),
    5: ((0, 2),),
    6: ((-1, 1),),
    7: ((2, -1), (2, 1), (1, 1)),
    8: ((-1, -1),),
    11: ((2, 2),),
    12: ((-1, 2),),
    13: ((1, 2),),
}
LAG = 6

LINES = (2, -1, 1, 0)
PART = {2: 0, 1: 1, -1: 2, 0: 3}

NN = (((1,), (0,)), ((), ()))
NT = (((1,), (1,)), ((), ()))
TN = (((0,), (0,)), ((), ()))


def dot(a, b, dims):
    return lax.dot_general(a, b, dims, preferred_element_type=F32)


def lut(k, vals):
    out = vals[0]
    for i, v in enumerate(vals):
        if i:
            out = jnp.where(k == i, v, out)
    return out


def kernel(n_dev, side, gy_ref, ids_ref, slots_ref, gates_ref, pc_ref, y_ref, x_ref, hg_ref, hu_ref, wg_ref, wu_ref, wd_ref,
           gx_ref, gg_ref, gwg_ref, gwu_ref, gwd_ref,
           tokens, stab, tabs, mids, mslots, rbuf, ret, relay, part, hop_in, fin, wgu, wd, xb, hgb, hub,
           tok_sem, tab_sem, meta_sem, ret_sem, relay_sem, hop_sem, fin_sem,
           ag_send, pair_send, tab_send, meta_send, ret_send, relay_send, part_send, load_sem, w_sem):
    me = lax.axis_index("ep")
    core = me % CORES
    mx = (me // CORES) % side
    my = me // (CORES * side)
    my_a = (1 - core) * mx + core * my
    my_b = (1 - core) * my + core * mx
    tok_dev, model_dim = gy_ref.shape
    top_k = ids_ref.shape[0]
    ffn = wg_ref.shape[1]
    cap = rbuf.shape[1]
    half = tok_dev // 2
    n_chip = side * side
    crow = CORES * cap
    partner = me + 1 - 2 * core

    def wrap(v):
        return (v + 2 * side) % side

    def device(x, y, c):
        return (wrap(y) * side + wrap(x)) * CORES + c

    def plane(a, b):
        return device(mx + (1 - core) * a + core * b, my + core * a + (1 - core) * b, core)

    def remote(src, dst, send_sem, recv_sem, to):
        return pltpu.make_async_remote_copy(src_ref=src, dst_ref=dst, send_sem=send_sem, recv_sem=recv_sem, device_id={"ep": to}, device_id_type=MESH)

    def landed(ref, sem):
        pltpu.make_async_copy(ref, ref, sem).wait()

    barrier = pltpu.get_barrier_semaphore()

    def signal_one(i, carry):
        pl.semaphore_signal(barrier, inc=1, device_id={"ep": (me + 1 + i) % n_dev}, device_id_type=MESH)
        return carry

    lax.fori_loop(0, n_dev - 1, signal_one, 0)

    wcopies = [
        pltpu.make_async_copy(wd_ref, wd, w_sem.at[0]),
        pltpu.make_async_copy(wg_ref, wgu.at[:, pl.ds(0, ffn)], w_sem.at[1]),
        pltpu.make_async_copy(wu_ref, wgu.at[:, pl.ds(ffn, ffn)], w_sem.at[2]),
    ]
    for c in wcopies:
        c.start()
    own_copies = [
        pltpu.make_async_copy(gy_ref, tokens.at[me], tok_sem.at[me, 0]),
        pltpu.make_async_copy(ids_ref, mids.at[my_b], meta_sem.at[my_b, 0]),
        pltpu.make_async_copy(slots_ref, mslots.at[my_b], meta_sem.at[my_b, 1]),
    ]
    for c in own_copies:
        c.start()

    def offset(k, axis):
        return lut(k, [o[axis] for o in ORDER])

    def chip_at(k):
        return wrap(my + offset(k, 1)) * side + wrap(mx + offset(k, 0))

    def loads(k):
        q = chip_at(k)
        slot = k % 2
        rows = pl.ds(pl.multiple_of(q * crow, crow), crow)
        return [
            pltpu.make_async_copy(x_ref.at[rows], xb.at[slot], load_sem.at[0, slot]),
            pltpu.make_async_copy(hg_ref.at[rows], hgb.at[slot], load_sem.at[1, slot]),
            pltpu.make_async_copy(hu_ref.at[rows], hub.at[slot], load_sem.at[2, slot]),
        ]

    for c in loads(0):
        c.start()

    ids = ids_ref[...]
    slots = slots_ref[...]
    gates = gates_ref[...]

    def table(e, carry):
        hit = ids == e
        slot = jnp.max(jnp.where(hit, slots, -1), axis=0, keepdims=True)
        slot = jnp.where(slot < pc_ref[0, e], slot, -1)
        gate = jnp.sum(jnp.where(hit, gates, 0.0), axis=0, keepdims=True)
        stab[e] = jnp.concatenate([slot.astype(F32), gate], axis=0)
        return carry

    lax.fori_loop(0, n_dev, table, 0)
    gwg_ref[...] = jnp.zeros_like(gwg_ref)
    gwu_ref[...] = jnp.zeros_like(gwu_ref)
    gwd_ref[...] = jnp.zeros_like(gwd_ref)
    pl.semaphore_wait(barrier, n_dev - 1)
    own_copies[0].wait()

    sends, pairs = [], []

    def block(src, h):
        return tokens.at[src, pl.ds(h * half, half)]

    def forward_msg(n, i, j, h, a, b):
        src = plane(i, j)
        return remote(block(src, h), block(src, h), ag_send.at[n], tok_sem.at[src, h], plane(a, b))

    def forward(*what):
        what = (len(sends), *what)
        sends.append(what)
        forward_msg(*what).start()

    def pair_msg(n, i, j):
        src = plane(i, j)
        return remote(tokens.at[src], tokens.at[src], pair_send.at[n], tok_sem.at[src, 0], partner)

    def to_partner(i, j):
        what = (len(pairs), i, j)
        pairs.append(what)
        pair_msg(*what).start()

    def arrived(src, h):
        landed(block(src, h), tok_sem.at[src, h])

    to_partner(0, 0)

    def tab_msg(i):
        to = (me + 1 + i) % n_dev
        return remote(stab.at[to], tabs.at[me], tab_send.at[i], tab_sem.at[me], to)

    def tab_start(i, carry):
        tab_msg(i).start()
        return carry

    lax.fori_loop(0, n_dev - 1, tab_start, 0)
    tab_copy = pltpu.make_async_copy(stab.at[me], tabs.at[me], tab_sem.at[me])
    tab_copy.start()
    for n in range(2):
        for a, b, h in ((1, 0, n), (-1, 0, 1 - n), (0, 1, n), (0, -1, 1 - n)):
            forward(0, 0, h, a, b)

    def meta_msgs():
        out = []
        for n, j in enumerate((1, -1, 2)):
            out.append(remote(ids_ref, mids.at[my_b], meta_send.at[n, 0], meta_sem.at[my_b, 0], plane(0, j)))
            out.append(remote(slots_ref, mslots.at[my_b], meta_send.at[n, 1], meta_sem.at[my_b, 1], plane(0, j)))
        return out

    for c in meta_msgs():
        c.start()

    def event(i, j):
        src = plane(i, j)
        first = 1 if (i == 1 and j == 0) or j == 1 else 0
        for n, h in enumerate((first, 1 - first)):
            arrived(src, h)
            if j == 0:
                if n == 0 and abs(i) == 1:
                    forward(i, j, h, -i, 0)
                forward(i, j, h, 0, 1)
                forward(i, j, h, 0, -1)
            elif n == 0 and abs(j) == 1:
                forward(i, j, h, 0, -j)
        to_partner(i, j)

    def r_block(k, cc):
        i, j = offset(k, cc), offset(k, 1 - cc)
        a, b = (mx, my) if cc == 0 else (my, mx)
        hb = wrap(b + j)
        home = chip_at(k) * CORES + cc
        step = jnp.where(i == 2, 1 - 2 * core, i)
        to = device(mx + step, my, cc) if cc == 0 else device(mx, my + step, cc)
        slot = (hb * side + a) * CORES + core
        hop = hb * 2 + core
        is_local = jnp.logical_and(i == 0, core == cc)
        return i, home, to, slot, hop, is_local

    def send_chunk(k):
        for cc in range(CORES):
            i, home, to, slot, hop, is_local = r_block(k, cc)

            @pl.when(is_local)
            def _():
                pltpu.make_async_copy(rbuf.at[home], ret.at[slot], ret_sem.at[slot]).start()

            @pl.when(i == 2)
            def _():
                remote(rbuf.at[home], relay.at[hop], ret_send.at[home], relay_sem.at[hop], to).start()

            @pl.when(jnp.logical_and(i != 2, jnp.logical_not(is_local)))
            def _():
                remote(rbuf.at[home], ret.at[slot], ret_send.at[home], ret_sem.at[slot], to).start()

    def relay_msg(j, way):
        hb = wrap(my_b + j)
        slot = (hb * side + wrap(my_a - 1 + 2 * way)) * CORES + way
        hop = hb * 2 + way
        return hop, remote(relay.at[hop], ret.at[slot], relay_send.at[hop], ret_sem.at[slot], plane(1 - 2 * way, 0))

    def hand_on(k):
        i = jnp.where(core == 0, offset(k, 0), offset(k, 1))
        j = jnp.where(core == 0, offset(k, 1), offset(k, 0))

        @pl.when(i == 2)
        def _():
            for way in range(2):
                hop, msg = relay_msg(j, way)
                landed(relay.at[hop], relay_sem.at[hop])
                msg.start()

    slot_iota = lax.broadcasted_iota(jnp.int32, (cap, tok_dev), 0)
    slot_iota_f = slot_iota.astype(F32)
    for c in wcopies:
        c.wait()

    def chunk(k, carry):
        for at, evs in EVENTS.items():
            @pl.when(k == at)
            def _(evs=evs):
                for i, j in evs:
                    event(i, j)

        @pl.when(k > 0)
        def _():
            send_chunk(k - 1)

        @pl.when(k >= LAG)
        def _():
            hand_on(k - LAG)

        slot = k % 2
        for c in loads(k):
            c.wait()

        @pl.when(k + 1 < n_chip)
        def _():
            for c in loads(k + 1):
                c.start()

        q = chip_at(k)
        landed(tokens.at[q * CORES + 1 - core], tok_sem.at[q * CORES + 1 - core, 0])

        d_parts = []
        for cc in range(CORES):
            home = q * CORES + cc
            landed(tabs.at[home], tab_sem.at[home])
            tab = tabs[home]
            pick = tab[0:1, :] == slot_iota_f
            gate = jnp.sum(jnp.where(pick, tab[1:2, :], 0.0), axis=1, keepdims=True)
            rows = dot(pick.astype(F32).astype(BF16), tokens[home], NN)
            d_parts.append((gate * rows).astype(BF16))
        d = jnp.concatenate(d_parts, axis=0)
        da = dot(d, wd[...], NT).astype(BF16).astype(F32)
        h1 = hgb[slot].astype(F32)
        h3 = hub[slot].astype(F32)
        g = jax.nn.sigmoid(h1)
        s = h1 * g
        act = (s * h3).astype(BF16)
        dh1 = (da * h3 * g * (1.0 + h1 * (1.0 - g))).astype(BF16)
        dh3 = (da * s).astype(BF16)
        dh = jnp.concatenate([dh1, dh3], axis=1)
        r = dot(dh, wgu[...], NT).astype(BF16)
        for cc in range(CORES):
            rbuf[q * CORES + cc] = r[cc * cap:(cc + 1) * cap]
        x = xb[slot]
        gwg_ref[...] += dot(x, dh1, TN)
        gwu_ref[...] += dot(x, dh3, TN)
        gwd_ref[...] += dot(act, d, TN)
        return carry

    lax.fori_loop(0, n_chip, chunk, 0)
    send_chunk(jnp.int32(n_chip - 1))

    n_run = crow // top_k
    n_step = tok_dev // n_run

    def y_load(m):
        return pltpu.make_async_copy(y_ref.at[pl.ds(pl.multiple_of(m * crow, crow), crow)], xb.at[m % 2], load_sem.at[0, m % 2])

    y_load(0).start()
    lane = lax.broadcasted_iota(jnp.int32, (crow, tok_dev), 1)
    token_of = lax.broadcasted_iota(jnp.int32, (crow, tok_dev), 0) // top_k
    gg_ref[...] = jnp.zeros_like(gg_ref)

    def gate_grad(m, carry):
        y_load(m).wait()

        @pl.when(m + 1 < n_step)
        def _():
            y_load(m + 1).start()

        gy = tokens[me, pl.ds(pl.multiple_of(m * n_run, n_run), n_run), :].astype(F32)
        gy = jnp.broadcast_to(gy[:, None, :], (n_run, top_k, model_dim)).reshape(crow, model_dim)
        col = jnp.sum(xb[m % 2].astype(F32) * gy, axis=1, keepdims=True)
        put = jnp.where(lane == token_of + m * n_run, col, 0.0)
        gg_ref[...] += jnp.sum(put.reshape(n_run, top_k, tok_dev), axis=0)
        return carry

    for k in range(n_chip - LAG, n_chip):
        hand_on(jnp.int32(k))

    lax.fori_loop(0, n_step - 1, gate_grad, 0)

    def add_rows(n, carry):
        j = lut(n, LINES)
        hb = wrap(my_b + j)
        landed(mids.at[hb], meta_sem.at[hb, 0])
        landed(mslots.at[hb], meta_sem.at[hb, 1])
        h_ids = mids[hb]
        h_slots = mslots[hb]
        picks = []
        for sa in range(side):
            for ce in range(CORES):
                slot = (hb * side + sa) * CORES + ce
                landed(ret.at[slot], ret_sem.at[slot])
                x = (1 - core) * sa + core * my_b
                y = (1 - core) * my_b + core * sa
                row = jnp.max(jnp.where(h_ids == (y * side + x) * CORES + ce, h_slots, -1), axis=0, keepdims=True)
                picks.append((row == slot_iota).astype(F32).astype(BF16))
        pick = jnp.concatenate(picks, axis=0)
        rows = ret[pl.ds(hb * side * CORES, side * CORES)].reshape(side * CORES * cap, model_dim)
        part[lut(n, [PART[v] for v in LINES])] = dot(pick, rows, TN)

        @pl.when(n == 0)
        def _():
            gate_grad(n_step - 1, 0)
            for c in hop_msgs():
                c.start()

        return carry

    def hop_msgs():
        return [
            remote(part.at[0, pl.ds(0, half)], hop_in.at[0], part_send.at[0], hop_sem.at[0], plane(0, 1)),
            remote(part.at[0, pl.ds(half, half)], hop_in.at[1], part_send.at[1], hop_sem.at[1], plane(0, -1)),
        ]

    def fin_msgs():
        return [
            remote(part.at[1 + n, pl.ds(h * half, half)], fin.at[n, pl.ds(h * half, half)], part_send.at[2 + 2 * n + h], fin_sem.at[n, h], plane(0, 1 - 2 * n))
            for n in range(2)
            for h in range(2)
        ]

    fins = fin_msgs()
    lax.fori_loop(0, len(LINES), add_rows, 0)
    fins[1].start()
    fins[2].start()
    landed(hop_in.at[0], hop_sem.at[0])
    part[1, pl.ds(0, half)] += hop_in[0]
    landed(hop_in.at[1], hop_sem.at[1])
    part[2, pl.ds(half, half)] += hop_in[1]
    for what in sends:
        forward_msg(*what).wait_send()
    for what in pairs:
        pair_msg(*what).wait_send()
    fins[0].start()
    fins[3].start()


    def tab_done(i, carry):
        tab_msg(i).wait_send()
        return carry

    lax.fori_loop(0, n_dev - 1, tab_done, 0)
    for c in meta_msgs() + hop_msgs():
        c.wait_send()

    def ret_done(k, carry):
        for cc in range(CORES):
            i, home, to, slot, hop, is_local = r_block(k, cc)

            @pl.when(jnp.logical_not(is_local))
            def _():
                remote(rbuf.at[home], ret.at[slot], ret_send.at[home], ret_sem.at[slot], to).wait_send()
        return carry

    lax.fori_loop(0, n_chip, ret_done, 0)
    for j in (0, 1, -1, 2):
        for way in range(2):
            relay_msg(j, way)[1].wait_send()
    for n in range(2):
        for h in range(2):
            landed(fin.at[n, pl.ds(h * half, half)], fin_sem.at[n, h])
    gx_ref[...] = (part[3] + fin[0] + fin[1]).astype(gx_ref.dtype)
    for c in fins:
        c.wait_send()


def write_out(*refs):
    n = len(refs) // 2
    sems = refs[-1]
    copies = [pltpu.make_async_copy(refs[i], refs[n + i], sems.at[i]) for i in range(n)]
    for c in copies:
        c.start()
    for c in copies:
        c.wait()


def solution(mesh):
    n_dev = mesh.shape["ep"]
    side = math.isqrt(n_dev // CORES)
    rows_spec = P(("dp", "ep"), None)
    cube_spec = P(("dp", "ep"), None, None)
    weight_spec = P("ep", None, None)

    def local_step(grad_y, gate_vals, topk_idx, slot_ids, pair_counts, y_routed, x_disp, h_gate, h_up, w_gate, w_up, w_down):
        assert w_gate.shape[0] == 1
        assert side * side * CORES == n_dev and len(ORDER) == side * side
        cap = x_disp.shape[1] // n_dev
        tok_dev, model_dim = grad_y.shape
        ffn = w_gate.shape[2]
        crow = CORES * cap
        n_chip = side * side
        top_k = topk_idx.shape[1]
        vmem = pl.BlockSpec(memory_space=pltpu.VMEM)
        smem = pl.BlockSpec(memory_space=pltpu.SMEM)
        anym = pl.BlockSpec(memory_space=pl.ANY)
        dma = pltpu.SemaphoreType.DMA
        results = pl.pallas_call(
            functools.partial(kernel, n_dev, side),
            out_shape=(
                pltpu.VMEM((tok_dev, model_dim), BF16),
                pltpu.VMEM((top_k, tok_dev), F32),
                pltpu.VMEM((model_dim, ffn), F32),
                pltpu.VMEM((model_dim, ffn), F32),
                pltpu.VMEM((ffn, model_dim), F32),
            ),
            in_specs=[anym, vmem, vmem, vmem, smem] + [anym] * 7,
            out_specs=(vmem,) * 5,
            scratch_shapes=[
                pltpu.VMEM((n_dev, tok_dev, model_dim), BF16),
                pltpu.VMEM((n_dev, 2, tok_dev), F32),
                pltpu.VMEM((n_dev, 2, tok_dev), F32),
                pltpu.VMEM((side, top_k, tok_dev), jnp.int32),
                pltpu.VMEM((side, top_k, tok_dev), jnp.int32),
                pltpu.VMEM((n_dev, cap, model_dim), BF16),
                pltpu.VMEM((n_dev, cap, model_dim), BF16),
                pltpu.VMEM((2 * side, cap, model_dim), BF16),
                pltpu.VMEM((4, tok_dev, model_dim), F32),
                pltpu.VMEM((2, tok_dev // 2, model_dim), F32),
                pltpu.VMEM((2, tok_dev, model_dim), F32),
                pltpu.VMEM((model_dim, 2 * ffn), BF16),
                pltpu.VMEM((ffn, model_dim), BF16),
                pltpu.VMEM((2, crow, model_dim), BF16),
                pltpu.VMEM((2, crow, ffn), BF16),
                pltpu.VMEM((2, crow, ffn), BF16),
                dma((n_dev, 2)),
                dma((n_dev,)),
                dma((side, 2)),
                dma((n_dev,)),
                dma((2 * side,)),
                dma((2,)),
                dma((2, 2)),
                dma((64,)),
                dma((n_chip,)),
                dma((n_dev,)),
                dma((3, 2)),
                dma((n_dev,)),
                dma((2 * side,)),
                dma((6,)),
                dma((3, 2)),
                dma((3,)),
            ],
            compiler_params=pltpu.CompilerParams(collective_id=0, has_side_effects=True, vmem_limit_bytes=58720256),
            name="moe_bwd",
        )(grad_y, topk_idx.T, slot_ids.T, gate_vals.T, pair_counts, y_routed.reshape(tok_dev * top_k, model_dim), x_disp[0], h_gate[0], h_up[0], w_gate[0], w_up[0], w_down[0])
        gx, gg, gwg, gwu, gwd = pl.pallas_call(
            write_out,
            out_shape=tuple(jax.ShapeDtypeStruct(r.shape, r.dtype) for r in results),
            in_specs=[anym] * len(results),
            out_specs=(anym,) * len(results),
            scratch_shapes=[dma((len(results),))],
            compiler_params=pltpu.CompilerParams(vmem_limit_bytes=1048576),
            name="write_out",
        )(*results)
        return gx, gg.T, gwg[None], gwu[None], gwd[None]

    return jax.shard_map(local_step, mesh=mesh, in_specs=(rows_spec, rows_spec, rows_spec, rows_spec, rows_spec, cube_spec, cube_spec, cube_spec, cube_spec, weight_spec, weight_spec, weight_spec), out_specs=(rows_spec, rows_spec, cube_spec, cube_spec, cube_spec), check_vma=False)
```

```python
import functools
import math

import jax
import jax.numpy as jnp
from jax import lax
from jax.experimental import pallas as pl
from jax.experimental.pallas import tpu as pltpu
from jax.sharding import PartitionSpec as P

MESH = pl.DeviceIdType.MESH
CORES = 2
BF16, F32 = jnp.bfloat16, jnp.float32

ORDER = ((1, 0), (0, 0), (0, 1), (-1, 0), (0, -1), (0, 2), (2, 0), (-1, 1), (1, -1), (-1, -1), (1, 1), (2, 2), (2, -1), (2, 1), (-1, 2), (1, 2))
EVENTS = {
    0: ((0, -1), (1, 0), (0, 1), (-1, 0)),
    2: ((2, 0),),
    3: ((1, -1),),
    5: ((0, 2),),
    6: ((-1, 1),),
    7: ((2, -1), (2, 1), (1, 1)),
    8: ((-1, -1),),
    11: ((2, 2),),
    12: ((-1, 2),),
    13: ((1, 2),),
}
FLIP = 1
LAG = 6

LINES = (2, -1, 1, 0)
PART = {2: 0, 1: 1, -1: 2, 0: 3}

NN = (((1,), (0,)), ((), ()))
NT = (((1,), (1,)), ((), ()))
TN = (((0,), (0,)), ((), ()))


def dot(a, b, dims):
    return lax.dot_general(a, b, dims, preferred_element_type=F32)


def lut(k, vals):
    out = vals[0]
    for i, v in enumerate(vals):
        if i:
            out = jnp.where(k == i, v, out)
    return out


def kernel(n_dev, side, gy_ref, ids_ref, slots_ref, gates_ref, pc_ref, y_ref, x_ref, hg_ref, hu_ref, wg_ref, wu_ref, wd_ref,
           gx_ref, gg_ref, gwg_ref, gwu_ref, gwd_ref,
           tokens, stab, tabs, mids, mslots, rbuf, ret, relay, part, hop_in, fin, wgu, wd, xb, hgb, hub,
           tok_sem, tab_sem, meta_sem, ret_sem, relay_sem, hop_sem, fin_sem,
           ag_send, pair_send, tab_send, meta_send, ret_send, relay_send, part_send, load_sem, w_sem):
    me = lax.axis_index("ep")
    core = me % CORES
    mx = (me // CORES) % side
    my = me // (CORES * side)
    turn = 1 - core if FLIP else core
    my_a = (1 - turn) * mx + turn * my
    my_b = (1 - turn) * my + turn * mx
    tok_dev, model_dim = gy_ref.shape
    top_k = ids_ref.shape[0]
    ffn = wg_ref.shape[1]
    cap = rbuf.shape[1]
    half = tok_dev // 2
    n_chip = side * side
    crow = CORES * cap
    partner = me + 1 - 2 * core

    def wrap(v):
        return (v + 2 * side) % side

    def device(x, y, c):
        return (wrap(y) * side + wrap(x)) * CORES + c

    def plane(a, b):
        return device(mx + (1 - turn) * a + turn * b, my + turn * a + (1 - turn) * b, core)

    def remote(src, dst, send_sem, recv_sem, to):
        return pltpu.make_async_remote_copy(src_ref=src, dst_ref=dst, send_sem=send_sem, recv_sem=recv_sem, device_id={"ep": to}, device_id_type=MESH)

    def landed(ref, sem):
        pltpu.make_async_copy(ref, ref, sem).wait()

    barrier = pltpu.get_barrier_semaphore()

    def signal_one(i, carry):
        pl.semaphore_signal(barrier, inc=1, device_id={"ep": (me + 1 + i) % n_dev}, device_id_type=MESH)
        return carry

    lax.fori_loop(0, n_dev - 1, signal_one, 0)

    wcopies = [
        pltpu.make_async_copy(wd_ref, wd, w_sem.at[0]),
        pltpu.make_async_copy(wg_ref, wgu.at[:, pl.ds(0, ffn)], w_sem.at[1]),
        pltpu.make_async_copy(wu_ref, wgu.at[:, pl.ds(ffn, ffn)], w_sem.at[2]),
    ]
    for c in wcopies:
        c.start()
    own_copies = [
        pltpu.make_async_copy(gy_ref, tokens.at[me], tok_sem.at[me, 0]),
        pltpu.make_async_copy(ids_ref, mids.at[my_b], meta_sem.at[my_b, 0]),
        pltpu.make_async_copy(slots_ref, mslots.at[my_b], meta_sem.at[my_b, 1]),
    ]
    for c in own_copies:
        c.start()

    def offset(k, axis):
        return lut(k, [o[axis] for o in ORDER])

    def chip_at(k):
        return wrap(my + offset(k, 1)) * side + wrap(mx + offset(k, 0))

    def loads(k):
        q = chip_at(k)
        slot = k % 2
        rows = pl.ds(pl.multiple_of(q * crow, crow), crow)
        return [
            pltpu.make_async_copy(x_ref.at[rows], xb.at[slot], load_sem.at[0, slot]),
            pltpu.make_async_copy(hg_ref.at[rows], hgb.at[slot], load_sem.at[1, slot]),
            pltpu.make_async_copy(hu_ref.at[rows], hub.at[slot], load_sem.at[2, slot]),
        ]

    for c in loads(0):
        c.start()

    ids = ids_ref[...]
    slots = slots_ref[...]
    gates = gates_ref[...]

    def table(e, carry):
        hit = ids == e
        slot = jnp.max(jnp.where(hit, slots, -1), axis=0, keepdims=True)
        slot = jnp.where(slot < pc_ref[0, e], slot, -1)
        gate = jnp.sum(jnp.where(hit, gates, 0.0), axis=0, keepdims=True)
        stab[e] = jnp.concatenate([slot.astype(F32), gate], axis=0)
        return carry

    lax.fori_loop(0, n_dev, table, 0)
    gwg_ref[...] = jnp.zeros_like(gwg_ref)
    gwu_ref[...] = jnp.zeros_like(gwu_ref)
    gwd_ref[...] = jnp.zeros_like(gwd_ref)
    pl.semaphore_wait(barrier, n_dev - 1)
    own_copies[0].wait()

    sends, pairs = [], []

    def block(src, h):
        return tokens.at[src, pl.ds(h * half, half)]

    def forward_msg(n, i, j, h, a, b):
        src = plane(i, j)
        return remote(block(src, h), block(src, h), ag_send.at[n], tok_sem.at[src, h], plane(a, b))

    def forward(*what):
        what = (len(sends), *what)
        sends.append(what)
        forward_msg(*what).start()

    def pair_msg(n, i, j):
        src = plane(i, j)
        return remote(tokens.at[src], tokens.at[src], pair_send.at[n], tok_sem.at[src, 0], partner)

    def to_partner(i, j):
        what = (len(pairs), i, j)
        pairs.append(what)
        pair_msg(*what).start()

    def arrived(src, h):
        landed(block(src, h), tok_sem.at[src, h])

    to_partner(0, 0)

    def tab_msg(i):
        to = (me + 1 + i) % n_dev
        return remote(stab.at[to], tabs.at[me], tab_send.at[i], tab_sem.at[me], to)

    def tab_start(i, carry):
        tab_msg(i).start()
        return carry

    lax.fori_loop(0, n_dev - 1, tab_start, 0)
    tab_copy = pltpu.make_async_copy(stab.at[me], tabs.at[me], tab_sem.at[me])
    tab_copy.start()
    for n in range(2):
        for a, b, h in ((1, 0, n), (-1, 0, 1 - n), (0, 1, n), (0, -1, 1 - n)):
            forward(0, 0, h, a, b)

    def meta_msgs():
        out = []
        for n, j in enumerate((1, -1, 2)):
            out.append(remote(ids_ref, mids.at[my_b], meta_send.at[n, 0], meta_sem.at[my_b, 0], plane(0, j)))
            out.append(remote(slots_ref, mslots.at[my_b], meta_send.at[n, 1], meta_sem.at[my_b, 1], plane(0, j)))
        return out

    for c in meta_msgs():
        c.start()

    def event(i, j):
        src = plane(i, j)
        first = 1 if (i == 1 and j == 0) or j == 1 else 0
        for n, h in enumerate((first, 1 - first)):
            arrived(src, h)
            if j == 0:
                if n == 0 and abs(i) == 1:
                    forward(i, j, h, -i, 0)
                forward(i, j, h, 0, 1)
                forward(i, j, h, 0, -1)
            elif n == 0 and abs(j) == 1:
                forward(i, j, h, 0, -j)
        to_partner(i, j)

    def r_block(k, cc):
        axis = 1 - cc if FLIP else cc
        i, j = offset(k, axis), offset(k, 1 - axis)
        a, b = (mx, my) if axis == 0 else (my, mx)
        hb = wrap(b + j)
        home = chip_at(k) * CORES + cc
        step = jnp.where(i == 2, 1 - 2 * core, i)
        to = device(mx + step, my, cc) if axis == 0 else device(mx, my + step, cc)
        slot = (hb * side + a) * CORES + core
        hop = hb * 2 + core
        is_local = jnp.logical_and(i == 0, core == cc)
        return i, home, to, slot, hop, is_local

    def send_chunk(k):
        for cc in range(CORES):
            i, home, to, slot, hop, is_local = r_block(k, cc)

            @pl.when(is_local)
            def _():
                pltpu.make_async_copy(rbuf.at[home], ret.at[slot], ret_sem.at[slot]).start()

            @pl.when(i == 2)
            def _():
                remote(rbuf.at[home], relay.at[hop], ret_send.at[home], relay_sem.at[hop], to).start()

            @pl.when(jnp.logical_and(i != 2, jnp.logical_not(is_local)))
            def _():
                remote(rbuf.at[home], ret.at[slot], ret_send.at[home], ret_sem.at[slot], to).start()

    def relay_msg(j, way):
        hb = wrap(my_b + j)
        slot = (hb * side + wrap(my_a - 1 + 2 * way)) * CORES + way
        hop = hb * 2 + way
        return hop, remote(relay.at[hop], ret.at[slot], relay_send.at[hop], ret_sem.at[slot], plane(1 - 2 * way, 0))

    def hand_on(k):
        i = jnp.where(turn == 0, offset(k, 0), offset(k, 1))
        j = jnp.where(turn == 0, offset(k, 1), offset(k, 0))

        @pl.when(i == 2)
        def _():
            for way in range(2):
                hop, msg = relay_msg(j, way)
                landed(relay.at[hop], relay_sem.at[hop])
                msg.start()

    slot_iota = lax.broadcasted_iota(jnp.int32, (cap, tok_dev), 0)
    slot_iota_f = slot_iota.astype(F32)
    for c in wcopies:
        c.wait()

    def chunk(k, carry):
        for at, evs in EVENTS.items():
            @pl.when(k == at)
            def _(evs=evs):
                for i, j in evs:
                    event(i, j)

        @pl.when(k > 0)
        def _():
            send_chunk(k - 1)

        @pl.when(k >= LAG)
        def _():
            hand_on(k - LAG)

        slot = k % 2
        for c in loads(k):
            c.wait()

        @pl.when(k + 1 < n_chip)
        def _():
            for c in loads(k + 1):
                c.start()

        q = chip_at(k)
        landed(tokens.at[q * CORES + 1 - core], tok_sem.at[q * CORES + 1 - core, 0])

        d_parts = []
        for cc in range(CORES):
            home = q * CORES + cc
            landed(tabs.at[home], tab_sem.at[home])
            tab = tabs[home]
            pick = tab[0:1, :] == slot_iota_f
            gate = jnp.sum(jnp.where(pick, tab[1:2, :], 0.0), axis=1, keepdims=True)
            rows = dot(pick.astype(F32).astype(BF16), tokens[home], NN)
            d_parts.append((gate * rows).astype(BF16))
        d = jnp.concatenate(d_parts, axis=0)
        da = dot(d, wd[...], NT).astype(BF16).astype(F32)
        h1 = hgb[slot].astype(F32)
        h3 = hub[slot].astype(F32)
        g = jax.nn.sigmoid(h1)
        s = h1 * g
        act = (s * h3).astype(BF16)
        dh1 = (da * h3 * g * (1.0 + h1 * (1.0 - g))).astype(BF16)
        dh3 = (da * s).astype(BF16)
        dh = jnp.concatenate([dh1, dh3], axis=1)
        r = dot(dh, wgu[...], NT).astype(BF16)
        for cc in range(CORES):
            rbuf[q * CORES + cc] = r[cc * cap:(cc + 1) * cap]
        x = xb[slot]
        gwg_ref[...] += dot(x, dh1, TN)
        gwu_ref[...] += dot(x, dh3, TN)
        gwd_ref[...] += dot(act, d, TN)
        return carry

    lax.fori_loop(0, n_chip, chunk, 0)
    send_chunk(jnp.int32(n_chip - 1))

    n_run = crow // top_k
    n_step = tok_dev // n_run

    def y_load(m):
        return pltpu.make_async_copy(y_ref.at[pl.ds(pl.multiple_of(m * crow, crow), crow)], xb.at[m % 2], load_sem.at[0, m % 2])

    y_load(0).start()
    lane = lax.broadcasted_iota(jnp.int32, (crow, tok_dev), 1)
    token_of = lax.broadcasted_iota(jnp.int32, (crow, tok_dev), 0) // top_k
    gg_ref[...] = jnp.zeros_like(gg_ref)

    def gate_grad(m, carry):
        y_load(m).wait()

        @pl.when(m + 1 < n_step)
        def _():
            y_load(m + 1).start()

        gy = tokens[me, pl.ds(pl.multiple_of(m * n_run, n_run), n_run), :].astype(F32)
        gy = jnp.broadcast_to(gy[:, None, :], (n_run, top_k, model_dim)).reshape(crow, model_dim)
        col = jnp.sum(xb[m % 2].astype(F32) * gy, axis=1, keepdims=True)
        put = jnp.where(lane == token_of + m * n_run, col, 0.0)
        gg_ref[...] += jnp.sum(put.reshape(n_run, top_k, tok_dev), axis=0)
        return carry

    for k in range(n_chip - LAG, n_chip):
        hand_on(jnp.int32(k))

    lax.fori_loop(0, n_step - 1, gate_grad, 0)

    def add_rows(n, carry):
        j = lut(n, LINES)
        hb = wrap(my_b + j)
        landed(mids.at[hb], meta_sem.at[hb, 0])
        landed(mslots.at[hb], meta_sem.at[hb, 1])
        h_ids = mids[hb]
        h_slots = mslots[hb]
        picks = []
        for sa in range(side):
            for ce in range(CORES):
                slot = (hb * side + sa) * CORES + ce
                landed(ret.at[slot], ret_sem.at[slot])
                x = (1 - turn) * sa + turn * my_b
                y = (1 - turn) * my_b + turn * sa
                row = jnp.max(jnp.where(h_ids == (y * side + x) * CORES + ce, h_slots, -1), axis=0, keepdims=True)
                picks.append((row == slot_iota).astype(F32).astype(BF16))
        pick = jnp.concatenate(picks, axis=0)
        rows = ret[pl.ds(hb * side * CORES, side * CORES)].reshape(side * CORES * cap, model_dim)
        part[lut(n, [PART[v] for v in LINES])] = dot(pick, rows, TN)

        @pl.when(n == 0)
        def _():
            gate_grad(n_step - 1, 0)
            for c in hop_msgs():
                c.start()

        return carry

    def hop_msgs():
        return [
            remote(part.at[0, pl.ds(0, half)], hop_in.at[0], part_send.at[0], hop_sem.at[0], plane(0, 1)),
            remote(part.at[0, pl.ds(half, half)], hop_in.at[1], part_send.at[1], hop_sem.at[1], plane(0, -1)),
        ]

    def fin_msgs():
        return [
            remote(part.at[1 + n, pl.ds(h * half, half)], fin.at[n, pl.ds(h * half, half)], part_send.at[2 + 2 * n + h], fin_sem.at[n, h], plane(0, 1 - 2 * n))
            for n in range(2)
            for h in range(2)
        ]

    fins = fin_msgs()
    lax.fori_loop(0, len(LINES), add_rows, 0)
    fins[1].start()
    fins[2].start()
    landed(hop_in.at[0], hop_sem.at[0])
    part[1, pl.ds(0, half)] += hop_in[0]
    landed(hop_in.at[1], hop_sem.at[1])
    part[2, pl.ds(half, half)] += hop_in[1]
    for what in sends:
        forward_msg(*what).wait_send()
    for what in pairs:
        pair_msg(*what).wait_send()
    fins[0].start()
    fins[3].start()


    def tab_done(i, carry):
        tab_msg(i).wait_send()
        return carry

    lax.fori_loop(0, n_dev - 1, tab_done, 0)
    for c in meta_msgs() + hop_msgs():
        c.wait_send()

    def ret_done(k, carry):
        for cc in range(CORES):
            i, home, to, slot, hop, is_local = r_block(k, cc)

            @pl.when(jnp.logical_not(is_local))
            def _():
                remote(rbuf.at[home], ret.at[slot], ret_send.at[home], ret_sem.at[slot], to).wait_send()
        return carry

    lax.fori_loop(0, n_chip, ret_done, 0)
    for j in (0, 1, -1, 2):
        for way in range(2):
            relay_msg(j, way)[1].wait_send()
    for n in range(2):
        for h in range(2):
            landed(fin.at[n, pl.ds(h * half, half)], fin_sem.at[n, h])
    gx_ref[...] = (part[3] + fin[0] + fin[1]).astype(gx_ref.dtype)
    for c in fins:
        c.wait_send()


def write_out(*refs):
    n = len(refs) // 2
    sems = refs[-1]
    copies = [pltpu.make_async_copy(refs[i], refs[n + i], sems.at[i]) for i in range(n)]
    for c in copies:
        c.start()
    for c in copies:
        c.wait()


def solution(mesh):
    n_dev = mesh.shape["ep"]
    side = math.isqrt(n_dev // CORES)
    rows_spec = P(("dp", "ep"), None)
    cube_spec = P(("dp", "ep"), None, None)
    weight_spec = P("ep", None, None)

    def local_step(grad_y, gate_vals, topk_idx, slot_ids, pair_counts, y_routed, x_disp, h_gate, h_up, w_gate, w_up, w_down):
        assert w_gate.shape[0] == 1
        assert side * side * CORES == n_dev and len(ORDER) == side * side
        cap = x_disp.shape[1] // n_dev
        tok_dev, model_dim = grad_y.shape
        ffn = w_gate.shape[2]
        crow = CORES * cap
        n_chip = side * side
        top_k = topk_idx.shape[1]
        vmem = pl.BlockSpec(memory_space=pltpu.VMEM)
        smem = pl.BlockSpec(memory_space=pltpu.SMEM)
        anym = pl.BlockSpec(memory_space=pl.ANY)
        dma = pltpu.SemaphoreType.DMA
        results = pl.pallas_call(
            functools.partial(kernel, n_dev, side),
            out_shape=(
                pltpu.VMEM((tok_dev, model_dim), BF16),
                pltpu.VMEM((top_k, tok_dev), F32),
                pltpu.VMEM((model_dim, ffn), F32),
                pltpu.VMEM((model_dim, ffn), F32),
                pltpu.VMEM((ffn, model_dim), F32),
            ),
            in_specs=[anym, vmem, vmem, vmem, smem] + [anym] * 7,
            out_specs=(vmem,) * 5,
            scratch_shapes=[
                pltpu.VMEM((n_dev, tok_dev, model_dim), BF16),
                pltpu.VMEM((n_dev, 2, tok_dev), F32),
                pltpu.VMEM((n_dev, 2, tok_dev), F32),
                pltpu.VMEM((side, top_k, tok_dev), jnp.int32),
                pltpu.VMEM((side, top_k, tok_dev), jnp.int32),
                pltpu.VMEM((n_dev, cap, model_dim), BF16),
                pltpu.VMEM((n_dev, cap, model_dim), BF16),
                pltpu.VMEM((2 * side, cap, model_dim), BF16),
                pltpu.VMEM((4, tok_dev, model_dim), F32),
                pltpu.VMEM((2, tok_dev // 2, model_dim), F32),
                pltpu.VMEM((2, tok_dev, model_dim), F32),
                pltpu.VMEM((model_dim, 2 * ffn), BF16),
                pltpu.VMEM((ffn, model_dim), BF16),
                pltpu.VMEM((2, crow, model_dim), BF16),
                pltpu.VMEM((2, crow, ffn), BF16),
                pltpu.VMEM((2, crow, ffn), BF16),
                dma((n_dev, 2)),
                dma((n_dev,)),
                dma((side, 2)),
                dma((n_dev,)),
                dma((2 * side,)),
                dma((2,)),
                dma((2, 2)),
                dma((64,)),
                dma((n_chip,)),
                dma((n_dev,)),
                dma((3, 2)),
                dma((n_dev,)),
                dma((2 * side,)),
                dma((6,)),
                dma((3, 2)),
                dma((3,)),
            ],
            compiler_params=pltpu.CompilerParams(collective_id=0, has_side_effects=True, vmem_limit_bytes=58720256),
            name="moe_bwd",
        )(grad_y, topk_idx.T, slot_ids.T, gate_vals.T, pair_counts, y_routed.reshape(tok_dev * top_k, model_dim), x_disp[0], h_gate[0], h_up[0], w_gate[0], w_up[0], w_down[0])
        gx, gg, gwg, gwu, gwd = pl.pallas_call(
            write_out,
            out_shape=tuple(jax.ShapeDtypeStruct(r.shape, r.dtype) for r in results),
            in_specs=[anym] * len(results),
            out_specs=(anym,) * len(results),
            scratch_shapes=[dma((len(results),))],
            compiler_params=pltpu.CompilerParams(vmem_limit_bytes=1048576),
            name="write_out",
        )(*results)
        return gx, gg.T, gwg[None], gwu[None], gwd[None]

    return jax.shard_map(local_step, mesh=mesh, in_specs=(rows_spec, rows_spec, rows_spec, rows_spec, rows_spec, cube_spec, cube_spec, cube_spec, cube_spec, weight_spec, weight_spec, weight_spec), out_specs=(rows_spec, rows_spec, cube_spec, cube_spec, cube_spec), check_vma=False)
```

```python
import functools
import math

import jax
import jax.numpy as jnp
from jax import lax
from jax.experimental import pallas as pl
from jax.experimental.pallas import tpu as pltpu
from jax.sharding import PartitionSpec as P

MESH = pl.DeviceIdType.MESH
CORES = 2
BF16, F32 = jnp.bfloat16, jnp.float32

ORDER = ((-1, 0), (0, 1), (0, -1), (0, 0), (-1, 1), (1, 0), (1, -1), (1, 1), (0, 2), (-1, -1), (2, 0), (2, 1), (2, -1), (2, 2), (1, 2), (-1, 2))
EVENTS = {
    0: ((-1, 0), (0, -1), (1, 0), (0, 1)),
    2: ((2, 0), (-1, 1)),
    4: ((0, 2), (1, -1), (-1, -1)),
    5: ((1, 1),),
    6: ((2, -1),),
    9: ((2, 1),),
    10: ((1, 2),),
    12: ((2, 2), (-1, 2)),
}
FLIP = 1
RELAY = {15: (11,)}
TAIL_RELAY = (13, 10, 8, 14), (15, 12)

LINES = (2, 0, -1, 1)
PART = {2: 0, 1: 1, -1: 2, 0: 3}

NN = (((1,), (0,)), ((), ()))
NT = (((1,), (1,)), ((), ()))
TN = (((0,), (0,)), ((), ()))


def dot(a, b, dims):
    return lax.dot_general(a, b, dims, preferred_element_type=F32)


def lut(k, vals):
    out = vals[0]
    for i, v in enumerate(vals):
        if i:
            out = jnp.where(k == i, v, out)
    return out


def kernel(n_dev, side, gy_ref, ids_ref, slots_ref, gates_ref, pc_ref, y_ref, x_ref, hg_ref, hu_ref, wg_ref, wu_ref, wd_ref,
           gx_ref, gg_ref, gwg_ref, gwu_ref, gwd_ref,
           tokens, stab, tabs, mids, mslots, rbuf, ret, relay, part, hop_in, fin, wgu, wd, xb, hgb, hub,
           tok_sem, tab_sem, meta_sem, ret_sem, relay_sem, hop_sem, fin_sem,
           ag_send, pair_send, tab_send, meta_send, ret_send, relay_send, part_send, load_sem, w_sem):
    me = lax.axis_index("ep")
    core = me % CORES
    mx = (me // CORES) % side
    my = me // (CORES * side)
    turn = 1 - core if FLIP else core
    my_a = (1 - turn) * mx + turn * my
    my_b = (1 - turn) * my + turn * mx
    tok_dev, model_dim = gy_ref.shape
    top_k = ids_ref.shape[0]
    ffn = wg_ref.shape[1]
    cap = rbuf.shape[1]
    half = tok_dev // 2
    n_chip = side * side
    crow = CORES * cap
    partner = me + 1 - 2 * core

    def wrap(v):
        return (v + 2 * side) % side

    def device(x, y, c):
        return (wrap(y) * side + wrap(x)) * CORES + c

    def plane(a, b):
        return device(mx + (1 - turn) * a + turn * b, my + turn * a + (1 - turn) * b, core)

    def remote(src, dst, send_sem, recv_sem, to):
        return pltpu.make_async_remote_copy(src_ref=src, dst_ref=dst, send_sem=send_sem, recv_sem=recv_sem, device_id={"ep": to}, device_id_type=MESH)

    def landed(ref, sem):
        pltpu.make_async_copy(ref, ref, sem).wait()

    barrier = pltpu.get_barrier_semaphore()

    def signal_one(i, carry):
        pl.semaphore_signal(barrier, inc=1, device_id={"ep": (me + 1 + i) % n_dev}, device_id_type=MESH)
        return carry

    lax.fori_loop(0, n_dev - 1, signal_one, 0)

    wcopies = [
        pltpu.make_async_copy(wd_ref, wd, w_sem.at[0]),
        pltpu.make_async_copy(wg_ref, wgu.at[:, pl.ds(0, ffn)], w_sem.at[1]),
        pltpu.make_async_copy(wu_ref, wgu.at[:, pl.ds(ffn, ffn)], w_sem.at[2]),
    ]
    for c in wcopies:
        c.start()
    own_copies = [
        pltpu.make_async_copy(gy_ref, tokens.at[me], tok_sem.at[me, 0]),
        pltpu.make_async_copy(ids_ref, mids.at[my_b], meta_sem.at[my_b, 0]),
        pltpu.make_async_copy(slots_ref, mslots.at[my_b], meta_sem.at[my_b, 1]),
    ]
    for c in own_copies:
        c.start()

    def offset(k, axis):
        return lut(k, [o[axis] for o in ORDER])

    def chip_at(k):
        return wrap(my + offset(k, 1)) * side + wrap(mx + offset(k, 0))

    def loads(k):
        q = chip_at(k)
        slot = k % 2
        rows = pl.ds(pl.multiple_of(q * crow, crow), crow)
        return [
            pltpu.make_async_copy(x_ref.at[rows], xb.at[slot], load_sem.at[0, slot]),
            pltpu.make_async_copy(hg_ref.at[rows], hgb.at[slot], load_sem.at[1, slot]),
            pltpu.make_async_copy(hu_ref.at[rows], hub.at[slot], load_sem.at[2, slot]),
        ]

    for c in loads(0):
        c.start()

    ids = ids_ref[...]
    slots = slots_ref[...]
    gates = gates_ref[...]

    def table(e, carry):
        hit = ids == e
        slot = jnp.max(jnp.where(hit, slots, -1), axis=0, keepdims=True)
        slot = jnp.where(slot < pc_ref[0, e], slot, -1)
        gate = jnp.sum(jnp.where(hit, gates, 0.0), axis=0, keepdims=True)
        stab[e] = jnp.concatenate([slot.astype(F32), gate], axis=0)
        return carry

    lax.fori_loop(0, n_dev, table, 0)
    gwg_ref[...] = jnp.zeros_like(gwg_ref)
    gwu_ref[...] = jnp.zeros_like(gwu_ref)
    gwd_ref[...] = jnp.zeros_like(gwd_ref)
    pl.semaphore_wait(barrier, n_dev - 1)
    own_copies[0].wait()

    sends, pairs = [], []

    def block(src, h):
        return tokens.at[src, pl.ds(h * half, half)]

    def forward_msg(n, i, j, h, a, b):
        src = plane(i, j)
        return remote(block(src, h), block(src, h), ag_send.at[n], tok_sem.at[src, h], plane(a, b))

    def forward(*what):
        what = (len(sends), *what)
        sends.append(what)
        forward_msg(*what).start()

    def pair_msg(n, i, j):
        src = plane(i, j)
        return remote(tokens.at[src], tokens.at[src], pair_send.at[n], tok_sem.at[src, 0], partner)

    def to_partner(i, j):
        what = (len(pairs), i, j)
        pairs.append(what)
        pair_msg(*what).start()

    def arrived(src, h):
        landed(block(src, h), tok_sem.at[src, h])

    to_partner(0, 0)

    def tab_msg(i):
        to = (me + 1 + i) % n_dev
        return remote(stab.at[to], tabs.at[me], tab_send.at[i], tab_sem.at[me], to)

    def tab_start(i, carry):
        tab_msg(i).start()
        return carry

    lax.fori_loop(0, n_dev - 1, tab_start, 0)
    tab_copy = pltpu.make_async_copy(stab.at[me], tabs.at[me], tab_sem.at[me])
    tab_copy.start()
    for n in range(2):
        for a, b, h in ((1, 0, n), (-1, 0, 1 - n), (0, 1, n), (0, -1, 1 - n)):
            forward(0, 0, h, a, b)

    def meta_msgs():
        out = []
        for n, j in enumerate((1, -1, 2)):
            out.append(remote(ids_ref, mids.at[my_b], meta_send.at[n, 0], meta_sem.at[my_b, 0], plane(0, j)))
            out.append(remote(slots_ref, mslots.at[my_b], meta_send.at[n, 1], meta_sem.at[my_b, 1], plane(0, j)))
        return out

    for c in meta_msgs():
        c.start()

    def event(i, j):
        src = plane(i, j)
        first = 1 if (i == 1 and j == 0) or j == 1 else 0
        for n, h in enumerate((first, 1 - first)):
            arrived(src, h)
            if j == 0:
                if n == 0 and abs(i) == 1:
                    forward(i, j, h, -i, 0)
                forward(i, j, h, 0, 1)
                forward(i, j, h, 0, -1)
            elif n == 0 and abs(j) == 1:
                forward(i, j, h, 0, -j)
        to_partner(i, j)

    def r_block(k, cc):
        axis = 1 - cc if FLIP else cc
        i, j = offset(k, axis), offset(k, 1 - axis)
        a, b = (mx, my) if axis == 0 else (my, mx)
        hb = wrap(b + j)
        home = chip_at(k) * CORES + cc
        step = jnp.where(i == 2, 1 - 2 * core, i)
        to = device(mx + step, my, cc) if axis == 0 else device(mx, my + step, cc)
        slot = (hb * side + a) * CORES + core
        hop = hb * 2 + core
        is_local = jnp.logical_and(i == 0, core == cc)
        return i, home, to, slot, hop, is_local

    def send_chunk(k):
        for cc in range(CORES):
            i, home, to, slot, hop, is_local = r_block(k, cc)

            @pl.when(is_local)
            def _():
                pltpu.make_async_copy(rbuf.at[home], ret.at[slot], ret_sem.at[slot]).start()

            @pl.when(i == 2)
            def _():
                remote(rbuf.at[home], relay.at[hop], ret_send.at[home], relay_sem.at[hop], to).start()

            @pl.when(jnp.logical_and(i != 2, jnp.logical_not(is_local)))
            def _():
                remote(rbuf.at[home], ret.at[slot], ret_send.at[home], ret_sem.at[slot], to).start()

    def relay_msg(j, way):
        hb = wrap(my_b + j)
        slot = (hb * side + wrap(my_a - 1 + 2 * way)) * CORES + way
        hop = hb * 2 + way
        return hop, remote(relay.at[hop], ret.at[slot], relay_send.at[hop], ret_sem.at[slot], plane(1 - 2 * way, 0))

    def hand_on(k):
        dx, dy = ORDER[k]
        i = jnp.where(turn == 0, dx, dy)
        j = jnp.where(turn == 0, dy, dx)

        @pl.when(i == 2)
        def _():
            for way in range(2):
                hop, msg = relay_msg(j, way)
                landed(relay.at[hop], relay_sem.at[hop])
                msg.start()

    slot_iota = lax.broadcasted_iota(jnp.int32, (cap, tok_dev), 0)
    slot_iota_f = slot_iota.astype(F32)
    for c in wcopies:
        c.wait()

    def chunk(k, carry):
        for at, evs in EVENTS.items():
            @pl.when(k == at)
            def _(evs=evs):
                for i, j in evs:
                    event(i, j)

        @pl.when(k > 0)
        def _():
            send_chunk(k - 1)

        for at, steps in RELAY.items():
            @pl.when(k == at)
            def _(steps=steps):
                for n in steps:
                    hand_on(n)

        slot = k % 2
        for c in loads(k):
            c.wait()

        @pl.when(k + 1 < n_chip)
        def _():
            for c in loads(k + 1):
                c.start()

        q = chip_at(k)
        landed(tokens.at[q * CORES + 1 - core], tok_sem.at[q * CORES + 1 - core, 0])

        d_parts = []
        for cc in range(CORES):
            home = q * CORES + cc
            landed(tabs.at[home], tab_sem.at[home])
            tab = tabs[home]
            pick = tab[0:1, :] == slot_iota_f
            gate = jnp.sum(jnp.where(pick, tab[1:2, :], 0.0), axis=1, keepdims=True)
            rows = dot(pick.astype(F32).astype(BF16), tokens[home], NN)
            d_parts.append((gate * rows).astype(BF16))
        d = jnp.concatenate(d_parts, axis=0)
        da = dot(d, wd[...], NT).astype(BF16).astype(F32)
        h1 = hgb[slot].astype(F32)
        h3 = hub[slot].astype(F32)
        g = jax.nn.sigmoid(h1)
        s = h1 * g
        act = (s * h3).astype(BF16)
        dh1 = (da * h3 * g * (1.0 + h1 * (1.0 - g))).astype(BF16)
        dh3 = (da * s).astype(BF16)
        dh = jnp.concatenate([dh1, dh3], axis=1)
        r = dot(dh, wgu[...], NT).astype(BF16)
        for cc in range(CORES):
            rbuf[q * CORES + cc] = r[cc * cap:(cc + 1) * cap]
        x = xb[slot]
        gwg_ref[...] += dot(x, dh1, TN)
        gwu_ref[...] += dot(x, dh3, TN)
        gwd_ref[...] += dot(act, d, TN)
        return carry

    lax.fori_loop(0, n_chip, chunk, 0)
    send_chunk(jnp.int32(n_chip - 1))

    n_run = crow // top_k
    n_step = tok_dev // n_run

    def y_load(m):
        return pltpu.make_async_copy(y_ref.at[pl.ds(pl.multiple_of(m * crow, crow), crow)], xb.at[m % 2], load_sem.at[0, m % 2])

    y_load(0).start()
    lane = lax.broadcasted_iota(jnp.int32, (crow, tok_dev), 1)
    token_of = lax.broadcasted_iota(jnp.int32, (crow, tok_dev), 0) // top_k
    gg_ref[...] = jnp.zeros_like(gg_ref)

    def gate_grad(m, carry):
        y_load(m).wait()

        @pl.when(m + 1 < n_step)
        def _():
            y_load(m + 1).start()

        gy = tokens[me, pl.ds(pl.multiple_of(m * n_run, n_run), n_run), :].astype(F32)
        gy = jnp.broadcast_to(gy[:, None, :], (n_run, top_k, model_dim)).reshape(crow, model_dim)
        col = jnp.sum(xb[m % 2].astype(F32) * gy, axis=1, keepdims=True)
        put = jnp.where(lane == token_of + m * n_run, col, 0.0)
        gg_ref[...] += jnp.sum(put.reshape(n_run, top_k, tok_dev), axis=0)
        return carry

    for k in TAIL_RELAY[0]:
        hand_on(k)
    lax.fori_loop(0, n_step, gate_grad, 0)
    for k in TAIL_RELAY[1]:
        hand_on(k)

    def add_rows(n, carry):
        j = lut(n, LINES)
        hb = wrap(my_b + j)
        landed(mids.at[hb], meta_sem.at[hb, 0])
        landed(mslots.at[hb], meta_sem.at[hb, 1])
        h_ids = mids[hb]
        h_slots = mslots[hb]
        picks = []
        for sa in range(side):
            for ce in range(CORES):
                slot = (hb * side + sa) * CORES + ce
                landed(ret.at[slot], ret_sem.at[slot])
                x = (1 - turn) * sa + turn * my_b
                y = (1 - turn) * my_b + turn * sa
                row = jnp.max(jnp.where(h_ids == (y * side + x) * CORES + ce, h_slots, -1), axis=0, keepdims=True)
                picks.append((row == slot_iota).astype(F32).astype(BF16))
        pick = jnp.concatenate(picks, axis=0)
        rows = ret[pl.ds(hb * side * CORES, side * CORES)].reshape(side * CORES * cap, model_dim)
        part[lut(n, [PART[v] for v in LINES])] = dot(pick, rows, TN)

        @pl.when(n == 1)
        def _():
            for c in hop_msgs():
                c.start()

        return carry

    def hop_msgs():
        return [
            remote(part.at[0, pl.ds(0, half)], hop_in.at[0], part_send.at[0], hop_sem.at[0], plane(0, 1)),
            remote(part.at[0, pl.ds(half, half)], hop_in.at[1], part_send.at[1], hop_sem.at[1], plane(0, -1)),
        ]

    def fin_msgs():
        return [
            remote(part.at[1 + n, pl.ds(h * half, half)], fin.at[n, pl.ds(h * half, half)], part_send.at[2 + 2 * n + h], fin_sem.at[n, h], plane(0, 1 - 2 * n))
            for n in range(2)
            for h in range(2)
        ]

    fins = fin_msgs()
    lax.fori_loop(0, len(LINES), add_rows, 0)
    fins[2].start()
    for what in sends:
        forward_msg(*what).wait_send()
    for what in pairs:
        pair_msg(*what).wait_send()
    fins[1].start()
    landed(hop_in.at[0], hop_sem.at[0])
    part[1, pl.ds(0, half)] += hop_in[0]
    landed(hop_in.at[1], hop_sem.at[1])
    part[2, pl.ds(half, half)] += hop_in[1]

    def tab_done(i, carry):
        tab_msg(i).wait_send()
        return carry

    lax.fori_loop(0, n_dev - 1, tab_done, 0)
    fins[0].start()
    fins[3].start()
    for c in meta_msgs() + hop_msgs():
        c.wait_send()

    def ret_done(k, carry):
        for cc in range(CORES):
            i, home, to, slot, hop, is_local = r_block(k, cc)

            @pl.when(jnp.logical_not(is_local))
            def _():
                remote(rbuf.at[home], ret.at[slot], ret_send.at[home], ret_sem.at[slot], to).wait_send()
        return carry

    lax.fori_loop(0, n_chip, ret_done, 0)
    for j in (0, 1, -1, 2):
        for way in range(2):
            relay_msg(j, way)[1].wait_send()
    for n in range(2):
        for h in range(2):
            landed(fin.at[n, pl.ds(h * half, half)], fin_sem.at[n, h])
    gx_ref[...] = (part[3] + fin[0] + fin[1]).astype(gx_ref.dtype)
    for c in fins:
        c.wait_send()


def write_out(*refs):
    n = len(refs) // 2
    sems = refs[-1]
    copies = [pltpu.make_async_copy(refs[i], refs[n + i], sems.at[i]) for i in range(n)]
    for c in copies:
        c.start()
    for c in copies:
        c.wait()


def solution(mesh):
    n_dev = mesh.shape["ep"]
    side = math.isqrt(n_dev // CORES)
    rows_spec = P(("dp", "ep"), None)
    cube_spec = P(("dp", "ep"), None, None)
    weight_spec = P("ep", None, None)

    def local_step(grad_y, gate_vals, topk_idx, slot_ids, pair_counts, y_routed, x_disp, h_gate, h_up, w_gate, w_up, w_down):
        assert w_gate.shape[0] == 1
        assert side * side * CORES == n_dev and len(ORDER) == side * side
        cap = x_disp.shape[1] // n_dev
        tok_dev, model_dim = grad_y.shape
        ffn = w_gate.shape[2]
        crow = CORES * cap
        n_chip = side * side
        top_k = topk_idx.shape[1]
        vmem = pl.BlockSpec(memory_space=pltpu.VMEM)
        smem = pl.BlockSpec(memory_space=pltpu.SMEM)
        anym = pl.BlockSpec(memory_space=pl.ANY)
        dma = pltpu.SemaphoreType.DMA
        results = pl.pallas_call(
            functools.partial(kernel, n_dev, side),
            out_shape=(
                pltpu.VMEM((tok_dev, model_dim), BF16),
                pltpu.VMEM((top_k, tok_dev), F32),
                pltpu.VMEM((model_dim, ffn), F32),
                pltpu.VMEM((model_dim, ffn), F32),
                pltpu.VMEM((ffn, model_dim), F32),
            ),
            in_specs=[anym, vmem, vmem, vmem, smem] + [anym] * 7,
            out_specs=(vmem,) * 5,
            scratch_shapes=[
                pltpu.VMEM((n_dev, tok_dev, model_dim), BF16),
                pltpu.VMEM((n_dev, 2, tok_dev), F32),
                pltpu.VMEM((n_dev, 2, tok_dev), F32),
                pltpu.VMEM((side, top_k, tok_dev), jnp.int32),
                pltpu.VMEM((side, top_k, tok_dev), jnp.int32),
                pltpu.VMEM((n_dev, cap, model_dim), BF16),
                pltpu.VMEM((n_dev, cap, model_dim), BF16),
                pltpu.VMEM((2 * side, cap, model_dim), BF16),
                pltpu.VMEM((4, tok_dev, model_dim), F32),
                pltpu.VMEM((2, tok_dev // 2, model_dim), F32),
                pltpu.VMEM((2, tok_dev, model_dim), F32),
                pltpu.VMEM((model_dim, 2 * ffn), BF16),
                pltpu.VMEM((ffn, model_dim), BF16),
                pltpu.VMEM((2, crow, model_dim), BF16),
                pltpu.VMEM((2, crow, ffn), BF16),
                pltpu.VMEM((2, crow, ffn), BF16),
                dma((n_dev, 2)),
                dma((n_dev,)),
                dma((side, 2)),
                dma((n_dev,)),
                dma((2 * side,)),
                dma((2,)),
                dma((2, 2)),
                dma((64,)),
                dma((n_chip,)),
                dma((n_dev,)),
                dma((3, 2)),
                dma((n_dev,)),
                dma((2 * side,)),
                dma((6,)),
                dma((3, 2)),
                dma((3,)),
            ],
            compiler_params=pltpu.CompilerParams(collective_id=0, has_side_effects=True, vmem_limit_bytes=58720256),
            name="moe_bwd",
        )(grad_y, topk_idx.T, slot_ids.T, gate_vals.T, pair_counts, y_routed.reshape(tok_dev * top_k, model_dim), x_disp[0], h_gate[0], h_up[0], w_gate[0], w_up[0], w_down[0])
        gx, gg, gwg, gwu, gwd = pl.pallas_call(
            write_out,
            out_shape=tuple(jax.ShapeDtypeStruct(r.shape, r.dtype) for r in results),
            in_specs=[anym] * len(results),
            out_specs=(anym,) * len(results),
            scratch_shapes=[dma((len(results),))],
            compiler_params=pltpu.CompilerParams(vmem_limit_bytes=1048576),
            name="write_out",
        )(*results)
        return gx, gg.T, gwg[None], gwu[None], gwd[None]

    return jax.shard_map(local_step, mesh=mesh, in_specs=(rows_spec, rows_spec, rows_spec, rows_spec, rows_spec, cube_spec, cube_spec, cube_spec, cube_spec, weight_spec, weight_spec, weight_spec), out_specs=(rows_spec, rows_spec, cube_spec, cube_spec, cube_spec), check_vma=False)
```

```python
import functools
import math

import jax
import jax.numpy as jnp
from jax import lax
from jax.experimental import pallas as pl
from jax.experimental.pallas import tpu as pltpu
from jax.sharding import PartitionSpec as P

MESH = pl.DeviceIdType.MESH
CORES = 2
BF16, F32 = jnp.bfloat16, jnp.float32

ORDER = ((-1, 0), (0, 1), (0, -1), (0, 0), (-1, 1), (1, 0), (1, -1), (1, 1), (0, 2), (-1, -1), (2, 0), (2, 1), (2, -1), (2, 2), (1, 2), (-1, 2))
EVENTS = {
    0: ((-1, 0), (0, -1), (1, 0), (0, 1)),
    2: ((2, 0), (-1, 1)),
    4: ((0, 2), (1, -1), (-1, -1)),
    5: ((1, 1),),
    6: ((2, -1),),
    9: ((2, 1),),
    10: ((1, 2),),
    12: ((2, 2), (-1, 2)),
}
FLIP = 1
RELAY = {15: (11,)}
TAIL_RELAY = (13, 10, 8, 14), (15, 12)

PIECE = 512 * 1024
LINES = (2, 0, -1, 1)
PART = {2: 0, 1: 1, -1: 2, 0: 3}

NN = (((1,), (0,)), ((), ()))
NT = (((1,), (1,)), ((), ()))
TN = (((0,), (0,)), ((), ()))


def dot(a, b, dims):
    return lax.dot_general(a, b, dims, preferred_element_type=F32)


def lut(k, vals):
    out = vals[0]
    for i, v in enumerate(vals):
        if i:
            out = jnp.where(k == i, v, out)
    return out


def kernel(n_dev, side, gy_ref, ids_ref, slots_ref, gates_ref, pc_ref, y_ref, x_ref, hg_ref, hu_ref, wg_ref, wu_ref, wd_ref,
           gx_ref, gg_ref, gwg_ref, gwu_ref, gwd_ref,
           tokens, stab, tabs, mids, mslots, rbuf, ret, relay, part, hop_in, fin, wgu, wd, xb, hgb, hub,
           tok_sem, tab_sem, meta_sem, ret_sem, relay_sem, hop_sem, fin_sem,
           ag_send, pair_send, tab_send, meta_send, ret_send, relay_send, part_send, load_sem, w_sem, round_sem):
    me = lax.axis_index("ep")
    core = me % CORES
    mx = (me // CORES) % side
    my = me // (CORES * side)
    turn = 1 - core if FLIP else core
    my_a = (1 - turn) * mx + turn * my
    my_b = (1 - turn) * my + turn * mx
    tok_dev, model_dim = gy_ref.shape
    top_k = ids_ref.shape[0]
    ffn = wg_ref.shape[1]
    cap = rbuf.shape[1]
    half = tok_dev // 2
    n_chip = side * side
    crow = CORES * cap
    partner = me + 1 - 2 * core

    def wrap(v):
        return (v + 2 * side) % side

    def device(x, y, c):
        return (wrap(y) * side + wrap(x)) * CORES + c

    def plane(a, b):
        return device(mx + (1 - turn) * a + turn * b, my + turn * a + (1 - turn) * b, core)

    def remote(src, dst, send_sem, recv_sem, to):
        return pltpu.make_async_remote_copy(src_ref=src, dst_ref=dst, send_sem=send_sem, recv_sem=recv_sem, device_id={"ep": to}, device_id_type=MESH)

    def landed(ref, sem):
        pltpu.make_async_copy(ref, ref, sem).wait()

    peers = [partner] + [device(mx + dx, my + dy, c) for dx, dy in ((1, 0), (-1, 0), (0, 1), (0, -1)) for c in range(CORES)]

    def tell(sem):
        for to in peers:
            pl.semaphore_signal(sem, inc=1, device_id={"ep": to}, device_id_type=MESH)

    barrier = pltpu.get_barrier_semaphore()
    tell(barrier)

    wcopies = [
        pltpu.make_async_copy(wd_ref, wd, w_sem.at[0]),
        pltpu.make_async_copy(wg_ref, wgu.at[:, pl.ds(0, ffn)], w_sem.at[1]),
        pltpu.make_async_copy(wu_ref, wgu.at[:, pl.ds(ffn, ffn)], w_sem.at[2]),
    ]
    for c in wcopies:
        c.start()
    own_copies = [
        pltpu.make_async_copy(gy_ref, tokens.at[me], tok_sem.at[me, 0]),
        pltpu.make_async_copy(ids_ref, mids.at[my_b], meta_sem.at[my_b, 0]),
        pltpu.make_async_copy(slots_ref, mslots.at[my_b], meta_sem.at[my_b, 1]),
    ]
    for c in own_copies:
        c.start()

    def offset(k, axis):
        return lut(k, [o[axis] for o in ORDER])

    def chip_at(k):
        return wrap(my + offset(k, 1)) * side + wrap(mx + offset(k, 0))

    def loads(k):
        q = chip_at(k)
        slot = k % 2
        rows = pl.ds(pl.multiple_of(q * crow, crow), crow)
        return [
            pltpu.make_async_copy(x_ref.at[rows], xb.at[slot], load_sem.at[0, slot]),
            pltpu.make_async_copy(hg_ref.at[rows], hgb.at[slot], load_sem.at[1, slot]),
            pltpu.make_async_copy(hu_ref.at[rows], hub.at[slot], load_sem.at[2, slot]),
        ]

    for c in loads(0):
        c.start()

    ids = ids_ref[...]
    slots = slots_ref[...]
    gates = gates_ref[...]

    def table(e, carry):
        hit = ids == e
        slot = jnp.max(jnp.where(hit, slots, -1), axis=0, keepdims=True)
        slot = jnp.where(slot < pc_ref[0, e], slot, -1)
        gate = jnp.sum(jnp.where(hit, gates, 0.0), axis=0, keepdims=True)
        stab[e] = jnp.concatenate([slot.astype(F32), gate], axis=0)
        return carry

    lax.fori_loop(0, n_dev, table, 0)
    gwg_ref[...] = jnp.zeros_like(gwg_ref)
    gwu_ref[...] = jnp.zeros_like(gwu_ref)
    gwd_ref[...] = jnp.zeros_like(gwd_ref)
    pl.semaphore_wait(barrier, len(peers))
    own_copies[0].wait()

    sends, pairs = [], []

    def block(src, h):
        return tokens.at[src, pl.ds(h * half, half)]

    def forward_msg(n, i, j, h, a, b):
        src = plane(i, j)
        return remote(block(src, h), block(src, h), ag_send.at[n], tok_sem.at[src, h], plane(a, b))

    def forward(*what):
        what = (len(sends), *what)
        sends.append(what)
        forward_msg(*what).start()

    def pair_msg(n, i, j):
        src = plane(i, j)
        return remote(tokens.at[src], tokens.at[src], pair_send.at[n], tok_sem.at[src, 0], partner)

    def to_partner(i, j):
        what = (len(pairs), i, j)
        pairs.append(what)
        pair_msg(*what).start()

    def arrived(src, h):
        landed(block(src, h), tok_sem.at[src, h])

    to_partner(0, 0)

    def tab_msg(i):
        to = (me + 1 + i) % n_dev
        return remote(stab.at[to], tabs.at[me], tab_send.at[i], tab_sem.at[me], to)

    def tab_start(i, carry):
        tab_msg(i).start()
        return carry

    for n in range(2):
        for a, b, h in ((1, 0, n), (-1, 0, 1 - n), (0, 1, n), (0, -1, 1 - n)):
            forward(0, 0, h, a, b)

    for n in range(side - 1):
        tell(round_sem.at[n])
        pl.semaphore_wait(round_sem.at[n], len(peers))
    lax.fori_loop(0, n_dev - 1, tab_start, 0)
    tab_copy = pltpu.make_async_copy(stab.at[me], tabs.at[me], tab_sem.at[me])
    tab_copy.start()
    def meta_msgs():
        out = []
        for n, j in enumerate((1, -1, 2)):
            out.append(remote(ids_ref, mids.at[my_b], meta_send.at[n, 0], meta_sem.at[my_b, 0], plane(0, j)))
            out.append(remote(slots_ref, mslots.at[my_b], meta_send.at[n, 1], meta_sem.at[my_b, 1], plane(0, j)))
        return out

    for c in meta_msgs():
        c.start()

    def event(i, j):
        src = plane(i, j)
        first = 1 if (i == 1 and j == 0) or j == 1 else 0
        for n, h in enumerate((first, 1 - first)):
            arrived(src, h)
            if j == 0:
                if n == 0 and abs(i) == 1:
                    forward(i, j, h, -i, 0)
                forward(i, j, h, 0, 1)
                forward(i, j, h, 0, -1)
            elif n == 0 and abs(j) == 1:
                forward(i, j, h, 0, -j)
        to_partner(i, j)

    def r_block(k, cc):
        axis = 1 - cc if FLIP else cc
        i, j = offset(k, axis), offset(k, 1 - axis)
        a, b = (mx, my) if axis == 0 else (my, mx)
        hb = wrap(b + j)
        home = chip_at(k) * CORES + cc
        step = jnp.where(i == 2, 1 - 2 * core, i)
        to = device(mx + step, my, cc) if axis == 0 else device(mx, my + step, cc)
        slot = (hb * side + a) * CORES + core
        hop = hb * 2 + core
        is_local = jnp.logical_and(i == 0, core == cc)
        return i, home, to, slot, hop, is_local

    def send_chunk(k):
        for cc in range(CORES):
            i, home, to, slot, hop, is_local = r_block(k, cc)

            @pl.when(is_local)
            def _():
                pltpu.make_async_copy(rbuf.at[home], ret.at[slot], ret_sem.at[slot]).start()

            @pl.when(i == 2)
            def _():
                remote(rbuf.at[home], relay.at[hop], ret_send.at[home], relay_sem.at[hop], to).start()

            @pl.when(jnp.logical_and(i != 2, jnp.logical_not(is_local)))
            def _():
                remote(rbuf.at[home], ret.at[slot], ret_send.at[home], ret_sem.at[slot], to).start()

    def relay_msg(j, way):
        hb = wrap(my_b + j)
        slot = (hb * side + wrap(my_a - 1 + 2 * way)) * CORES + way
        hop = hb * 2 + way
        return hop, remote(relay.at[hop], ret.at[slot], relay_send.at[hop], ret_sem.at[slot], plane(1 - 2 * way, 0))

    def hand_on(k):
        dx, dy = ORDER[k]
        i = jnp.where(turn == 0, dx, dy)
        j = jnp.where(turn == 0, dy, dx)

        @pl.when(i == 2)
        def _():
            for way in range(2):
                hop, msg = relay_msg(j, way)
                landed(relay.at[hop], relay_sem.at[hop])
                msg.start()

    slot_iota = lax.broadcasted_iota(jnp.int32, (cap, tok_dev), 0)
    slot_iota_f = slot_iota.astype(F32)
    for c in wcopies:
        c.wait()

    def chunk(k, carry):
        for at, evs in EVENTS.items():
            @pl.when(k == at)
            def _(evs=evs):
                for i, j in evs:
                    event(i, j)

        @pl.when(k > 0)
        def _():
            send_chunk(k - 1)

        for at, steps in RELAY.items():
            @pl.when(k == at)
            def _(steps=steps):
                for n in steps:
                    hand_on(n)

        slot = k % 2
        for c in loads(k):
            c.wait()

        @pl.when(k + 1 < n_chip)
        def _():
            for c in loads(k + 1):
                c.start()

        q = chip_at(k)
        landed(tokens.at[q * CORES + 1 - core], tok_sem.at[q * CORES + 1 - core, 0])

        d_parts = []
        for cc in range(CORES):
            home = q * CORES + cc
            landed(tabs.at[home], tab_sem.at[home])
            tab = tabs[home]
            pick = tab[0:1, :] == slot_iota_f
            gate = jnp.sum(jnp.where(pick, tab[1:2, :], 0.0), axis=1, keepdims=True)
            rows = dot(pick.astype(F32).astype(BF16), tokens[home], NN)
            d_parts.append((gate * rows).astype(BF16))
        d = jnp.concatenate(d_parts, axis=0)
        da = dot(d, wd[...], NT).astype(BF16).astype(F32)
        h1 = hgb[slot].astype(F32)
        h3 = hub[slot].astype(F32)
        g = jax.nn.sigmoid(h1)
        s = h1 * g
        act = (s * h3).astype(BF16)
        dh1 = (da * h3 * g * (1.0 + h1 * (1.0 - g))).astype(BF16)
        dh3 = (da * s).astype(BF16)
        dh = jnp.concatenate([dh1, dh3], axis=1)
        r = dot(dh, wgu[...], NT).astype(BF16)
        for cc in range(CORES):
            rbuf[q * CORES + cc] = r[cc * cap:(cc + 1) * cap]
        x = xb[slot]
        gwg_ref[...] += dot(x, dh1, TN)
        gwu_ref[...] += dot(x, dh3, TN)
        gwd_ref[...] += dot(act, d, TN)
        return carry

    lax.fori_loop(0, n_chip, chunk, 0)
    send_chunk(jnp.int32(n_chip - 1))

    n_run = crow // top_k
    n_step = tok_dev // n_run

    def y_load(m):
        return pltpu.make_async_copy(y_ref.at[pl.ds(pl.multiple_of(m * crow, crow), crow)], xb.at[m % 2], load_sem.at[0, m % 2])

    y_load(0).start()
    lane = lax.broadcasted_iota(jnp.int32, (crow, tok_dev), 1)
    token_of = lax.broadcasted_iota(jnp.int32, (crow, tok_dev), 0) // top_k
    gg_ref[...] = jnp.zeros_like(gg_ref)

    def gate_grad(m, carry):
        y_load(m).wait()

        @pl.when(m + 1 < n_step)
        def _():
            y_load(m + 1).start()

        gy = tokens[me, pl.ds(pl.multiple_of(m * n_run, n_run), n_run), :].astype(F32)
        gy = jnp.broadcast_to(gy[:, None, :], (n_run, top_k, model_dim)).reshape(crow, model_dim)
        col = jnp.sum(xb[m % 2].astype(F32) * gy, axis=1, keepdims=True)
        put = jnp.where(lane == token_of + m * n_run, col, 0.0)
        gg_ref[...] += jnp.sum(put.reshape(n_run, top_k, tok_dev), axis=0)
        return carry

    for k in TAIL_RELAY[0]:
        hand_on(k)
    lax.fori_loop(0, n_step, gate_grad, 0)
    for k in TAIL_RELAY[1]:
        hand_on(k)

    def add_rows(n, carry):
        j = lut(n, LINES)
        hb = wrap(my_b + j)
        landed(mids.at[hb], meta_sem.at[hb, 0])
        landed(mslots.at[hb], meta_sem.at[hb, 1])
        h_ids = mids[hb]
        h_slots = mslots[hb]
        picks = []
        for sa in range(side):
            for ce in range(CORES):
                slot = (hb * side + sa) * CORES + ce
                landed(ret.at[slot], ret_sem.at[slot])
                x = (1 - turn) * sa + turn * my_b
                y = (1 - turn) * my_b + turn * sa
                row = jnp.max(jnp.where(h_ids == (y * side + x) * CORES + ce, h_slots, -1), axis=0, keepdims=True)
                picks.append((row == slot_iota).astype(F32).astype(BF16))
        pick = jnp.concatenate(picks, axis=0)
        rows = ret[pl.ds(hb * side * CORES, side * CORES)].reshape(side * CORES * cap, model_dim)
        part[lut(n, [PART[v] for v in LINES])] = dot(pick, rows, TN)

        @pl.when(n == 1)
        def _():
            for c in hop_msgs():
                c.start()

        return carry

    def hop_msgs():
        return [
            remote(part.at[0, pl.ds(0, half)], hop_in.at[0], part_send.at[0], hop_sem.at[0], plane(0, 1)),
            remote(part.at[0, pl.ds(half, half)], hop_in.at[1], part_send.at[1], hop_sem.at[1], plane(0, -1)),
        ]

    def fin_msgs():
        return [
            remote(part.at[1 + n, pl.ds(h * half, half)], fin.at[n, pl.ds(h * half, half)], part_send.at[2 + 2 * n + h], fin_sem.at[n, h], plane(0, 1 - 2 * n))
            for n in range(2)
            for h in range(2)
        ]

    fins = fin_msgs()
    lax.fori_loop(0, len(LINES), add_rows, 0)
    fins[2].start()
    for what in sends:
        forward_msg(*what).wait_send()
    for what in pairs:
        pair_msg(*what).wait_send()
    fins[1].start()
    landed(hop_in.at[0], hop_sem.at[0])
    part[1, pl.ds(0, half)] += hop_in[0]
    landed(hop_in.at[1], hop_sem.at[1])
    part[2, pl.ds(half, half)] += hop_in[1]

    def tab_done(i, carry):
        tab_msg(i).wait_send()
        return carry

    lax.fori_loop(0, n_dev - 1, tab_done, 0)
    fins[0].start()
    fins[3].start()
    for c in meta_msgs() + hop_msgs():
        c.wait_send()

    def ret_done(k, carry):
        for cc in range(CORES):
            i, home, to, slot, hop, is_local = r_block(k, cc)

            @pl.when(jnp.logical_not(is_local))
            def _():
                remote(rbuf.at[home], ret.at[slot], ret_send.at[home], ret_sem.at[slot], to).wait_send()
        return carry

    lax.fori_loop(0, n_chip, ret_done, 0)
    for j in (0, 1, -1, 2):
        for way in range(2):
            relay_msg(j, way)[1].wait_send()
    for n, h in ((0, 1), (1, 0), (0, 0), (1, 1)):
        rows = pl.ds(h * half, half)
        landed(fin.at[n, rows], fin_sem.at[n, h])
        if (n, h) == (0, 0):
            gx_ref[rows] = (part[3, rows] + fin[0, rows] + fin[1, rows]).astype(gx_ref.dtype)
    rows = pl.ds(half, half)
    gx_ref[rows] = (part[3, rows] + fin[0, rows] + fin[1, rows]).astype(gx_ref.dtype)
    for c in fins:
        c.wait_send()


def write_out(*refs):
    n = len(refs) // 2
    sems = refs[-1]
    copies = []
    for i in range(n):
        src, dst = refs[i], refs[n + i]
        rows = src.shape[0]
        step = max(8, min(rows, PIECE // (src.shape[1] * src.dtype.itemsize)))
        for r in range(0, rows, step):
            copies.append(pltpu.make_async_copy(src.at[pl.ds(r, step)], dst.at[pl.ds(r, step)], sems.at[len(copies)]))
    for c in copies:
        c.start()
    for c in copies:
        c.wait()


def solution(mesh):
    n_dev = mesh.shape["ep"]
    side = math.isqrt(n_dev // CORES)
    rows_spec = P(("dp", "ep"), None)
    cube_spec = P(("dp", "ep"), None, None)
    weight_spec = P("ep", None, None)

    def local_step(grad_y, gate_vals, topk_idx, slot_ids, pair_counts, y_routed, x_disp, h_gate, h_up, w_gate, w_up, w_down):
        assert w_gate.shape[0] == 1
        assert side * side * CORES == n_dev and len(ORDER) == side * side
        cap = x_disp.shape[1] // n_dev
        tok_dev, model_dim = grad_y.shape
        ffn = w_gate.shape[2]
        crow = CORES * cap
        n_chip = side * side
        top_k = topk_idx.shape[1]
        vmem = pl.BlockSpec(memory_space=pltpu.VMEM)
        smem = pl.BlockSpec(memory_space=pltpu.SMEM)
        anym = pl.BlockSpec(memory_space=pl.ANY)
        dma = pltpu.SemaphoreType.DMA
        results = pl.pallas_call(
            functools.partial(kernel, n_dev, side),
            out_shape=(
                pltpu.VMEM((tok_dev, model_dim), BF16),
                pltpu.VMEM((top_k, tok_dev), F32),
                pltpu.VMEM((model_dim, ffn), F32),
                pltpu.VMEM((model_dim, ffn), F32),
                pltpu.VMEM((ffn, model_dim), F32),
            ),
            in_specs=[anym, vmem, vmem, vmem, smem] + [anym] * 7,
            out_specs=(vmem,) * 5,
            scratch_shapes=[
                pltpu.VMEM((n_dev, tok_dev, model_dim), BF16),
                pltpu.VMEM((n_dev, 2, tok_dev), F32),
                pltpu.VMEM((n_dev, 2, tok_dev), F32),
                pltpu.VMEM((side, top_k, tok_dev), jnp.int32),
                pltpu.VMEM((side, top_k, tok_dev), jnp.int32),
                pltpu.VMEM((n_dev, cap, model_dim), BF16),
                pltpu.VMEM((n_dev, cap, model_dim), BF16),
                pltpu.VMEM((2 * side, cap, model_dim), BF16),
                pltpu.VMEM((4, tok_dev, model_dim), F32),
                pltpu.VMEM((2, tok_dev // 2, model_dim), F32),
                pltpu.VMEM((2, tok_dev, model_dim), F32),
                pltpu.VMEM((model_dim, 2 * ffn), BF16),
                pltpu.VMEM((ffn, model_dim), BF16),
                pltpu.VMEM((2, crow, model_dim), BF16),
                pltpu.VMEM((2, crow, ffn), BF16),
                pltpu.VMEM((2, crow, ffn), BF16),
                dma((n_dev, 2)),
                dma((n_dev,)),
                dma((side, 2)),
                dma((n_dev,)),
                dma((2 * side,)),
                dma((2,)),
                dma((2, 2)),
                dma((64,)),
                dma((n_chip,)),
                dma((n_dev,)),
                dma((3, 2)),
                dma((n_dev,)),
                dma((2 * side,)),
                dma((6,)),
                dma((3, 2)),
                dma((3,)),
                pltpu.SemaphoreType.REGULAR((side - 1,)),
            ],
            compiler_params=pltpu.CompilerParams(collective_id=0, has_side_effects=True, vmem_limit_bytes=58720256),
            name="moe_bwd",
        )(grad_y, topk_idx.T, slot_ids.T, gate_vals.T, pair_counts, y_routed.reshape(tok_dev * top_k, model_dim), x_disp[0], h_gate[0], h_up[0], w_gate[0], w_up[0], w_down[0])
        gx, gg, gwg, gwu, gwd = pl.pallas_call(
            write_out,
            out_shape=tuple(jax.ShapeDtypeStruct(r.shape, r.dtype) for r in results),
            in_specs=[anym] * len(results),
            out_specs=(anym,) * len(results),
            scratch_shapes=[dma((32,))],
            compiler_params=pltpu.CompilerParams(vmem_limit_bytes=1048576),
            name="write_out",
        )(*results)
        return gx, gg.T, gwg[None], gwu[None], gwd[None]

    return jax.shard_map(local_step, mesh=mesh, in_specs=(rows_spec, rows_spec, rows_spec, rows_spec, rows_spec, cube_spec, cube_spec, cube_spec, cube_spec, weight_spec, weight_spec, weight_spec), out_specs=(rows_spec, rows_spec, cube_spec, cube_spec, cube_spec), check_vma=False)
```

```python
import functools
import math

import jax
import jax.numpy as jnp
from jax import lax
from jax.experimental import pallas as pl
from jax.experimental.pallas import tpu as pltpu
from jax.sharding import PartitionSpec as P

MESH = pl.DeviceIdType.MESH
CORES = 2
BF16, F32 = jnp.bfloat16, jnp.float32

ORDER = ((-1, 0), (0, 1), (0, -1), (0, 0), (-1, 1), (1, 0), (1, -1), (1, 1), (0, 2), (-1, -1), (2, 0), (2, 1), (2, -1), (2, 2), (1, 2), (-1, 2))
EVENTS = {
    0: ((-1, 0), (0, -1), (1, 0), (0, 1)),
    2: ((2, 0), (-1, 1)),
    4: ((0, 2), (1, -1), (-1, -1)),
    5: ((1, 1),),
    6: ((2, -1),),
    9: ((2, 1),),
    10: ((1, 2),),
    12: ((2, 2), (-1, 2)),
}
FLIP = 1
RELAY = {15: (11,)}
TAIL_RELAY = (13, 10, 8, 14), (15, 12)

LINES = (2, 0, -1, 1)
PART = {2: 0, 1: 1, -1: 2, 0: 3}

NN = (((1,), (0,)), ((), ()))
NT = (((1,), (1,)), ((), ()))
TN = (((0,), (0,)), ((), ()))


def dot(a, b, dims):
    return lax.dot_general(a, b, dims, preferred_element_type=F32)


def lut(k, vals):
    out = vals[0]
    for i, v in enumerate(vals):
        if i:
            out = jnp.where(k == i, v, out)
    return out


def kernel(n_dev, side, gy_ref, ids_ref, slots_ref, gates_ref, pc_ref, y_ref, x_ref, hg_ref, hu_ref, wg_ref, wu_ref, wd_ref,
           gx_ref, gg_ref, gwg_ref, gwu_ref, gwd_ref,
           tokens, stab, tabs, mids, mslots, rbuf, ret, relay, part, hop_in, fin, wgu, wd, xb, hgb, hub,
           tok_sem, tab_sem, meta_sem, ret_sem, relay_sem, hop_sem, fin_sem,
           ag_send, pair_send, tab_send, meta_send, ret_send, relay_send, part_send, load_sem, w_sem, round_sem, gates, counts, in_sem):
    me = lax.axis_index("ep")
    core = me % CORES
    mx = (me // CORES) % side
    my = me // (CORES * side)
    turn = 1 - core if FLIP else core
    my_a = (1 - turn) * mx + turn * my
    my_b = (1 - turn) * my + turn * mx
    tok_dev, model_dim = gy_ref.shape
    top_k = ids_ref.shape[0]
    ffn = wg_ref.shape[1]
    cap = rbuf.shape[1]
    half = tok_dev // 2
    n_chip = side * side
    crow = CORES * cap
    partner = me + 1 - 2 * core

    def wrap(v):
        return (v + 2 * side) % side

    def device(x, y, c):
        return (wrap(y) * side + wrap(x)) * CORES + c

    def plane(a, b):
        return device(mx + (1 - turn) * a + turn * b, my + turn * a + (1 - turn) * b, core)

    def remote(src, dst, send_sem, recv_sem, to):
        return pltpu.make_async_remote_copy(src_ref=src, dst_ref=dst, send_sem=send_sem, recv_sem=recv_sem, device_id={"ep": to}, device_id_type=MESH)

    def landed(ref, sem):
        pltpu.make_async_copy(ref, ref, sem).wait()

    peers = [partner] + [device(mx + dx, my + dy, c) for dx, dy in ((1, 0), (-1, 0), (0, 1), (0, -1)) for c in range(CORES)]

    def tell(sem):
        for to in peers:
            pl.semaphore_signal(sem, inc=1, device_id={"ep": to}, device_id_type=MESH)

    barrier = pltpu.get_barrier_semaphore()
    tell(barrier)

    own_copies = [
        pltpu.make_async_copy(gy_ref, tokens.at[me], in_sem.at[0]),
        pltpu.make_async_copy(ids_ref, mids.at[my_b], in_sem.at[1]),
        pltpu.make_async_copy(slots_ref, mslots.at[my_b], in_sem.at[2]),
        pltpu.make_async_copy(gates_ref, gates, in_sem.at[3]),
        pltpu.make_async_copy(pc_ref, counts, in_sem.at[4]),
    ]
    for c in own_copies:
        c.start()
    wcopies = [
        pltpu.make_async_copy(wd_ref, wd, w_sem.at[0]),
        pltpu.make_async_copy(wg_ref, wgu.at[:, pl.ds(0, ffn)], w_sem.at[1]),
        pltpu.make_async_copy(wu_ref, wgu.at[:, pl.ds(ffn, ffn)], w_sem.at[2]),
    ]
    for c in wcopies:
        c.start()

    def offset(k, axis):
        return lut(k, [o[axis] for o in ORDER])

    def chip_at(k):
        return wrap(my + offset(k, 1)) * side + wrap(mx + offset(k, 0))

    def loads(k):
        q = chip_at(k)
        slot = k % 2
        rows = pl.ds(pl.multiple_of(q * crow, crow), crow)
        return [
            pltpu.make_async_copy(x_ref.at[rows], xb.at[slot], load_sem.at[0, slot]),
            pltpu.make_async_copy(hg_ref.at[rows], hgb.at[slot], load_sem.at[1, slot]),
            pltpu.make_async_copy(hu_ref.at[rows], hub.at[slot], load_sem.at[2, slot]),
        ]

    pl.semaphore_wait(barrier, len(peers))
    own_copies[0].wait()

    sends, pairs = [], []

    def block(src, h):
        return tokens.at[src, pl.ds(h * half, half)]

    def forward_msg(n, i, j, h, a, b):
        src = plane(i, j)
        return remote(block(src, h), block(src, h), ag_send.at[n], tok_sem.at[src, h], plane(a, b))

    def forward(*what):
        what = (len(sends), *what)
        sends.append(what)
        forward_msg(*what).start()

    def pair_msg(n, i, j):
        src = plane(i, j)
        return remote(tokens.at[src], tokens.at[src], pair_send.at[n], tok_sem.at[src, 0], partner)

    def to_partner(i, j):
        what = (len(pairs), i, j)
        pairs.append(what)
        pair_msg(*what).start()

    def arrived(src, h):
        landed(block(src, h), tok_sem.at[src, h])

    to_partner(0, 0)

    def tab_msg(i):
        to = (me + 1 + i) % n_dev
        return remote(stab.at[to], tabs.at[me], tab_send.at[i], tab_sem.at[me], to)

    def tab_start(i, carry):
        tab_msg(i).start()
        return carry

    for n in range(2):
        for a, b, h in ((1, 0, n), (-1, 0, 1 - n), (0, 1, n), (0, -1, 1 - n)):
            forward(0, 0, h, a, b)

    tell(round_sem.at[0])
    for c in loads(0):
        c.start()

    for c in own_copies[1:]:
        c.wait()
    ids = mids[my_b]
    slots = mslots[my_b]

    def table(e, carry):
        hit = ids == e
        slot = jnp.max(jnp.where(hit, slots, -1), axis=0, keepdims=True)
        slot = jnp.where(slot < counts[0, e], slot, -1)
        gate = jnp.sum(jnp.where(hit, gates[...], 0.0), axis=0, keepdims=True)
        stab[e] = jnp.concatenate([slot.astype(F32), gate], axis=0)
        return carry

    lax.fori_loop(0, n_dev, table, 0)
    gwg_ref[...] = jnp.zeros_like(gwg_ref)
    gwu_ref[...] = jnp.zeros_like(gwu_ref)
    gwd_ref[...] = jnp.zeros_like(gwd_ref)

    for n in range(side - 1):
        if n:
            tell(round_sem.at[n])
        pl.semaphore_wait(round_sem.at[n], len(peers))
    lax.fori_loop(0, n_dev - 1, tab_start, 0)
    tab_copy = pltpu.make_async_copy(stab.at[me], tabs.at[me], tab_sem.at[me])
    tab_copy.start()
    def meta_msgs():
        out = []
        for n, j in enumerate((1, -1, 2)):
            out.append(remote(mids.at[my_b], mids.at[my_b], meta_send.at[n, 0], meta_sem.at[my_b, 0], plane(0, j)))
            out.append(remote(mslots.at[my_b], mslots.at[my_b], meta_send.at[n, 1], meta_sem.at[my_b, 1], plane(0, j)))
        return out

    for c in meta_msgs():
        c.start()

    def event(i, j):
        src = plane(i, j)
        first = 1 if (i == 1 and j == 0) or j == 1 else 0
        for n, h in enumerate((first, 1 - first)):
            arrived(src, h)
            if j == 0:
                if n == 0 and abs(i) == 1:
                    forward(i, j, h, -i, 0)
                forward(i, j, h, 0, 1)
                forward(i, j, h, 0, -1)
            elif n == 0 and abs(j) == 1:
                forward(i, j, h, 0, -j)
        to_partner(i, j)

    def r_block(k, cc):
        axis = 1 - cc if FLIP else cc
        i, j = offset(k, axis), offset(k, 1 - axis)
        a, b = (mx, my) if axis == 0 else (my, mx)
        hb = wrap(b + j)
        home = chip_at(k) * CORES + cc
        step = jnp.where(i == 2, 1 - 2 * core, i)
        to = device(mx + step, my, cc) if axis == 0 else device(mx, my + step, cc)
        slot = (hb * side + a) * CORES + core
        hop = hb * 2 + core
        is_local = jnp.logical_and(i == 0, core == cc)
        return i, home, to, slot, hop, is_local

    def send_chunk(k):
        for cc in range(CORES):
            i, home, to, slot, hop, is_local = r_block(k, cc)

            @pl.when(is_local)
            def _():
                pltpu.make_async_copy(rbuf.at[home], ret.at[slot], ret_sem.at[slot]).start()

            @pl.when(i == 2)
            def _():
                remote(rbuf.at[home], relay.at[hop], ret_send.at[home], relay_sem.at[hop], to).start()

            @pl.when(jnp.logical_and(i != 2, jnp.logical_not(is_local)))
            def _():
                remote(rbuf.at[home], ret.at[slot], ret_send.at[home], ret_sem.at[slot], to).start()

    def relay_msg(j, way):
        hb = wrap(my_b + j)
        slot = (hb * side + wrap(my_a - 1 + 2 * way)) * CORES + way
        hop = hb * 2 + way
        return hop, remote(relay.at[hop], ret.at[slot], relay_send.at[hop], ret_sem.at[slot], plane(1 - 2 * way, 0))

    def hand_on(k):
        dx, dy = ORDER[k]
        i = jnp.where(turn == 0, dx, dy)
        j = jnp.where(turn == 0, dy, dx)

        @pl.when(i == 2)
        def _():
            for way in range(2):
                hop, msg = relay_msg(j, way)
                landed(relay.at[hop], relay_sem.at[hop])
                msg.start()

    slot_iota = lax.broadcasted_iota(jnp.int32, (cap, tok_dev), 0)
    slot_iota_f = slot_iota.astype(F32)
    for c in wcopies:
        c.wait()

    def chunk(k, carry):
        for at, evs in EVENTS.items():
            @pl.when(k == at)
            def _(evs=evs):
                for i, j in evs:
                    event(i, j)

        @pl.when(k > 0)
        def _():
            send_chunk(k - 1)

        for at, steps in RELAY.items():
            @pl.when(k == at)
            def _(steps=steps):
                for n in steps:
                    hand_on(n)

        slot = k % 2
        for c in loads(k):
            c.wait()

        @pl.when(k + 1 < n_chip)
        def _():
            for c in loads(k + 1):
                c.start()

        q = chip_at(k)
        landed(tokens.at[q * CORES + 1 - core], tok_sem.at[q * CORES + 1 - core, 0])

        d_parts = []
        for cc in range(CORES):
            home = q * CORES + cc
            landed(tabs.at[home], tab_sem.at[home])
            tab = tabs[home]
            pick = tab[0:1, :] == slot_iota_f
            gate = jnp.sum(jnp.where(pick, tab[1:2, :], 0.0), axis=1, keepdims=True)
            rows = dot(pick.astype(F32).astype(BF16), tokens[home], NN)
            d_parts.append((gate * rows).astype(BF16))
        d = jnp.concatenate(d_parts, axis=0)
        da = dot(d, wd[...], NT).astype(BF16).astype(F32)
        h1 = hgb[slot].astype(F32)
        h3 = hub[slot].astype(F32)
        g = jax.nn.sigmoid(h1)
        s = h1 * g
        act = (s * h3).astype(BF16)
        dh1 = (da * h3 * g * (1.0 + h1 * (1.0 - g))).astype(BF16)
        dh3 = (da * s).astype(BF16)
        dh = jnp.concatenate([dh1, dh3], axis=1)
        r = dot(dh, wgu[...], NT).astype(BF16)
        for cc in range(CORES):
            rbuf[q * CORES + cc] = r[cc * cap:(cc + 1) * cap]
        x = xb[slot]
        gwg_ref[...] += dot(x, dh1, TN)
        gwu_ref[...] += dot(x, dh3, TN)
        gwd_ref[...] += dot(act, d, TN)
        return carry

    lax.fori_loop(0, n_chip, chunk, 0)
    send_chunk(jnp.int32(n_chip - 1))

    n_run = crow // top_k
    n_step = tok_dev // n_run

    def y_load(m):
        return pltpu.make_async_copy(y_ref.at[pl.ds(pl.multiple_of(m * crow, crow), crow)], xb.at[m % 2], load_sem.at[0, m % 2])

    y_load(0).start()
    lane = lax.broadcasted_iota(jnp.int32, (crow, tok_dev), 1)
    token_of = lax.broadcasted_iota(jnp.int32, (crow, tok_dev), 0) // top_k
    gg_ref[...] = jnp.zeros_like(gg_ref)

    def gate_grad(m, carry):
        y_load(m).wait()

        @pl.when(m + 1 < n_step)
        def _():
            y_load(m + 1).start()

        gy = tokens[me, pl.ds(pl.multiple_of(m * n_run, n_run), n_run), :].astype(F32)
        gy = jnp.broadcast_to(gy[:, None, :], (n_run, top_k, model_dim)).reshape(crow, model_dim)
        col = jnp.sum(xb[m % 2].astype(F32) * gy, axis=1, keepdims=True)
        put = jnp.where(lane == token_of + m * n_run, col, 0.0)
        gg_ref[...] += jnp.sum(put.reshape(n_run, top_k, tok_dev), axis=0)
        return carry

    for k in TAIL_RELAY[0]:
        hand_on(k)
    lax.fori_loop(0, n_step, gate_grad, 0)
    for k in TAIL_RELAY[1]:
        hand_on(k)

    def add_rows(n, carry):
        j = lut(n, LINES)
        hb = wrap(my_b + j)

        @pl.when(j != 0)
        def _():
            landed(mids.at[hb], meta_sem.at[hb, 0])
            landed(mslots.at[hb], meta_sem.at[hb, 1])

        h_ids = mids[hb]
        h_slots = mslots[hb]
        picks = []
        for sa in range(side):
            for ce in range(CORES):
                slot = (hb * side + sa) * CORES + ce
                landed(ret.at[slot], ret_sem.at[slot])
                x = (1 - turn) * sa + turn * my_b
                y = (1 - turn) * my_b + turn * sa
                row = jnp.max(jnp.where(h_ids == (y * side + x) * CORES + ce, h_slots, -1), axis=0, keepdims=True)
                picks.append((row == slot_iota).astype(F32).astype(BF16))
        pick = jnp.concatenate(picks, axis=0)
        rows = ret[pl.ds(hb * side * CORES, side * CORES)].reshape(side * CORES * cap, model_dim)
        part[lut(n, [PART[v] for v in LINES])] = dot(pick, rows, TN)

        @pl.when(n == 1)
        def _():
            for c in hop_msgs():
                c.start()

        return carry

    def hop_msgs():
        return [
            remote(part.at[0, pl.ds(0, half)], hop_in.at[0], part_send.at[0], hop_sem.at[0], plane(0, 1)),
            remote(part.at[0, pl.ds(half, half)], hop_in.at[1], part_send.at[1], hop_sem.at[1], plane(0, -1)),
        ]

    def fin_msgs():
        return [
            remote(part.at[1 + n, pl.ds(h * half, half)], fin.at[n, pl.ds(h * half, half)], part_send.at[2 + 2 * n + h], fin_sem.at[n, h], plane(0, 1 - 2 * n))
            for n in range(2)
            for h in range(2)
        ]

    fins = fin_msgs()
    lax.fori_loop(0, len(LINES), add_rows, 0)
    fins[2].start()
    for what in sends:
        forward_msg(*what).wait_send()
    for what in pairs:
        pair_msg(*what).wait_send()
    fins[1].start()
    landed(hop_in.at[0], hop_sem.at[0])
    part[1, pl.ds(0, half)] += hop_in[0]
    landed(hop_in.at[1], hop_sem.at[1])
    part[2, pl.ds(half, half)] += hop_in[1]

    def tab_done(i, carry):
        tab_msg(i).wait_send()
        return carry

    lax.fori_loop(0, n_dev - 1, tab_done, 0)
    fins[0].start()
    fins[3].start()
    for c in meta_msgs() + hop_msgs():
        c.wait_send()

    def ret_done(k, carry):
        for cc in range(CORES):
            i, home, to, slot, hop, is_local = r_block(k, cc)

            @pl.when(jnp.logical_not(is_local))
            def _():
                remote(rbuf.at[home], ret.at[slot], ret_send.at[home], ret_sem.at[slot], to).wait_send()
        return carry

    lax.fori_loop(0, n_chip, ret_done, 0)
    for j in (0, 1, -1, 2):
        for way in range(2):
            relay_msg(j, way)[1].wait_send()
    for n, h in ((0, 1), (1, 0), (0, 0), (1, 1)):
        rows = pl.ds(h * half, half)
        landed(fin.at[n, rows], fin_sem.at[n, h])
        if (n, h) == (0, 0):
            gx_ref[rows] = (part[3, rows] + fin[0, rows] + fin[1, rows]).astype(gx_ref.dtype)
    rows = pl.ds(half, half)
    gx_ref[rows] = (part[3, rows] + fin[0, rows] + fin[1, rows]).astype(gx_ref.dtype)
    for c in fins:
        c.wait_send()


def write_out(*refs):
    n = len(refs) // 2
    sems = refs[-1]
    copies = [pltpu.make_async_copy(refs[i], refs[n + i], sems.at[i]) for i in range(n)]
    for c in copies:
        c.start()
    for c in copies:
        c.wait()


def solution(mesh):
    n_dev = mesh.shape["ep"]
    side = math.isqrt(n_dev // CORES)
    rows_spec = P(("dp", "ep"), None)
    cube_spec = P(("dp", "ep"), None, None)
    weight_spec = P("ep", None, None)

    def local_step(grad_y, gate_vals, topk_idx, slot_ids, pair_counts, y_routed, x_disp, h_gate, h_up, w_gate, w_up, w_down):
        assert w_gate.shape[0] == 1
        assert side * side * CORES == n_dev and len(ORDER) == side * side
        cap = x_disp.shape[1] // n_dev
        tok_dev, model_dim = grad_y.shape
        ffn = w_gate.shape[2]
        crow = CORES * cap
        n_chip = side * side
        top_k = topk_idx.shape[1]
        vmem = pl.BlockSpec(memory_space=pltpu.VMEM)
        anym = pl.BlockSpec(memory_space=pl.ANY)
        dma = pltpu.SemaphoreType.DMA
        results = pl.pallas_call(
            functools.partial(kernel, n_dev, side),
            out_shape=(
                pltpu.VMEM((tok_dev, model_dim), BF16),
                pltpu.VMEM((top_k, tok_dev), F32),
                pltpu.VMEM((model_dim, ffn), F32),
                pltpu.VMEM((model_dim, ffn), F32),
                pltpu.VMEM((ffn, model_dim), F32),
            ),
            in_specs=[anym] * 12,
            out_specs=(vmem,) * 5,
            scratch_shapes=[
                pltpu.VMEM((n_dev, tok_dev, model_dim), BF16),
                pltpu.VMEM((n_dev, 2, tok_dev), F32),
                pltpu.VMEM((n_dev, 2, tok_dev), F32),
                pltpu.VMEM((side, top_k, tok_dev), jnp.int32),
                pltpu.VMEM((side, top_k, tok_dev), jnp.int32),
                pltpu.VMEM((n_dev, cap, model_dim), BF16),
                pltpu.VMEM((n_dev, cap, model_dim), BF16),
                pltpu.VMEM((2 * side, cap, model_dim), BF16),
                pltpu.VMEM((4, tok_dev, model_dim), F32),
                pltpu.VMEM((2, tok_dev // 2, model_dim), F32),
                pltpu.VMEM((2, tok_dev, model_dim), F32),
                pltpu.VMEM((model_dim, 2 * ffn), BF16),
                pltpu.VMEM((ffn, model_dim), BF16),
                pltpu.VMEM((2, crow, model_dim), BF16),
                pltpu.VMEM((2, crow, ffn), BF16),
                pltpu.VMEM((2, crow, ffn), BF16),
                dma((n_dev, 2)),
                dma((n_dev,)),
                dma((side, 2)),
                dma((n_dev,)),
                dma((2 * side,)),
                dma((2,)),
                dma((2, 2)),
                dma((64,)),
                dma((n_chip,)),
                dma((n_dev,)),
                dma((3, 2)),
                dma((n_dev,)),
                dma((2 * side,)),
                dma((6,)),
                dma((3, 2)),
                dma((3,)),
                pltpu.SemaphoreType.REGULAR((side - 1,)),
                pltpu.VMEM((top_k, tok_dev), F32),
                pltpu.SMEM(pair_counts.shape, jnp.int32),
                dma((5,)),
            ],
            compiler_params=pltpu.CompilerParams(collective_id=0, has_side_effects=True, vmem_limit_bytes=58720256),
            name="moe_bwd",
        )(grad_y, topk_idx.T, slot_ids.T, gate_vals.T, pair_counts, y_routed.reshape(tok_dev * top_k, model_dim), x_disp[0], h_gate[0], h_up[0], w_gate[0], w_up[0], w_down[0])
        gx, gg, gwg, gwu, gwd = pl.pallas_call(
            write_out,
            out_shape=tuple(jax.ShapeDtypeStruct(r.shape, r.dtype) for r in results),
            in_specs=[anym] * len(results),
            out_specs=(anym,) * len(results),
            scratch_shapes=[dma((len(results),))],
            compiler_params=pltpu.CompilerParams(vmem_limit_bytes=1048576),
            name="write_out",
        )(*results)
        return gx, gg.T, gwg[None], gwu[None], gwd[None]

    return jax.shard_map(local_step, mesh=mesh, in_specs=(rows_spec, rows_spec, rows_spec, rows_spec, rows_spec, cube_spec, cube_spec, cube_spec, cube_spec, weight_spec, weight_spec, weight_spec), out_specs=(rows_spec, rows_spec, cube_spec, cube_spec, cube_spec), check_vma=False)
```

```python
import functools
import math

import jax
import jax.numpy as jnp
from jax import lax
from jax.experimental import pallas as pl
from jax.experimental.pallas import tpu as pltpu
from jax.sharding import PartitionSpec as P

MESH = pl.DeviceIdType.MESH
CORES = 2
BF16, F32 = jnp.bfloat16, jnp.float32

ORDER = ((0, 0), (-1, 0), (0, 1), (1, 0), (0, -1), (1, -1), (-1, 1), (1, 1), (0, 2), (2, 0), (-1, 2), (2, -1), (2, 1), (-1, -1), (2, 2), (1, 2))
EVENTS = {
    0: ((-1, 0), (0, 1), (1, 0)),
    1: ((0, -1),),
    2: ((1, -1), (-1, -1), (2, 0)),
    4: ((1, 1), (-1, 1)),
    6: ((2, -1),),
    7: ((0, 2),),
    8: ((2, 1),),
    9: ((-1, 2),),
    10: ((1, 2),),
    13: ((2, 2),),
}
FLIP = 1
RELAY = {14: (9,), 15: (11, 10)}
TAIL_RELAY = (14, 8), (12, 15)

LINES = (-1, 2, 1, 0)
PART = {2: 0, 1: 1, -1: 2, 0: 3}

NN = (((1,), (0,)), ((), ()))
NT = (((1,), (1,)), ((), ()))
TN = (((0,), (0,)), ((), ()))


def dot(a, b, dims):
    return lax.dot_general(a, b, dims, preferred_element_type=F32)


def lut(k, vals):
    out = vals[0]
    for i, v in enumerate(vals):
        if i:
            out = jnp.where(k == i, v, out)
    return out


def kernel(n_dev, side, gy_ref, ids_ref, slots_ref, gates_ref, pc_ref, y_ref, x_ref, hg_ref, hu_ref, wg_ref, wu_ref, wd_ref,
           gx_ref, gg_ref, gwg_ref, gwu_ref, gwd_ref,
           tokens, stab, tabs, mids, mslots, rbuf, ret, relay, part, hop_in, fin, wgu, wd, xb, hgb, hub,
           tok_sem, tab_sem, meta_sem, ret_sem, relay_sem, hop_sem, fin_sem,
           ag_send, pair_send, tab_send, meta_send, ret_send, relay_send, part_send, load_sem, w_sem, round_sem, gates, counts, in_sem):
    me = lax.axis_index("ep")
    core = me % CORES
    mx = (me // CORES) % side
    my = me // (CORES * side)
    turn = 1 - core if FLIP else core
    my_a = (1 - turn) * mx + turn * my
    my_b = (1 - turn) * my + turn * mx
    tok_dev, model_dim = gy_ref.shape
    top_k = ids_ref.shape[0]
    ffn = wg_ref.shape[1]
    cap = rbuf.shape[1]
    half = tok_dev // 2
    n_chip = side * side
    crow = CORES * cap
    partner = me + 1 - 2 * core

    def wrap(v):
        return (v + 2 * side) % side

    def device(x, y, c):
        return (wrap(y) * side + wrap(x)) * CORES + c

    def plane(a, b):
        return device(mx + (1 - turn) * a + turn * b, my + turn * a + (1 - turn) * b, core)

    def remote(src, dst, send_sem, recv_sem, to):
        return pltpu.make_async_remote_copy(src_ref=src, dst_ref=dst, send_sem=send_sem, recv_sem=recv_sem, device_id={"ep": to}, device_id_type=MESH)

    def landed(ref, sem):
        pltpu.make_async_copy(ref, ref, sem).wait()

    peers = [partner] + [device(mx + dx, my + dy, c) for dx, dy in ((1, 0), (-1, 0), (0, 1), (0, -1)) for c in range(CORES)]

    def tell(sem):
        for to in peers:
            pl.semaphore_signal(sem, inc=1, device_id={"ep": to}, device_id_type=MESH)

    barrier = pltpu.get_barrier_semaphore()
    tell(barrier)

    own_copies = [
        pltpu.make_async_copy(gy_ref, tokens.at[me], in_sem.at[0]),
        pltpu.make_async_copy(ids_ref, mids.at[my_b], in_sem.at[1]),
        pltpu.make_async_copy(slots_ref, mslots.at[my_b], in_sem.at[2]),
        pltpu.make_async_copy(gates_ref, gates, in_sem.at[3]),
        pltpu.make_async_copy(pc_ref, counts, in_sem.at[4]),
    ]
    for c in own_copies:
        c.start()
    wcopies = [
        pltpu.make_async_copy(wd_ref, wd, w_sem.at[0]),
        pltpu.make_async_copy(wg_ref, wgu.at[:, pl.ds(0, ffn)], w_sem.at[1]),
        pltpu.make_async_copy(wu_ref, wgu.at[:, pl.ds(ffn, ffn)], w_sem.at[2]),
    ]
    for c in wcopies:
        c.start()

    def offset(k, axis):
        return lut(k, [o[axis] for o in ORDER])

    def chip_at(k):
        return wrap(my + offset(k, 1)) * side + wrap(mx + offset(k, 0))

    def loads(k):
        q = chip_at(k)
        slot = k % 2
        rows = pl.ds(pl.multiple_of(q * crow, crow), crow)
        return [
            pltpu.make_async_copy(x_ref.at[rows], xb.at[slot], load_sem.at[0, slot]),
            pltpu.make_async_copy(hg_ref.at[rows], hgb.at[slot], load_sem.at[1, slot]),
            pltpu.make_async_copy(hu_ref.at[rows], hub.at[slot], load_sem.at[2, slot]),
        ]

    pl.semaphore_wait(barrier, len(peers))
    own_copies[0].wait()

    sends, pairs = [], []

    def block(src, h):
        return tokens.at[src, pl.ds(h * half, half)]

    def forward_msg(n, i, j, h, a, b):
        src = plane(i, j)
        return remote(block(src, h), block(src, h), ag_send.at[n], tok_sem.at[src, h], plane(a, b))

    def forward(*what):
        what = (len(sends), *what)
        sends.append(what)
        forward_msg(*what).start()

    def pair_msg(n, i, j):
        src = plane(i, j)
        return remote(tokens.at[src], tokens.at[src], pair_send.at[n], tok_sem.at[src, 0], partner)

    def to_partner(i, j):
        what = (len(pairs), i, j)
        pairs.append(what)
        pair_msg(*what).start()

    def arrived(src, h):
        landed(block(src, h), tok_sem.at[src, h])

    to_partner(0, 0)

    def tab_msg(i):
        to = (me + 1 + i) % n_dev
        return remote(stab.at[to], tabs.at[me], tab_send.at[i], tab_sem.at[me], to)

    def tab_start(i, carry):
        tab_msg(i).start()
        return carry

    for n in range(2):
        for a, b, h in ((1, 0, n), (-1, 0, 1 - n), (0, 1, n), (0, -1, 1 - n)):
            forward(0, 0, h, a, b)

    tell(round_sem.at[0])
    for c in loads(0):
        c.start()

    for c in own_copies[1:]:
        c.wait()
    ids = mids[my_b]
    slots = mslots[my_b]

    def table(e, carry):
        hit = ids == e
        slot = jnp.max(jnp.where(hit, slots, -1), axis=0, keepdims=True)
        slot = jnp.where(slot < counts[0, e], slot, -1)
        gate = jnp.sum(jnp.where(hit, gates[...], 0.0), axis=0, keepdims=True)
        stab[e] = jnp.concatenate([slot.astype(F32), gate], axis=0)
        return carry

    lax.fori_loop(0, n_dev, table, 0)
    gwg_ref[...] = jnp.zeros_like(gwg_ref)
    gwu_ref[...] = jnp.zeros_like(gwu_ref)
    gwd_ref[...] = jnp.zeros_like(gwd_ref)

    for n in range(side - 1):
        if n:
            tell(round_sem.at[n])
        pl.semaphore_wait(round_sem.at[n], len(peers))
    lax.fori_loop(0, n_dev - 1, tab_start, 0)
    tab_copy = pltpu.make_async_copy(stab.at[me], tabs.at[me], tab_sem.at[me])
    tab_copy.start()
    def meta_msgs():
        out = []
        for n, j in enumerate((1, -1, 2)):
            out.append(remote(mids.at[my_b], mids.at[my_b], meta_send.at[n, 0], meta_sem.at[my_b, 0], plane(0, j)))
            out.append(remote(mslots.at[my_b], mslots.at[my_b], meta_send.at[n, 1], meta_sem.at[my_b, 1], plane(0, j)))
        return out

    for c in meta_msgs():
        c.start()

    def event(i, j):
        src = plane(i, j)
        first = 1 if (i == 1 and j == 0) or j == 1 else 0
        for n, h in enumerate((first, 1 - first)):
            arrived(src, h)
            if j == 0:
                if n == 0 and abs(i) == 1:
                    forward(i, j, h, -i, 0)
                forward(i, j, h, 0, 1)
                forward(i, j, h, 0, -1)
            elif n == 0 and abs(j) == 1:
                forward(i, j, h, 0, -j)
        to_partner(i, j)

    def r_block(k, cc):
        axis = 1 - cc if FLIP else cc
        i, j = offset(k, axis), offset(k, 1 - axis)
        a, b = (mx, my) if axis == 0 else (my, mx)
        hb = wrap(b + j)
        home = chip_at(k) * CORES + cc
        step = jnp.where(i == 2, 1 - 2 * core, i)
        to = device(mx + step, my, cc) if axis == 0 else device(mx, my + step, cc)
        slot = (hb * side + a) * CORES + core
        hop = hb * 2 + core
        is_local = jnp.logical_and(i == 0, core == cc)
        return i, home, to, slot, hop, is_local

    def send_chunk(k):
        for cc in range(CORES):
            i, home, to, slot, hop, is_local = r_block(k, cc)

            @pl.when(is_local)
            def _():
                pltpu.make_async_copy(rbuf.at[home], ret.at[slot], ret_sem.at[slot]).start()

            @pl.when(i == 2)
            def _():
                remote(rbuf.at[home], relay.at[hop], ret_send.at[home], relay_sem.at[hop], to).start()

            @pl.when(jnp.logical_and(i != 2, jnp.logical_not(is_local)))
            def _():
                remote(rbuf.at[home], ret.at[slot], ret_send.at[home], ret_sem.at[slot], to).start()

    def relay_msg(j, way):
        hb = wrap(my_b + j)
        slot = (hb * side + wrap(my_a - 1 + 2 * way)) * CORES + way
        hop = hb * 2 + way
        return hop, remote(relay.at[hop], ret.at[slot], relay_send.at[hop], ret_sem.at[slot], plane(1 - 2 * way, 0))

    def hand_on(k):
        dx, dy = ORDER[k]
        i = jnp.where(turn == 0, dx, dy)
        j = jnp.where(turn == 0, dy, dx)

        @pl.when(i == 2)
        def _():
            for way in range(2):
                hop, msg = relay_msg(j, way)
                landed(relay.at[hop], relay_sem.at[hop])
                msg.start()

    slot_iota = lax.broadcasted_iota(jnp.int32, (cap, tok_dev), 0)
    slot_iota_f = slot_iota.astype(F32)
    for c in wcopies:
        c.wait()

    def chunk(k, carry):
        @pl.when(k > 0)
        def _():
            send_chunk(k - 1)

        for at, evs in EVENTS.items():
            @pl.when(k == at)
            def _(evs=evs):
                for i, j in evs:
                    event(i, j)

        for at, steps in RELAY.items():
            @pl.when(k == at)
            def _(steps=steps):
                for n in steps:
                    hand_on(n)

        slot = k % 2
        for c in loads(k):
            c.wait()

        @pl.when(k + 1 < n_chip)
        def _():
            for c in loads(k + 1):
                c.start()

        q = chip_at(k)
        landed(tokens.at[q * CORES + 1 - core], tok_sem.at[q * CORES + 1 - core, 0])

        d_parts = []
        for cc in range(CORES):
            home = q * CORES + cc
            landed(tabs.at[home], tab_sem.at[home])
            tab = tabs[home]
            pick = tab[0:1, :] == slot_iota_f
            gate = jnp.sum(jnp.where(pick, tab[1:2, :], 0.0), axis=1, keepdims=True)
            rows = dot(pick.astype(F32).astype(BF16), tokens[home], NN)
            d_parts.append((gate * rows).astype(BF16))
        d = jnp.concatenate(d_parts, axis=0)
        da = dot(d, wd[...], NT).astype(BF16).astype(F32)
        h1 = hgb[slot].astype(F32)
        h3 = hub[slot].astype(F32)
        g = jax.nn.sigmoid(h1)
        s = h1 * g
        act = (s * h3).astype(BF16)
        dh1 = (da * h3 * g * (1.0 + h1 * (1.0 - g))).astype(BF16)
        dh3 = (da * s).astype(BF16)
        dh = jnp.concatenate([dh1, dh3], axis=1)
        r = dot(dh, wgu[...], NT).astype(BF16)
        for cc in range(CORES):
            rbuf[q * CORES + cc] = r[cc * cap:(cc + 1) * cap]
        x = xb[slot]
        gwg_ref[...] += dot(x, dh1, TN)
        gwu_ref[...] += dot(x, dh3, TN)
        gwd_ref[...] += dot(act, d, TN)
        return carry

    lax.fori_loop(0, n_chip, chunk, 0)
    send_chunk(jnp.int32(n_chip - 1))

    n_run = crow // top_k
    n_step = tok_dev // n_run

    def y_load(m):
        return pltpu.make_async_copy(y_ref.at[pl.ds(pl.multiple_of(m * crow, crow), crow)], xb.at[m % 2], load_sem.at[0, m % 2])

    y_load(0).start()
    lane = lax.broadcasted_iota(jnp.int32, (crow, tok_dev), 1)
    token_of = lax.broadcasted_iota(jnp.int32, (crow, tok_dev), 0) // top_k
    gg_ref[...] = jnp.zeros_like(gg_ref)

    def gate_grad(m, carry):
        y_load(m).wait()

        @pl.when(m + 1 < n_step)
        def _():
            y_load(m + 1).start()

        gy = tokens[me, pl.ds(pl.multiple_of(m * n_run, n_run), n_run), :].astype(F32)
        gy = jnp.broadcast_to(gy[:, None, :], (n_run, top_k, model_dim)).reshape(crow, model_dim)
        col = jnp.sum(xb[m % 2].astype(F32) * gy, axis=1, keepdims=True)
        put = jnp.where(lane == token_of + m * n_run, col, 0.0)
        gg_ref[...] += jnp.sum(put.reshape(n_run, top_k, tok_dev), axis=0)
        return carry

    for k in TAIL_RELAY[0]:
        hand_on(k)
    lax.fori_loop(0, n_step, gate_grad, 0)
    for k in TAIL_RELAY[1]:
        hand_on(k)

    def add_rows(n, carry):
        j = lut(n, LINES)
        hb = wrap(my_b + j)

        @pl.when(j != 0)
        def _():
            landed(mids.at[hb], meta_sem.at[hb, 0])
            landed(mslots.at[hb], meta_sem.at[hb, 1])

        h_ids = mids[hb]
        h_slots = mslots[hb]
        picks = []
        for sa in range(side):
            for ce in range(CORES):
                x = (1 - turn) * sa + turn * my_b
                y = (1 - turn) * my_b + turn * sa
                row = jnp.max(jnp.where(h_ids == (y * side + x) * CORES + ce, h_slots, -1), axis=0, keepdims=True)
                picks.append((row == slot_iota).astype(F32).astype(BF16))
        pick = jnp.concatenate(picks, axis=0)

        @pl.when(n == 2)
        def _():
            for c in hop_msgs():
                c.start()

        for sa in range(side):
            for ce in range(CORES):
                slot = (hb * side + sa) * CORES + ce
                landed(ret.at[slot], ret_sem.at[slot])
        rows = ret[pl.ds(hb * side * CORES, side * CORES)].reshape(side * CORES * cap, model_dim)
        part[lut(n, [PART[v] for v in LINES])] = dot(pick, rows, TN)
        return carry

    def hop_msgs():
        return [
            remote(part.at[0, pl.ds(0, half)], hop_in.at[0], part_send.at[0], hop_sem.at[0], plane(0, 1)),
            remote(part.at[0, pl.ds(half, half)], hop_in.at[1], part_send.at[1], hop_sem.at[1], plane(0, -1)),
        ]

    def fin_msgs():
        return [
            remote(part.at[1 + n, pl.ds(h * half, half)], fin.at[n, pl.ds(h * half, half)], part_send.at[2 + 2 * n + h], fin_sem.at[n, h], plane(0, 1 - 2 * n))
            for n in range(2)
            for h in range(2)
        ]

    fins = fin_msgs()
    lax.fori_loop(0, len(LINES), add_rows, 0)
    fins[2].start()
    fins[1].start()
    for what in sends:
        forward_msg(*what).wait_send()
    for what in pairs:
        pair_msg(*what).wait_send()
    landed(hop_in.at[0], hop_sem.at[0])
    part[1, pl.ds(0, half)] += hop_in[0]
    landed(hop_in.at[1], hop_sem.at[1])
    part[2, pl.ds(half, half)] += hop_in[1]

    def tab_done(i, carry):
        tab_msg(i).wait_send()
        return carry

    lax.fori_loop(0, n_dev - 1, tab_done, 0)
    fins[0].start()
    fins[3].start()
    for c in meta_msgs() + hop_msgs():
        c.wait_send()

    def ret_done(k, carry):
        for cc in range(CORES):
            i, home, to, slot, hop, is_local = r_block(k, cc)

            @pl.when(jnp.logical_not(is_local))
            def _():
                remote(rbuf.at[home], ret.at[slot], ret_send.at[home], ret_sem.at[slot], to).wait_send()
        return carry

    lax.fori_loop(0, n_chip, ret_done, 0)
    for j in (0, 1, -1, 2):
        for way in range(2):
            relay_msg(j, way)[1].wait_send()
    for n, h in ((0, 1), (1, 0), (0, 0), (1, 1)):
        rows = pl.ds(h * half, half)
        landed(fin.at[n, rows], fin_sem.at[n, h])
        if (n, h) == (0, 0):
            gx_ref[rows] = (part[3, rows] + fin[0, rows] + fin[1, rows]).astype(gx_ref.dtype)
    rows = pl.ds(half, half)
    gx_ref[rows] = (part[3, rows] + fin[0, rows] + fin[1, rows]).astype(gx_ref.dtype)
    for c in fins:
        c.wait_send()


def write_out(*refs):
    n = len(refs) // 2
    sems = refs[-1]
    copies = [pltpu.make_async_copy(refs[i], refs[n + i], sems.at[i]) for i in range(n)]
    for c in copies:
        c.start()
    for c in copies:
        c.wait()


def solution(mesh):
    n_dev = mesh.shape["ep"]
    side = math.isqrt(n_dev // CORES)
    rows_spec = P(("dp", "ep"), None)
    cube_spec = P(("dp", "ep"), None, None)
    weight_spec = P("ep", None, None)

    def local_step(grad_y, gate_vals, topk_idx, slot_ids, pair_counts, y_routed, x_disp, h_gate, h_up, w_gate, w_up, w_down):
        assert w_gate.shape[0] == 1
        assert side * side * CORES == n_dev and len(ORDER) == side * side
        cap = x_disp.shape[1] // n_dev
        tok_dev, model_dim = grad_y.shape
        ffn = w_gate.shape[2]
        crow = CORES * cap
        n_chip = side * side
        top_k = topk_idx.shape[1]
        vmem = pl.BlockSpec(memory_space=pltpu.VMEM)
        anym = pl.BlockSpec(memory_space=pl.ANY)
        dma = pltpu.SemaphoreType.DMA
        results = pl.pallas_call(
            functools.partial(kernel, n_dev, side),
            out_shape=(
                pltpu.VMEM((tok_dev, model_dim), BF16),
                pltpu.VMEM((top_k, tok_dev), F32),
                pltpu.VMEM((model_dim, ffn), F32),
                pltpu.VMEM((model_dim, ffn), F32),
                pltpu.VMEM((ffn, model_dim), F32),
            ),
            in_specs=[anym] * 12,
            out_specs=(vmem,) * 5,
            scratch_shapes=[
                pltpu.VMEM((n_dev, tok_dev, model_dim), BF16),
                pltpu.VMEM((n_dev, 2, tok_dev), F32),
                pltpu.VMEM((n_dev, 2, tok_dev), F32),
                pltpu.VMEM((side, top_k, tok_dev), jnp.int32),
                pltpu.VMEM((side, top_k, tok_dev), jnp.int32),
                pltpu.VMEM((n_dev, cap, model_dim), BF16),
                pltpu.VMEM((n_dev, cap, model_dim), BF16),
                pltpu.VMEM((2 * side, cap, model_dim), BF16),
                pltpu.VMEM((4, tok_dev, model_dim), F32),
                pltpu.VMEM((2, tok_dev // 2, model_dim), F32),
                pltpu.VMEM((2, tok_dev, model_dim), F32),
                pltpu.VMEM((model_dim, 2 * ffn), BF16),
                pltpu.VMEM((ffn, model_dim), BF16),
                pltpu.VMEM((2, crow, model_dim), BF16),
                pltpu.VMEM((2, crow, ffn), BF16),
                pltpu.VMEM((2, crow, ffn), BF16),
                dma((n_dev, 2)),
                dma((n_dev,)),
                dma((side, 2)),
                dma((n_dev,)),
                dma((2 * side,)),
                dma((2,)),
                dma((2, 2)),
                dma((64,)),
                dma((n_chip,)),
                dma((n_dev,)),
                dma((3, 2)),
                dma((n_dev,)),
                dma((2 * side,)),
                dma((6,)),
                dma((3, 2)),
                dma((3,)),
                pltpu.SemaphoreType.REGULAR((side - 1,)),
                pltpu.VMEM((top_k, tok_dev), F32),
                pltpu.SMEM(pair_counts.shape, jnp.int32),
                dma((5,)),
            ],
            compiler_params=pltpu.CompilerParams(collective_id=0, has_side_effects=True, vmem_limit_bytes=58720256),
            name="moe_bwd",
        )(grad_y, topk_idx.T, slot_ids.T, gate_vals.T, pair_counts, y_routed.reshape(tok_dev * top_k, model_dim), x_disp[0], h_gate[0], h_up[0], w_gate[0], w_up[0], w_down[0])
        gx, gg, gwg, gwu, gwd = pl.pallas_call(
            write_out,
            out_shape=tuple(jax.ShapeDtypeStruct(r.shape, r.dtype) for r in results),
            in_specs=[anym] * len(results),
            out_specs=(anym,) * len(results),
            scratch_shapes=[dma((len(results),))],
            compiler_params=pltpu.CompilerParams(vmem_limit_bytes=1048576),
            name="write_out",
        )(*results)
        return gx, gg.T, gwg[None], gwu[None], gwd[None]

    return jax.shard_map(local_step, mesh=mesh, in_specs=(rows_spec, rows_spec, rows_spec, rows_spec, rows_spec, cube_spec, cube_spec, cube_spec, cube_spec, weight_spec, weight_spec, weight_spec), out_specs=(rows_spec, rows_spec, cube_spec, cube_spec, cube_spec), check_vma=False)
```

```python
import functools
import math

import jax
import jax.numpy as jnp
from jax import lax
from jax.experimental import pallas as pl
from jax.experimental.pallas import tpu as pltpu
from jax.sharding import PartitionSpec as P

MESH = pl.DeviceIdType.MESH
CORES = 2
BF16, F32 = jnp.bfloat16, jnp.float32

ORDER = ((-1, 0), (0, 1), (0, -1), (0, 0), (-1, 1), (1, 0), (1, -1), (1, 1), (0, 2), (-1, -1), (2, 0), (2, 1), (2, -1), (2, 2), (1, 2), (-1, 2))
EVENTS = {
    0: ((-1, 0), (0, -1), (1, 0), (0, 1)),
    2: ((2, 0), (-1, 1)),
    4: ((0, 2), (1, -1), (-1, -1)),
    5: ((1, 1),),
    6: ((2, -1),),
    9: ((2, 1),),
    10: ((1, 2),),
    12: ((2, 2), (-1, 2)),
}
FLIP = 1
RELAY = {15: (11,)}
TAIL_RELAY = (13, 10, 8, 14), (15, 12)

LINES = (2, 0, -1, 1)
PART = {2: 0, 1: 1, -1: 2, 0: 3}

NN = (((1,), (0,)), ((), ()))
NT = (((1,), (1,)), ((), ()))
TN = (((0,), (0,)), ((), ()))


def dot(a, b, dims):
    return lax.dot_general(a, b, dims, preferred_element_type=F32)


def lut(k, vals):
    out = vals[0]
    for i, v in enumerate(vals):
        if i:
            out = jnp.where(k == i, v, out)
    return out


def kernel(n_dev, side, gy_ref, ids_ref, slots_ref, gates_ref, pc_ref, y_ref, x_ref, hg_ref, hu_ref, wg_ref, wu_ref, wd_ref,
           gx_ref, gg_ref, gwg_ref, gwu_ref, gwd_ref,
           tokens, stab, tabs, mids, mslots, rbuf, ret, relay, part, hop_in, fin, wgu, wd, xb, hgb, hub,
           tok_sem, tab_sem, meta_sem, ret_sem, relay_sem, hop_sem, fin_sem,
           ag_send, pair_send, tab_send, meta_send, ret_send, relay_send, part_send, load_sem, w_sem, round_sem, gates, counts, in_sem):
    me = lax.axis_index("ep")
    core = me % CORES
    mx = (me // CORES) % side
    my = me // (CORES * side)
    turn = 1 - core if FLIP else core
    my_a = (1 - turn) * mx + turn * my
    my_b = (1 - turn) * my + turn * mx
    tok_dev, model_dim = gy_ref.shape
    top_k = ids_ref.shape[0]
    ffn = wg_ref.shape[1]
    cap = rbuf.shape[1]
    half = tok_dev // 2
    n_chip = side * side
    crow = CORES * cap
    partner = me + 1 - 2 * core

    def wrap(v):
        return (v + 2 * side) % side

    def device(x, y, c):
        return (wrap(y) * side + wrap(x)) * CORES + c

    def plane(a, b):
        return device(mx + (1 - turn) * a + turn * b, my + turn * a + (1 - turn) * b, core)

    def remote(src, dst, send_sem, recv_sem, to):
        return pltpu.make_async_remote_copy(src_ref=src, dst_ref=dst, send_sem=send_sem, recv_sem=recv_sem, device_id={"ep": to}, device_id_type=MESH)

    def landed(ref, sem):
        pltpu.make_async_copy(ref, ref, sem).wait()

    peers = [partner] + [device(mx + dx, my + dy, c) for dx, dy in ((1, 0), (-1, 0), (0, 1), (0, -1)) for c in range(CORES)]

    def tell(sem):
        for to in peers:
            pl.semaphore_signal(sem, inc=1, device_id={"ep": to}, device_id_type=MESH)

    barrier = pltpu.get_barrier_semaphore()
    tell(barrier)

    own_copies = [
        pltpu.make_async_copy(gy_ref, tokens.at[me], in_sem.at[0]),
        pltpu.make_async_copy(ids_ref, mids.at[my_b], in_sem.at[1]),
        pltpu.make_async_copy(slots_ref, mslots.at[my_b], in_sem.at[2]),
        pltpu.make_async_copy(gates_ref, gates, in_sem.at[3]),
        pltpu.make_async_copy(pc_ref, counts, in_sem.at[4]),
    ]
    for c in own_copies:
        c.start()
    wcopies = [
        pltpu.make_async_copy(wd_ref, wd, w_sem.at[0]),
        pltpu.make_async_copy(wg_ref, wgu.at[:, pl.ds(0, ffn)], w_sem.at[1]),
        pltpu.make_async_copy(wu_ref, wgu.at[:, pl.ds(ffn, ffn)], w_sem.at[2]),
    ]
    for c in wcopies:
        c.start()

    def offset(k, axis):
        return lut(k, [o[axis] for o in ORDER])

    def chip_at(k):
        return wrap(my + offset(k, 1)) * side + wrap(mx + offset(k, 0))

    def loads(k):
        q = chip_at(k)
        slot = k % 2
        rows = pl.ds(pl.multiple_of(q * crow, crow), crow)
        return [
            pltpu.make_async_copy(x_ref.at[rows], xb.at[slot], load_sem.at[0, slot]),
            pltpu.make_async_copy(hg_ref.at[rows], hgb.at[slot], load_sem.at[1, slot]),
            pltpu.make_async_copy(hu_ref.at[rows], hub.at[slot], load_sem.at[2, slot]),
        ]

    pl.semaphore_wait(barrier, len(peers))
    own_copies[0].wait()

    sends, pairs = [], []

    def block(src, h):
        return tokens.at[src, pl.ds(h * half, half)]

    def forward_msg(n, i, j, h, a, b):
        src = plane(i, j)
        return remote(block(src, h), block(src, h), ag_send.at[n], tok_sem.at[src, h], plane(a, b))

    def forward(*what):
        what = (len(sends), *what)
        sends.append(what)
        forward_msg(*what).start()

    def pair_msg(n, i, j):
        src = plane(i, j)
        return remote(tokens.at[src], tokens.at[src], pair_send.at[n], tok_sem.at[src, 0], partner)

    def to_partner(i, j):
        what = (len(pairs), i, j)
        pairs.append(what)
        pair_msg(*what).start()

    def arrived(src, h):
        landed(block(src, h), tok_sem.at[src, h])

    to_partner(0, 0)

    def tab_msg(i):
        to = (me + 1 + i) % n_dev
        return remote(stab.at[to], tabs.at[me], tab_send.at[i], tab_sem.at[me], to)

    def tab_start(i, carry):
        tab_msg(i).start()
        return carry

    for n in range(2):
        for a, b, h in ((1, 0, n), (-1, 0, 1 - n), (0, 1, n), (0, -1, 1 - n)):
            forward(0, 0, h, a, b)

    tell(round_sem.at[0])
    for c in loads(0):
        c.start()

    for c in own_copies[1:]:
        c.wait()
    ids = mids[my_b]
    slots = mslots[my_b]

    def table(e, carry):
        hit = ids == e
        slot = jnp.max(jnp.where(hit, slots, -1), axis=0, keepdims=True)
        slot = jnp.where(slot < counts[0, e], slot, -1)
        gate = jnp.sum(jnp.where(hit, gates[...], 0.0), axis=0, keepdims=True)
        stab[e] = jnp.concatenate([slot.astype(F32), gate], axis=0)
        return carry

    lax.fori_loop(0, n_dev, table, 0)
    gwg_ref[...] = jnp.zeros_like(gwg_ref)
    gwu_ref[...] = jnp.zeros_like(gwu_ref)
    gwd_ref[...] = jnp.zeros_like(gwd_ref)

    for n in range(side - 1):
        if n:
            tell(round_sem.at[n])
        pl.semaphore_wait(round_sem.at[n], len(peers))
    lax.fori_loop(0, n_dev - 1, tab_start, 0)
    tab_copy = pltpu.make_async_copy(stab.at[me], tabs.at[me], tab_sem.at[me])
    tab_copy.start()
    def meta_msgs():
        out = []
        for n, j in enumerate((1, -1, 2)):
            out.append(remote(mids.at[my_b], mids.at[my_b], meta_send.at[n, 0], meta_sem.at[my_b, 0], plane(0, j)))
            out.append(remote(mslots.at[my_b], mslots.at[my_b], meta_send.at[n, 1], meta_sem.at[my_b, 1], plane(0, j)))
        return out

    for c in meta_msgs():
        c.start()

    def event(i, j):
        src = plane(i, j)
        first = 1 if (i == 1 and j == 0) or j == 1 else 0
        for n, h in enumerate((first, 1 - first)):
            arrived(src, h)
            if j == 0:
                if n == 0 and abs(i) == 1:
                    forward(i, j, h, -i, 0)
                forward(i, j, h, 0, 1)
                forward(i, j, h, 0, -1)
            elif n == 0 and abs(j) == 1:
                forward(i, j, h, 0, -j)
        to_partner(i, j)

    def r_block(k, cc):
        axis = 1 - cc if FLIP else cc
        i, j = offset(k, axis), offset(k, 1 - axis)
        a, b = (mx, my) if axis == 0 else (my, mx)
        hb = wrap(b + j)
        home = chip_at(k) * CORES + cc
        step = jnp.where(i == 2, 1 - 2 * core, i)
        to = device(mx + step, my, cc) if axis == 0 else device(mx, my + step, cc)
        slot = (hb * side + a) * CORES + core
        hop = hb * 2 + core
        is_local = jnp.logical_and(i == 0, core == cc)
        return i, home, to, slot, hop, is_local

    def send_chunk(k):
        for cc in range(CORES):
            i, home, to, slot, hop, is_local = r_block(k, cc)

            @pl.when(is_local)
            def _():
                pltpu.make_async_copy(rbuf.at[home], ret.at[slot], ret_sem.at[slot]).start()

            @pl.when(i == 2)
            def _():
                remote(rbuf.at[home], relay.at[hop], ret_send.at[home], relay_sem.at[hop], to).start()

            @pl.when(jnp.logical_and(i != 2, jnp.logical_not(is_local)))
            def _():
                remote(rbuf.at[home], ret.at[slot], ret_send.at[home], ret_sem.at[slot], to).start()

    def relay_msg(j, way):
        hb = wrap(my_b + j)
        slot = (hb * side + wrap(my_a - 1 + 2 * way)) * CORES + way
        hop = hb * 2 + way
        return hop, remote(relay.at[hop], ret.at[slot], relay_send.at[hop], ret_sem.at[slot], plane(1 - 2 * way, 0))

    def hand_on(k):
        dx, dy = ORDER[k]
        i = jnp.where(turn == 0, dx, dy)
        j = jnp.where(turn == 0, dy, dx)

        @pl.when(i == 2)
        def _():
            for way in range(2):
                hop, msg = relay_msg(j, way)
                landed(relay.at[hop], relay_sem.at[hop])
                msg.start()

    slot_iota = lax.broadcasted_iota(jnp.int32, (cap, tok_dev), 0)
    slot_iota_f = slot_iota.astype(F32)
    for c in wcopies:
        c.wait()

    def chunk(k, carry):
        @pl.when(k > 0)
        def _():
            send_chunk(k - 1)

        for at, evs in EVENTS.items():
            @pl.when(k == at)
            def _(evs=evs):
                for i, j in evs:
                    event(i, j)

        for at, steps in RELAY.items():
            @pl.when(k == at)
            def _(steps=steps):
                for n in steps:
                    hand_on(n)

        slot = k % 2
        for c in loads(k):
            c.wait()

        @pl.when(k + 1 < n_chip)
        def _():
            for c in loads(k + 1):
                c.start()

        q = chip_at(k)
        landed(tokens.at[q * CORES + 1 - core], tok_sem.at[q * CORES + 1 - core, 0])

        d_parts = []
        for cc in range(CORES):
            home = q * CORES + cc
            landed(tabs.at[home], tab_sem.at[home])
            tab = tabs[home]
            pick = tab[0:1, :] == slot_iota_f
            gate = jnp.sum(jnp.where(pick, tab[1:2, :], 0.0), axis=1, keepdims=True)
            rows = dot(pick.astype(F32).astype(BF16), tokens[home], NN)
            d_parts.append((gate * rows).astype(BF16))
        d = jnp.concatenate(d_parts, axis=0)
        da = dot(d, wd[...], NT).astype(BF16).astype(F32)
        h1 = hgb[slot].astype(F32)
        h3 = hub[slot].astype(F32)
        g = jax.nn.sigmoid(h1)
        s = h1 * g
        act = (s * h3).astype(BF16)
        dh1 = (da * h3 * g * (1.0 + h1 * (1.0 - g))).astype(BF16)
        dh3 = (da * s).astype(BF16)
        dh = jnp.concatenate([dh1, dh3], axis=1)
        r = dot(dh, wgu[...], NT).astype(BF16)
        for cc in range(CORES):
            rbuf[q * CORES + cc] = r[cc * cap:(cc + 1) * cap]
        x = xb[slot]
        gwg_ref[...] += dot(x, dh1, TN)
        gwu_ref[...] += dot(x, dh3, TN)
        gwd_ref[...] += dot(act, d, TN)
        return carry

    lax.fori_loop(0, n_chip, chunk, 0)
    send_chunk(jnp.int32(n_chip - 1))

    n_run = crow // top_k
    n_step = tok_dev // n_run

    def y_load(m):
        return pltpu.make_async_copy(y_ref.at[pl.ds(pl.multiple_of(m * crow, crow), crow)], xb.at[m % 2], load_sem.at[0, m % 2])

    y_load(0).start()
    lane = lax.broadcasted_iota(jnp.int32, (crow, tok_dev), 1)
    token_of = lax.broadcasted_iota(jnp.int32, (crow, tok_dev), 0) // top_k
    gg_ref[...] = jnp.zeros_like(gg_ref)

    def gate_grad(m, carry):
        y_load(m).wait()

        @pl.when(m + 1 < n_step)
        def _():
            y_load(m + 1).start()

        gy = tokens[me, pl.ds(pl.multiple_of(m * n_run, n_run), n_run), :].astype(F32)
        gy = jnp.broadcast_to(gy[:, None, :], (n_run, top_k, model_dim)).reshape(crow, model_dim)
        col = jnp.sum(xb[m % 2].astype(F32) * gy, axis=1, keepdims=True)
        put = jnp.where(lane == token_of + m * n_run, col, 0.0)
        gg_ref[...] += jnp.sum(put.reshape(n_run, top_k, tok_dev), axis=0)
        return carry

    for k in TAIL_RELAY[0]:
        hand_on(k)
    lax.fori_loop(0, n_step, gate_grad, 0)
    for k in TAIL_RELAY[1]:
        hand_on(k)

    def add_rows(n, carry):
        j = lut(n, LINES)
        hb = wrap(my_b + j)

        @pl.when(j != 0)
        def _():
            landed(mids.at[hb], meta_sem.at[hb, 0])
            landed(mslots.at[hb], meta_sem.at[hb, 1])

        h_ids = mids[hb]
        h_slots = mslots[hb]
        picks = []
        for sa in range(side):
            for ce in range(CORES):
                slot = (hb * side + sa) * CORES + ce
                landed(ret.at[slot], ret_sem.at[slot])
                x = (1 - turn) * sa + turn * my_b
                y = (1 - turn) * my_b + turn * sa
                row = jnp.max(jnp.where(h_ids == (y * side + x) * CORES + ce, h_slots, -1), axis=0, keepdims=True)
                picks.append((row == slot_iota).astype(F32).astype(BF16))
        pick = jnp.concatenate(picks, axis=0)
        rows = ret[pl.ds(hb * side * CORES, side * CORES)].reshape(side * CORES * cap, model_dim)
        part[lut(n, [PART[v] for v in LINES])] = dot(pick, rows, TN)

        @pl.when(n == 1)
        def _():
            for c in hop_msgs():
                c.start()

        return carry

    def hop_msgs():
        return [
            remote(part.at[0, pl.ds(0, half)], hop_in.at[0], part_send.at[0], hop_sem.at[0], plane(0, 1)),
            remote(part.at[0, pl.ds(half, half)], hop_in.at[1], part_send.at[1], hop_sem.at[1], plane(0, -1)),
        ]

    def fin_msgs():
        return [
            remote(part.at[1 + n, pl.ds(h * half, half)], fin.at[n, pl.ds(h * half, half)], part_send.at[2 + 2 * n + h], fin_sem.at[n, h], plane(0, 1 - 2 * n))
            for n in range(2)
            for h in range(2)
        ]

    fins = fin_msgs()
    lax.fori_loop(0, len(LINES), add_rows, 0)
    fins[2].start()
    for what in sends:
        forward_msg(*what).wait_send()
    for what in pairs:
        pair_msg(*what).wait_send()
    fins[1].start()
    landed(hop_in.at[0], hop_sem.at[0])
    part[1, pl.ds(0, half)] += hop_in[0]
    landed(hop_in.at[1], hop_sem.at[1])
    part[2, pl.ds(half, half)] += hop_in[1]

    def tab_done(i, carry):
        tab_msg(i).wait_send()
        return carry

    lax.fori_loop(0, n_dev - 1, tab_done, 0)
    fins[0].start()
    fins[3].start()
    for c in meta_msgs() + hop_msgs():
        c.wait_send()

    def ret_done(k, carry):
        for cc in range(CORES):
            i, home, to, slot, hop, is_local = r_block(k, cc)

            @pl.when(jnp.logical_not(is_local))
            def _():
                remote(rbuf.at[home], ret.at[slot], ret_send.at[home], ret_sem.at[slot], to).wait_send()
        return carry

    lax.fori_loop(0, n_chip, ret_done, 0)
    for j in (0, 1, -1, 2):
        for way in range(2):
            relay_msg(j, way)[1].wait_send()
    for n, h in ((0, 1), (1, 0), (0, 0), (1, 1)):
        rows = pl.ds(h * half, half)
        landed(fin.at[n, rows], fin_sem.at[n, h])
        if (n, h) == (0, 0):
            gx_ref[rows] = (part[3, rows] + fin[0, rows] + fin[1, rows]).astype(gx_ref.dtype)
    rows = pl.ds(half, half)
    gx_ref[rows] = (part[3, rows] + fin[0, rows] + fin[1, rows]).astype(gx_ref.dtype)
    for c in fins:
        c.wait_send()


def write_out(*refs):
    n = len(refs) // 2
    sems = refs[-1]
    copies = [pltpu.make_async_copy(refs[i], refs[n + i], sems.at[i]) for i in range(n)]
    for c in copies:
        c.start()
    for c in copies:
        c.wait()


def solution(mesh):
    n_dev = mesh.shape["ep"]
    side = math.isqrt(n_dev // CORES)
    rows_spec = P(("dp", "ep"), None)
    cube_spec = P(("dp", "ep"), None, None)
    weight_spec = P("ep", None, None)

    def local_step(grad_y, gate_vals, topk_idx, slot_ids, pair_counts, y_routed, x_disp, h_gate, h_up, w_gate, w_up, w_down):
        assert w_gate.shape[0] == 1
        assert side * side * CORES == n_dev and len(ORDER) == side * side
        cap = x_disp.shape[1] // n_dev
        tok_dev, model_dim = grad_y.shape
        ffn = w_gate.shape[2]
        crow = CORES * cap
        n_chip = side * side
        top_k = topk_idx.shape[1]
        vmem = pl.BlockSpec(memory_space=pltpu.VMEM)
        anym = pl.BlockSpec(memory_space=pl.ANY)
        dma = pltpu.SemaphoreType.DMA
        results = pl.pallas_call(
            functools.partial(kernel, n_dev, side),
            out_shape=(
                pltpu.VMEM((tok_dev, model_dim), BF16),
                pltpu.VMEM((top_k, tok_dev), F32),
                pltpu.VMEM((model_dim, ffn), F32),
                pltpu.VMEM((model_dim, ffn), F32),
                pltpu.VMEM((ffn, model_dim), F32),
            ),
            in_specs=[anym] * 12,
            out_specs=(vmem,) * 5,
            scratch_shapes=[
                pltpu.VMEM((n_dev, tok_dev, model_dim), BF16),
                pltpu.VMEM((n_dev, 2, tok_dev), F32),
                pltpu.VMEM((n_dev, 2, tok_dev), F32),
                pltpu.VMEM((side, top_k, tok_dev), jnp.int32),
                pltpu.VMEM((side, top_k, tok_dev), jnp.int32),
                pltpu.VMEM((n_dev, cap, model_dim), BF16),
                pltpu.VMEM((n_dev, cap, model_dim), BF16),
                pltpu.VMEM((2 * side, cap, model_dim), BF16),
                pltpu.VMEM((4, tok_dev, model_dim), F32),
                pltpu.VMEM((2, tok_dev // 2, model_dim), F32),
                pltpu.VMEM((2, tok_dev, model_dim), F32),
                pltpu.VMEM((model_dim, 2 * ffn), BF16),
                pltpu.VMEM((ffn, model_dim), BF16),
                pltpu.VMEM((2, crow, model_dim), BF16),
                pltpu.VMEM((2, crow, ffn), BF16),
                pltpu.VMEM((2, crow, ffn), BF16),
                dma((n_dev, 2)),
                dma((n_dev,)),
                dma((side, 2)),
                dma((n_dev,)),
                dma((2 * side,)),
                dma((2,)),
                dma((2, 2)),
                dma((64,)),
                dma((n_chip,)),
                dma((n_dev,)),
                dma((3, 2)),
                dma((n_dev,)),
                dma((2 * side,)),
                dma((6,)),
                dma((3, 2)),
                dma((3,)),
                pltpu.SemaphoreType.REGULAR((side - 1,)),
                pltpu.VMEM((top_k, tok_dev), F32),
                pltpu.SMEM(pair_counts.shape, jnp.int32),
                dma((5,)),
            ],
            compiler_params=pltpu.CompilerParams(collective_id=0, has_side_effects=True, vmem_limit_bytes=58720256),
            name="moe_bwd",
        )(grad_y, topk_idx.T, slot_ids.T, gate_vals.T, pair_counts, y_routed.reshape(tok_dev * top_k, model_dim), x_disp[0], h_gate[0], h_up[0], w_gate[0], w_up[0], w_down[0])
        gx, gg, gwg, gwu, gwd = pl.pallas_call(
            write_out,
            out_shape=tuple(jax.ShapeDtypeStruct(r.shape, r.dtype) for r in results),
            in_specs=[anym] * len(results),
            out_specs=(anym,) * len(results),
            scratch_shapes=[dma((len(results),))],
            compiler_params=pltpu.CompilerParams(vmem_limit_bytes=1048576),
            name="write_out",
        )(*results)
        return gx, gg.T, gwg[None], gwu[None], gwd[None]

    return jax.shard_map(local_step, mesh=mesh, in_specs=(rows_spec, rows_spec, rows_spec, rows_spec, rows_spec, cube_spec, cube_spec, cube_spec, cube_spec, weight_spec, weight_spec, weight_spec), out_specs=(rows_spec, rows_spec, cube_spec, cube_spec, cube_spec), check_vma=False)
```

```python
import functools
import math

import jax
import jax.numpy as jnp
from jax import lax
from jax.experimental import pallas as pl
from jax.experimental.pallas import tpu as pltpu
from jax.sharding import PartitionSpec as P

MESH = pl.DeviceIdType.MESH
CORES = 2
BF16, F32 = jnp.bfloat16, jnp.float32

ORDER = ((-1, 0), (0, 1), (0, -1), (0, 0), (-1, 1), (1, 0), (1, -1), (1, 1), (0, 2), (-1, -1), (2, 0), (2, 1), (2, -1), (2, 2), (1, 2), (-1, 2))
EVENTS = {
    0: ((-1, 0), (0, -1), (1, 0), (0, 1)),
    2: ((2, 0), (-1, 1)),
    4: ((0, 2), (1, -1), (-1, -1)),
    5: ((1, 1),),
    6: ((2, -1),),
    9: ((2, 1),),
    10: ((1, 2),),
    12: ((2, 2), (-1, 2)),
}
FLIP = 1
RELAY = {}
TAIL_RELAY = (11, 13, 10, 8, 14), (15, 12)

LINES = (2, 0, -1, 1)
PART = {2: 0, 1: 1, -1: 2, 0: 3}

NN = (((1,), (0,)), ((), ()))
NT = (((1,), (1,)), ((), ()))
TN = (((0,), (0,)), ((), ()))


def dot(a, b, dims):
    return lax.dot_general(a, b, dims, preferred_element_type=F32)


def lut(k, vals):
    out = vals[0]
    for i, v in enumerate(vals):
        if i:
            out = jnp.where(k == i, v, out)
    return out


def kernel(n_dev, side, gy_ref, ids_ref, slots_ref, gates_ref, pc_ref, y_ref, x_ref, hg_ref, hu_ref, wg_ref, wu_ref, wd_ref,
           gx_ref, gg_ref, gwg_ref, gwu_ref, gwd_ref,
           tokens, stab, tabs, mids, mslots, rbuf, ret, relay, part, hop_in, fin, wgu, wd, xb, hgb, hub,
           tok_sem, tab_sem, meta_sem, ret_sem, relay_sem, hop_sem, fin_sem,
           ag_send, pair_send, tab_send, meta_send, ret_send, relay_send, part_send, load_sem, w_sem, round_sem, gates, counts, in_sem):
    me = lax.axis_index("ep")
    core = me % CORES
    mx = (me // CORES) % side
    my = me // (CORES * side)
    turn = 1 - core if FLIP else core
    my_a = (1 - turn) * mx + turn * my
    my_b = (1 - turn) * my + turn * mx
    tok_dev, model_dim = gy_ref.shape
    top_k = ids_ref.shape[0]
    ffn = wg_ref.shape[1]
    cap = rbuf.shape[1]
    half = tok_dev // 2
    n_chip = side * side
    crow = CORES * cap
    partner = me + 1 - 2 * core

    def wrap(v):
        return (v + 2 * side) % side

    def device(x, y, c):
        return (wrap(y) * side + wrap(x)) * CORES + c

    def plane(a, b):
        return device(mx + (1 - turn) * a + turn * b, my + turn * a + (1 - turn) * b, core)

    def remote(src, dst, send_sem, recv_sem, to):
        return pltpu.make_async_remote_copy(src_ref=src, dst_ref=dst, send_sem=send_sem, recv_sem=recv_sem, device_id={"ep": to}, device_id_type=MESH)

    def landed(ref, sem):
        pltpu.make_async_copy(ref, ref, sem).wait()

    peers = [partner] + [device(mx + dx, my + dy, c) for dx, dy in ((1, 0), (-1, 0), (0, 1), (0, -1)) for c in range(CORES)]

    def tell(sem):
        for to in peers:
            pl.semaphore_signal(sem, inc=1, device_id={"ep": to}, device_id_type=MESH)

    barrier = pltpu.get_barrier_semaphore()
    tell(barrier)

    own_copies = [
        pltpu.make_async_copy(gy_ref, tokens.at[me], in_sem.at[0]),
        pltpu.make_async_copy(ids_ref, mids.at[my_b], in_sem.at[1]),
        pltpu.make_async_copy(slots_ref, mslots.at[my_b], in_sem.at[2]),
        pltpu.make_async_copy(gates_ref, gates, in_sem.at[3]),
        pltpu.make_async_copy(pc_ref, counts, in_sem.at[4]),
    ]
    for c in own_copies:
        c.start()
    wcopies = [
        pltpu.make_async_copy(wd_ref, wd, w_sem.at[0]),
        pltpu.make_async_copy(wg_ref, wgu.at[:, pl.ds(0, ffn)], w_sem.at[1]),
        pltpu.make_async_copy(wu_ref, wgu.at[:, pl.ds(ffn, ffn)], w_sem.at[2]),
    ]
    for c in wcopies:
        c.start()

    def offset(k, axis):
        return lut(k, [o[axis] for o in ORDER])

    def chip_at(k):
        return wrap(my + offset(k, 1)) * side + wrap(mx + offset(k, 0))

    def loads(k):
        q = chip_at(k)
        slot = k % 2
        rows = pl.ds(pl.multiple_of(q * crow, crow), crow)
        return [
            pltpu.make_async_copy(x_ref.at[rows], xb.at[slot], load_sem.at[0, slot]),
            pltpu.make_async_copy(hg_ref.at[rows], hgb.at[slot], load_sem.at[1, slot]),
            pltpu.make_async_copy(hu_ref.at[rows], hub.at[slot], load_sem.at[2, slot]),
        ]

    pl.semaphore_wait(barrier, len(peers))
    own_copies[0].wait()

    sends, pairs = [], []

    def block(src, h):
        return tokens.at[src, pl.ds(h * half, half)]

    def forward_msg(n, i, j, h, a, b):
        src = plane(i, j)
        return remote(block(src, h), block(src, h), ag_send.at[n], tok_sem.at[src, h], plane(a, b))

    def forward(*what):
        what = (len(sends), *what)
        sends.append(what)
        forward_msg(*what).start()

    def pair_msg(n, i, j):
        src = plane(i, j)
        return remote(tokens.at[src], tokens.at[src], pair_send.at[n], tok_sem.at[src, 0], partner)

    def to_partner(i, j):
        what = (len(pairs), i, j)
        pairs.append(what)
        pair_msg(*what).start()

    def arrived(src, h):
        landed(block(src, h), tok_sem.at[src, h])

    to_partner(0, 0)

    def tab_msg(i):
        to = (me + 1 + i) % n_dev
        return remote(stab.at[to], tabs.at[me], tab_send.at[i], tab_sem.at[me], to)

    def tab_start(i, carry):
        tab_msg(i).start()
        return carry

    for n in range(2):
        for a, b, h in ((1, 0, n), (-1, 0, 1 - n), (0, 1, n), (0, -1, 1 - n)):
            forward(0, 0, h, a, b)

    tell(round_sem.at[0])
    for c in loads(0):
        c.start()

    for c in own_copies[1:]:
        c.wait()
    ids = mids[my_b]
    slots = mslots[my_b]

    def table(e, carry):
        hit = ids == e
        slot = jnp.max(jnp.where(hit, slots, -1), axis=0, keepdims=True)
        slot = jnp.where(slot < counts[0, e], slot, -1)
        gate = jnp.sum(jnp.where(hit, gates[...], 0.0), axis=0, keepdims=True)
        stab[e] = jnp.concatenate([slot.astype(F32), gate], axis=0)
        return carry

    lax.fori_loop(0, n_dev, table, 0)
    gwg_ref[...] = jnp.zeros_like(gwg_ref)
    gwu_ref[...] = jnp.zeros_like(gwu_ref)
    gwd_ref[...] = jnp.zeros_like(gwd_ref)

    for n in range(side - 1):
        if n:
            tell(round_sem.at[n])
        pl.semaphore_wait(round_sem.at[n], len(peers))
    lax.fori_loop(0, n_dev - 1, tab_start, 0)
    tab_copy = pltpu.make_async_copy(stab.at[me], tabs.at[me], tab_sem.at[me])
    tab_copy.start()
    def meta_msgs():
        out = []
        for n, j in enumerate((1, -1, 2)):
            out.append(remote(mids.at[my_b], mids.at[my_b], meta_send.at[n, 0], meta_sem.at[my_b, 0], plane(0, j)))
            out.append(remote(mslots.at[my_b], mslots.at[my_b], meta_send.at[n, 1], meta_sem.at[my_b, 1], plane(0, j)))
        return out

    for c in meta_msgs():
        c.start()

    def event(i, j):
        src = plane(i, j)
        first = 1 if (i == 1 and j == 0) or j == 1 else 0
        for n, h in enumerate((first, 1 - first)):
            arrived(src, h)
            if j == 0:
                if n == 0 and abs(i) == 1:
                    forward(i, j, h, -i, 0)
                forward(i, j, h, 0, 1)
                forward(i, j, h, 0, -1)
            elif n == 0 and abs(j) == 1:
                forward(i, j, h, 0, -j)
        to_partner(i, j)

    def r_block(k, cc):
        axis = 1 - cc if FLIP else cc
        i, j = offset(k, axis), offset(k, 1 - axis)
        a, b = (mx, my) if axis == 0 else (my, mx)
        hb = wrap(b + j)
        home = chip_at(k) * CORES + cc
        step = jnp.where(i == 2, 1 - 2 * core, i)
        to = device(mx + step, my, cc) if axis == 0 else device(mx, my + step, cc)
        slot = (hb * side + a) * CORES + core
        hop = hb * 2 + core
        is_local = jnp.logical_and(i == 0, core == cc)
        return i, home, to, slot, hop, is_local

    def send_chunk(k):
        for cc in range(CORES):
            i, home, to, slot, hop, is_local = r_block(k, cc)

            @pl.when(is_local)
            def _():
                pltpu.make_async_copy(rbuf.at[home], ret.at[slot], ret_sem.at[slot]).start()

            @pl.when(i == 2)
            def _():
                remote(rbuf.at[home], relay.at[hop], ret_send.at[home], relay_sem.at[hop], to).start()

            @pl.when(jnp.logical_and(i != 2, jnp.logical_not(is_local)))
            def _():
                remote(rbuf.at[home], ret.at[slot], ret_send.at[home], ret_sem.at[slot], to).start()

    def relay_msg(j, way):
        hb = wrap(my_b + j)
        slot = (hb * side + wrap(my_a - 1 + 2 * way)) * CORES + way
        hop = hb * 2 + way
        return hop, remote(relay.at[hop], ret.at[slot], relay_send.at[hop], ret_sem.at[slot], plane(1 - 2 * way, 0))

    def hand_on(k):
        dx, dy = ORDER[k]
        i = jnp.where(turn == 0, dx, dy)
        j = jnp.where(turn == 0, dy, dx)

        @pl.when(i == 2)
        def _():
            for way in range(2):
                hop, msg = relay_msg(j, way)
                landed(relay.at[hop], relay_sem.at[hop])
                msg.start()

    slot_iota = lax.broadcasted_iota(jnp.int32, (cap, tok_dev), 0)
    slot_iota_f = slot_iota.astype(F32)
    for c in wcopies:
        c.wait()

    def chunk(k, carry):
        @pl.when(k > 0)
        def _():
            send_chunk(k - 1)

        for at, evs in EVENTS.items():
            @pl.when(k == at)
            def _(evs=evs):
                for i, j in evs:
                    event(i, j)

        for at, steps in RELAY.items():
            @pl.when(k == at)
            def _(steps=steps):
                for n in steps:
                    hand_on(n)

        slot = k % 2
        for c in loads(k):
            c.wait()

        @pl.when(k + 1 < n_chip)
        def _():
            for c in loads(k + 1):
                c.start()

        q = chip_at(k)
        landed(tokens.at[q * CORES + 1 - core], tok_sem.at[q * CORES + 1 - core, 0])

        d_parts = []
        for cc in range(CORES):
            home = q * CORES + cc
            landed(tabs.at[home], tab_sem.at[home])
            tab = tabs[home]
            pick = tab[0:1, :] == slot_iota_f
            gate = jnp.sum(jnp.where(pick, tab[1:2, :], 0.0), axis=1, keepdims=True)
            rows = dot(pick.astype(F32).astype(BF16), tokens[home], NN)
            d_parts.append((gate * rows).astype(BF16))
        d = jnp.concatenate(d_parts, axis=0)
        da = dot(d, wd[...], NT).astype(BF16).astype(F32)
        h1 = hgb[slot].astype(F32)
        h3 = hub[slot].astype(F32)
        g = jax.nn.sigmoid(h1)
        s = h1 * g
        act = (s * h3).astype(BF16)
        dh1 = (da * h3 * g * (1.0 + h1 * (1.0 - g))).astype(BF16)
        dh3 = (da * s).astype(BF16)
        dh = jnp.concatenate([dh1, dh3], axis=1)
        r = dot(dh, wgu[...], NT).astype(BF16)
        for cc in range(CORES):
            rbuf[q * CORES + cc] = r[cc * cap:(cc + 1) * cap]
        x = xb[slot]
        gwg_ref[...] += dot(x, dh1, TN)
        gwu_ref[...] += dot(x, dh3, TN)
        gwd_ref[...] += dot(act, d, TN)
        return carry

    lax.fori_loop(0, n_chip, chunk, 0)
    send_chunk(jnp.int32(n_chip - 1))

    n_run = crow // top_k
    n_step = tok_dev // n_run

    def y_load(m):
        return pltpu.make_async_copy(y_ref.at[pl.ds(pl.multiple_of(m * crow, crow), crow)], xb.at[m % 2], load_sem.at[0, m % 2])

    y_load(0).start()
    lane = lax.broadcasted_iota(jnp.int32, (crow, tok_dev), 1)
    token_of = lax.broadcasted_iota(jnp.int32, (crow, tok_dev), 0) // top_k
    gg_ref[...] = jnp.zeros_like(gg_ref)

    def gate_grad(m, carry):
        y_load(m).wait()

        @pl.when(m + 1 < n_step)
        def _():
            y_load(m + 1).start()

        gy = tokens[me, pl.ds(pl.multiple_of(m * n_run, n_run), n_run), :].astype(F32)
        gy = jnp.broadcast_to(gy[:, None, :], (n_run, top_k, model_dim)).reshape(crow, model_dim)
        col = jnp.sum(xb[m % 2].astype(F32) * gy, axis=1, keepdims=True)
        put = jnp.where(lane == token_of + m * n_run, col, 0.0)
        gg_ref[...] += jnp.sum(put.reshape(n_run, top_k, tok_dev), axis=0)
        return carry

    for k in TAIL_RELAY[0]:
        hand_on(k)
    lax.fori_loop(0, n_step, gate_grad, 0)
    for k in TAIL_RELAY[1]:
        hand_on(k)

    def add_rows(n, carry):
        j = lut(n, LINES)
        hb = wrap(my_b + j)

        @pl.when(j != 0)
        def _():
            landed(mids.at[hb], meta_sem.at[hb, 0])
            landed(mslots.at[hb], meta_sem.at[hb, 1])

        h_ids = mids[hb]
        h_slots = mslots[hb]
        picks = []
        for sa in range(side):
            for ce in range(CORES):
                x = (1 - turn) * sa + turn * my_b
                y = (1 - turn) * my_b + turn * sa
                row = jnp.max(jnp.where(h_ids == (y * side + x) * CORES + ce, h_slots, -1), axis=0, keepdims=True)
                picks.append((row == slot_iota).astype(F32).astype(BF16))
        pick = jnp.concatenate(picks, axis=0)

        @pl.when(n == 1)
        def _():
            for c in hop_msgs():
                c.start()

        for sa in range(side):
            for ce in range(CORES):
                slot = (hb * side + sa) * CORES + ce
                landed(ret.at[slot], ret_sem.at[slot])
        rows = ret[pl.ds(hb * side * CORES, side * CORES)].reshape(side * CORES * cap, model_dim)
        part[lut(n, [PART[v] for v in LINES])] = dot(pick, rows, TN)
        return carry

    def hop_msgs():
        return [
            remote(part.at[0, pl.ds(0, half)], hop_in.at[0], part_send.at[0], hop_sem.at[0], plane(0, 1)),
            remote(part.at[0, pl.ds(half, half)], hop_in.at[1], part_send.at[1], hop_sem.at[1], plane(0, -1)),
        ]

    def fin_msgs():
        return [
            remote(part.at[1 + n, pl.ds(h * half, half)], fin.at[n, pl.ds(h * half, half)], part_send.at[2 + 2 * n + h], fin_sem.at[n, h], plane(0, 1 - 2 * n))
            for n in range(2)
            for h in range(2)
        ]

    fins = fin_msgs()
    lax.fori_loop(0, len(LINES), add_rows, 0)
    fins[2].start()
    for what in sends:
        forward_msg(*what).wait_send()
    for what in pairs:
        pair_msg(*what).wait_send()
    fins[1].start()
    landed(hop_in.at[0], hop_sem.at[0])
    part[1, pl.ds(0, half)] += hop_in[0]
    landed(hop_in.at[1], hop_sem.at[1])
    part[2, pl.ds(half, half)] += hop_in[1]

    def tab_done(i, carry):
        tab_msg(i).wait_send()
        return carry

    lax.fori_loop(0, n_dev - 1, tab_done, 0)
    fins[0].start()
    fins[3].start()
    for c in meta_msgs() + hop_msgs():
        c.wait_send()

    def ret_done(k, carry):
        for cc in range(CORES):
            i, home, to, slot, hop, is_local = r_block(k, cc)

            @pl.when(jnp.logical_not(is_local))
            def _():
                remote(rbuf.at[home], ret.at[slot], ret_send.at[home], ret_sem.at[slot], to).wait_send()
        return carry

    lax.fori_loop(0, n_chip, ret_done, 0)
    for j in (0, 1, -1, 2):
        for way in range(2):
            relay_msg(j, way)[1].wait_send()
    for n, h in ((0, 1), (1, 0), (0, 0), (1, 1)):
        rows = pl.ds(h * half, half)
        landed(fin.at[n, rows], fin_sem.at[n, h])
        if (n, h) == (0, 0):
            gx_ref[rows] = (part[3, rows] + fin[0, rows] + fin[1, rows]).astype(gx_ref.dtype)
    rows = pl.ds(half, half)
    gx_ref[rows] = (part[3, rows] + fin[0, rows] + fin[1, rows]).astype(gx_ref.dtype)
    for c in fins:
        c.wait_send()


def write_out(*refs):
    n = len(refs) // 2
    sems = refs[-1]
    copies = [pltpu.make_async_copy(refs[i], refs[n + i], sems.at[i]) for i in range(n)]
    for c in copies:
        c.start()
    for c in copies:
        c.wait()


def solution(mesh):
    n_dev = mesh.shape["ep"]
    side = math.isqrt(n_dev // CORES)
    rows_spec = P(("dp", "ep"), None)
    cube_spec = P(("dp", "ep"), None, None)
    weight_spec = P("ep", None, None)

    def local_step(grad_y, gate_vals, topk_idx, slot_ids, pair_counts, y_routed, x_disp, h_gate, h_up, w_gate, w_up, w_down):
        assert w_gate.shape[0] == 1
        assert side * side * CORES == n_dev and len(ORDER) == side * side
        cap = x_disp.shape[1] // n_dev
        tok_dev, model_dim = grad_y.shape
        ffn = w_gate.shape[2]
        crow = CORES * cap
        n_chip = side * side
        top_k = topk_idx.shape[1]
        vmem = pl.BlockSpec(memory_space=pltpu.VMEM)
        anym = pl.BlockSpec(memory_space=pl.ANY)
        dma = pltpu.SemaphoreType.DMA
        results = pl.pallas_call(
            functools.partial(kernel, n_dev, side),
            out_shape=(
                pltpu.VMEM((tok_dev, model_dim), BF16),
                pltpu.VMEM((top_k, tok_dev), F32),
                pltpu.VMEM((model_dim, ffn), F32),
                pltpu.VMEM((model_dim, ffn), F32),
                pltpu.VMEM((ffn, model_dim), F32),
            ),
            in_specs=[anym] * 12,
            out_specs=(vmem,) * 5,
            scratch_shapes=[
                pltpu.VMEM((n_dev, tok_dev, model_dim), BF16),
                pltpu.VMEM((n_dev, 2, tok_dev), F32),
                pltpu.VMEM((n_dev, 2, tok_dev), F32),
                pltpu.VMEM((side, top_k, tok_dev), jnp.int32),
                pltpu.VMEM((side, top_k, tok_dev), jnp.int32),
                pltpu.VMEM((n_dev, cap, model_dim), BF16),
                pltpu.VMEM((n_dev, cap, model_dim), BF16),
                pltpu.VMEM((2 * side, cap, model_dim), BF16),
                pltpu.VMEM((4, tok_dev, model_dim), F32),
                pltpu.VMEM((2, tok_dev // 2, model_dim), F32),
                pltpu.VMEM((2, tok_dev, model_dim), F32),
                pltpu.VMEM((model_dim, 2 * ffn), BF16),
                pltpu.VMEM((ffn, model_dim), BF16),
                pltpu.VMEM((2, crow, model_dim), BF16),
                pltpu.VMEM((2, crow, ffn), BF16),
                pltpu.VMEM((2, crow, ffn), BF16),
                dma((n_dev, 2)),
                dma((n_dev,)),
                dma((side, 2)),
                dma((n_dev,)),
                dma((2 * side,)),
                dma((2,)),
                dma((2, 2)),
                dma((64,)),
                dma((n_chip,)),
                dma((n_dev,)),
                dma((3, 2)),
                dma((n_dev,)),
                dma((2 * side,)),
                dma((6,)),
                dma((3, 2)),
                dma((3,)),
                pltpu.SemaphoreType.REGULAR((side - 1,)),
                pltpu.VMEM((top_k, tok_dev), F32),
                pltpu.SMEM(pair_counts.shape, jnp.int32),
                dma((5,)),
            ],
            compiler_params=pltpu.CompilerParams(collective_id=0, has_side_effects=True, vmem_limit_bytes=58720256),
            name="moe_bwd",
        )(grad_y, topk_idx.T, slot_ids.T, gate_vals.T, pair_counts, y_routed.reshape(tok_dev * top_k, model_dim), x_disp[0], h_gate[0], h_up[0], w_gate[0], w_up[0], w_down[0])
        gx, gg, gwg, gwu, gwd = pl.pallas_call(
            write_out,
            out_shape=tuple(jax.ShapeDtypeStruct(r.shape, r.dtype) for r in results),
            in_specs=[anym] * len(results),
            out_specs=(anym,) * len(results),
            scratch_shapes=[dma((len(results),))],
            compiler_params=pltpu.CompilerParams(vmem_limit_bytes=1048576),
            name="write_out",
        )(*results)
        return gx, gg.T, gwg[None], gwu[None], gwd[None]

    return jax.shard_map(local_step, mesh=mesh, in_specs=(rows_spec, rows_spec, rows_spec, rows_spec, rows_spec, cube_spec, cube_spec, cube_spec, cube_spec, weight_spec, weight_spec, weight_spec), out_specs=(rows_spec, rows_spec, cube_spec, cube_spec, cube_spec), check_vma=False)
```

```python
import functools
import math

import jax
import jax.numpy as jnp
from jax import lax
from jax.experimental import pallas as pl
from jax.experimental.pallas import tpu as pltpu
from jax.sharding import PartitionSpec as P

MESH = pl.DeviceIdType.MESH
CORES = 2
BF16, F32 = jnp.bfloat16, jnp.float32

ORDER = ((1, 0), (0, 0), (-1, 0), (1, 1), (0, 2), (0, -1), (2, 0), (0, 1), (-1, -1), (1, -1), (-1, 1), (2, 1), (2, -1), (2, 2), (1, 2), (-1, 2))
EVENTS = {
    0: ((1, 0), (-1, 0), (0, 1), (0, -1)),
    1: ((1, -1), (1, 1)),
    2: ((2, 0),),
    4: ((0, 2), (-1, -1)),
    6: ((-1, 1), (2, 1)),
    7: ((1, 2),),
    9: ((2, -1),),
    11: ((-1, 2),),
    13: ((2, 2),),
}
FLIP = 1
RELAY = {10: (4,), 13: (6,), 15: (11,)}
TAIL_RELAY = (13, 14), (15, 12)

LINES = (0, 2, 1, -1)
PART = {2: 0, 1: 1, -1: 2, 0: 3}

NN = (((1,), (0,)), ((), ()))
NT = (((1,), (1,)), ((), ()))
TN = (((0,), (0,)), ((), ()))


def dot(a, b, dims):
    return lax.dot_general(a, b, dims, preferred_element_type=F32)


def lut(k, vals):
    out = vals[0]
    for i, v in enumerate(vals):
        if i:
            out = jnp.where(k == i, v, out)
    return out


def kernel(n_dev, side, gy_ref, ids_ref, slots_ref, gates_ref, pc_ref, y_ref, x_ref, hg_ref, hu_ref, wg_ref, wu_ref, wd_ref,
           gx_ref, gg_ref, gwg_ref, gwu_ref, gwd_ref,
           tokens, stab, tabs, mids, mslots, rbuf, ret, relay, part, hop_in, fin, wgu, wd, xb, hgb, hub,
           tok_sem, tab_sem, meta_sem, ret_sem, relay_sem, hop_sem, fin_sem,
           ag_send, pair_send, tab_send, meta_send, ret_send, relay_send, part_send, load_sem, w_sem, round_sem, gates, counts, in_sem):
    me = lax.axis_index("ep")
    core = me % CORES
    mx = (me // CORES) % side
    my = me // (CORES * side)
    turn = 1 - core if FLIP else core
    my_a = (1 - turn) * mx + turn * my
    my_b = (1 - turn) * my + turn * mx
    tok_dev, model_dim = gy_ref.shape
    top_k = ids_ref.shape[0]
    ffn = wg_ref.shape[1]
    cap = rbuf.shape[1]
    half = tok_dev // 2
    n_chip = side * side
    crow = CORES * cap
    partner = me + 1 - 2 * core

    def wrap(v):
        return (v + 2 * side) % side

    def device(x, y, c):
        return (wrap(y) * side + wrap(x)) * CORES + c

    def plane(a, b):
        return device(mx + (1 - turn) * a + turn * b, my + turn * a + (1 - turn) * b, core)

    def remote(src, dst, send_sem, recv_sem, to):
        return pltpu.make_async_remote_copy(src_ref=src, dst_ref=dst, send_sem=send_sem, recv_sem=recv_sem, device_id={"ep": to}, device_id_type=MESH)

    def landed(ref, sem):
        pltpu.make_async_copy(ref, ref, sem).wait()

    peers = [partner] + [device(mx + dx, my + dy, c) for dx, dy in ((1, 0), (-1, 0), (0, 1), (0, -1)) for c in range(CORES)]

    def tell(sem):
        for to in peers:
            pl.semaphore_signal(sem, inc=1, device_id={"ep": to}, device_id_type=MESH)

    barrier = pltpu.get_barrier_semaphore()
    tell(barrier)

    own_copies = [
        pltpu.make_async_copy(gy_ref, tokens.at[me], in_sem.at[0]),
        pltpu.make_async_copy(ids_ref, mids.at[my_b], in_sem.at[1]),
        pltpu.make_async_copy(slots_ref, mslots.at[my_b], in_sem.at[2]),
        pltpu.make_async_copy(gates_ref, gates, in_sem.at[3]),
        pltpu.make_async_copy(pc_ref, counts, in_sem.at[4]),
    ]
    for c in own_copies:
        c.start()
    wcopies = [
        pltpu.make_async_copy(wd_ref, wd, w_sem.at[0]),
        pltpu.make_async_copy(wg_ref, wgu.at[:, pl.ds(0, ffn)], w_sem.at[1]),
        pltpu.make_async_copy(wu_ref, wgu.at[:, pl.ds(ffn, ffn)], w_sem.at[2]),
    ]
    for c in wcopies:
        c.start()

    def offset(k, axis):
        return lut(k, [o[axis] for o in ORDER])

    def chip_at(k):
        return wrap(my + offset(k, 1)) * side + wrap(mx + offset(k, 0))

    def loads(k):
        q = chip_at(k)
        slot = k % 2
        rows = pl.ds(pl.multiple_of(q * crow, crow), crow)
        return [
            pltpu.make_async_copy(x_ref.at[rows], xb.at[slot], load_sem.at[0, slot]),
            pltpu.make_async_copy(hg_ref.at[rows], hgb.at[slot], load_sem.at[1, slot]),
            pltpu.make_async_copy(hu_ref.at[rows], hub.at[slot], load_sem.at[2, slot]),
        ]

    pl.semaphore_wait(barrier, len(peers))
    own_copies[0].wait()

    sends, pairs = [], []

    def block(src, h):
        return tokens.at[src, pl.ds(h * half, half)]

    def forward_msg(n, i, j, h, a, b):
        src = plane(i, j)
        return remote(block(src, h), block(src, h), ag_send.at[n], tok_sem.at[src, h], plane(a, b))

    def forward(*what):
        what = (len(sends), *what)
        sends.append(what)
        forward_msg(*what).start()

    def pair_msg(n, i, j):
        src = plane(i, j)
        return remote(tokens.at[src], tokens.at[src], pair_send.at[n], tok_sem.at[src, 0], partner)

    def to_partner(i, j):
        what = (len(pairs), i, j)
        pairs.append(what)
        pair_msg(*what).start()

    def arrived(src, h):
        landed(block(src, h), tok_sem.at[src, h])

    to_partner(0, 0)

    def tab_msg(i):
        to = (me + 1 + i) % n_dev
        return remote(stab.at[to], tabs.at[me], tab_send.at[i], tab_sem.at[me], to)

    def tab_start(i, carry):
        tab_msg(i).start()
        return carry

    for n in range(2):
        for a, b, h in ((1, 0, n), (-1, 0, 1 - n), (0, 1, n), (0, -1, 1 - n)):
            forward(0, 0, h, a, b)

    tell(round_sem.at[0])
    for c in loads(0):
        c.start()

    for c in own_copies[1:]:
        c.wait()
    ids = mids[my_b]
    slots = mslots[my_b]

    def table(e, carry):
        hit = ids == e
        slot = jnp.max(jnp.where(hit, slots, -1), axis=0, keepdims=True)
        slot = jnp.where(slot < counts[0, e], slot, -1)
        gate = jnp.sum(jnp.where(hit, gates[...], 0.0), axis=0, keepdims=True)
        stab[e] = jnp.concatenate([slot.astype(F32), gate], axis=0)
        return carry

    lax.fori_loop(0, n_dev, table, 0)
    gwg_ref[...] = jnp.zeros_like(gwg_ref)
    gwu_ref[...] = jnp.zeros_like(gwu_ref)
    gwd_ref[...] = jnp.zeros_like(gwd_ref)

    for n in range(side - 1):
        if n:
            tell(round_sem.at[n])
        pl.semaphore_wait(round_sem.at[n], len(peers))
    lax.fori_loop(0, n_dev - 1, tab_start, 0)
    tab_copy = pltpu.make_async_copy(stab.at[me], tabs.at[me], tab_sem.at[me])
    tab_copy.start()
    def meta_msgs():
        out = []
        for n, j in enumerate((1, -1, 2)):
            out.append(remote(mids.at[my_b], mids.at[my_b], meta_send.at[n, 0], meta_sem.at[my_b, 0], plane(0, j)))
            out.append(remote(mslots.at[my_b], mslots.at[my_b], meta_send.at[n, 1], meta_sem.at[my_b, 1], plane(0, j)))
        return out

    for c in meta_msgs():
        c.start()

    def event(i, j):
        src = plane(i, j)
        first = 1 if (i == 1 and j == 0) or j == 1 else 0
        for n, h in enumerate((first, 1 - first)):
            arrived(src, h)
            if j == 0:
                if n == 0 and abs(i) == 1:
                    forward(i, j, h, -i, 0)
                forward(i, j, h, 0, 1)
                forward(i, j, h, 0, -1)
            elif n == 0 and abs(j) == 1:
                forward(i, j, h, 0, -j)
        to_partner(i, j)

    def r_block(k, cc):
        axis = 1 - cc if FLIP else cc
        i, j = offset(k, axis), offset(k, 1 - axis)
        a, b = (mx, my) if axis == 0 else (my, mx)
        hb = wrap(b + j)
        home = chip_at(k) * CORES + cc
        step = jnp.where(i == 2, 1 - 2 * core, i)
        to = device(mx + step, my, cc) if axis == 0 else device(mx, my + step, cc)
        slot = (hb * side + a) * CORES + core
        hop = hb * 2 + core
        is_local = jnp.logical_and(i == 0, core == cc)
        return i, home, to, slot, hop, is_local

    def send_chunk(k):
        for cc in range(CORES):
            i, home, to, slot, hop, is_local = r_block(k, cc)

            @pl.when(is_local)
            def _():
                pltpu.make_async_copy(rbuf.at[home], ret.at[slot], ret_sem.at[slot]).start()

            @pl.when(i == 2)
            def _():
                remote(rbuf.at[home], relay.at[hop], ret_send.at[home], relay_sem.at[hop], to).start()

            @pl.when(jnp.logical_and(i != 2, jnp.logical_not(is_local)))
            def _():
                remote(rbuf.at[home], ret.at[slot], ret_send.at[home], ret_sem.at[slot], to).start()

    def relay_msg(j, way):
        hb = wrap(my_b + j)
        slot = (hb * side + wrap(my_a - 1 + 2 * way)) * CORES + way
        hop = hb * 2 + way
        return hop, remote(relay.at[hop], ret.at[slot], relay_send.at[hop], ret_sem.at[slot], plane(1 - 2 * way, 0))

    def hand_on(k):
        dx, dy = ORDER[k]
        i = jnp.where(turn == 0, dx, dy)
        j = jnp.where(turn == 0, dy, dx)

        @pl.when(i == 2)
        def _():
            for way in range(2):
                hop, msg = relay_msg(j, way)
                landed(relay.at[hop], relay_sem.at[hop])
                msg.start()

    slot_iota = lax.broadcasted_iota(jnp.int32, (cap, tok_dev), 0)
    slot_iota_f = slot_iota.astype(F32)
    for c in wcopies:
        c.wait()

    def chunk(k, carry):
        @pl.when(k > 0)
        def _():
            send_chunk(k - 1)

        for at, evs in EVENTS.items():
            @pl.when(k == at)
            def _(evs=evs):
                for i, j in evs:
                    event(i, j)

        for at, steps in RELAY.items():
            @pl.when(k == at)
            def _(steps=steps):
                for n in steps:
                    hand_on(n)

        slot = k % 2
        for c in loads(k):
            c.wait()

        @pl.when(k + 1 < n_chip)
        def _():
            for c in loads(k + 1):
                c.start()

        q = chip_at(k)
        landed(tokens.at[q * CORES + 1 - core], tok_sem.at[q * CORES + 1 - core, 0])

        d_parts = []
        for cc in range(CORES):
            home = q * CORES + cc
            landed(tabs.at[home], tab_sem.at[home])
            tab = tabs[home]
            pick = tab[0:1, :] == slot_iota_f
            gate = jnp.sum(jnp.where(pick, tab[1:2, :], 0.0), axis=1, keepdims=True)
            rows = dot(pick.astype(F32).astype(BF16), tokens[home], NN)
            d_parts.append((gate * rows).astype(BF16))
        d = jnp.concatenate(d_parts, axis=0)
        da = dot(d, wd[...], NT).astype(BF16).astype(F32)
        h1 = hgb[slot].astype(F32)
        h3 = hub[slot].astype(F32)
        g = jax.nn.sigmoid(h1)
        s = h1 * g
        act = (s * h3).astype(BF16)
        dh1 = (da * h3 * g * (1.0 + h1 * (1.0 - g))).astype(BF16)
        dh3 = (da * s).astype(BF16)
        dh = jnp.concatenate([dh1, dh3], axis=1)
        r = dot(dh, wgu[...], NT).astype(BF16)
        for cc in range(CORES):
            rbuf[q * CORES + cc] = r[cc * cap:(cc + 1) * cap]
        x = xb[slot]
        gwg_ref[...] += dot(x, dh1, TN)
        gwu_ref[...] += dot(x, dh3, TN)
        gwd_ref[...] += dot(act, d, TN)
        return carry

    lax.fori_loop(0, n_chip, chunk, 0)
    send_chunk(jnp.int32(n_chip - 1))

    n_run = crow // top_k
    n_step = tok_dev // n_run

    def y_load(m):
        return pltpu.make_async_copy(y_ref.at[pl.ds(pl.multiple_of(m * crow, crow), crow)], xb.at[m % 2], load_sem.at[0, m % 2])

    y_load(0).start()
    lane = lax.broadcasted_iota(jnp.int32, (crow, tok_dev), 1)
    token_of = lax.broadcasted_iota(jnp.int32, (crow, tok_dev), 0) // top_k
    gg_ref[...] = jnp.zeros_like(gg_ref)

    def gate_grad(m, carry):
        y_load(m).wait()

        @pl.when(m + 1 < n_step)
        def _():
            y_load(m + 1).start()

        gy = tokens[me, pl.ds(pl.multiple_of(m * n_run, n_run), n_run), :].astype(F32)
        gy = jnp.broadcast_to(gy[:, None, :], (n_run, top_k, model_dim)).reshape(crow, model_dim)
        col = jnp.sum(xb[m % 2].astype(F32) * gy, axis=1, keepdims=True)
        put = jnp.where(lane == token_of + m * n_run, col, 0.0)
        gg_ref[...] += jnp.sum(put.reshape(n_run, top_k, tok_dev), axis=0)
        return carry

    for k in TAIL_RELAY[0]:
        hand_on(k)
    lax.fori_loop(0, n_step, gate_grad, 0)
    for k in TAIL_RELAY[1]:
        hand_on(k)

    def add_rows(n, carry):
        j = lut(n, LINES)
        hb = wrap(my_b + j)

        @pl.when(j != 0)
        def _():
            landed(mids.at[hb], meta_sem.at[hb, 0])
            landed(mslots.at[hb], meta_sem.at[hb, 1])

        h_ids = mids[hb]
        h_slots = mslots[hb]
        picks = []
        for sa in range(side):
            for ce in range(CORES):
                x = (1 - turn) * sa + turn * my_b
                y = (1 - turn) * my_b + turn * sa
                row = jnp.max(jnp.where(h_ids == (y * side + x) * CORES + ce, h_slots, -1), axis=0, keepdims=True)
                picks.append((row == slot_iota).astype(F32).astype(BF16))
        pick = jnp.concatenate(picks, axis=0)

        @pl.when(n == 2)
        def _():
            for c in hop_msgs():
                c.start()

        for sa in range(side):
            for ce in range(CORES):
                slot = (hb * side + sa) * CORES + ce
                landed(ret.at[slot], ret_sem.at[slot])
        rows = ret[pl.ds(hb * side * CORES, side * CORES)].reshape(side * CORES * cap, model_dim)
        part[lut(n, [PART[v] for v in LINES])] = dot(pick, rows, TN)
        return carry

    def hop_msgs():
        return [
            remote(part.at[0, pl.ds(0, half)], hop_in.at[0], part_send.at[0], hop_sem.at[0], plane(0, 1)),
            remote(part.at[0, pl.ds(half, half)], hop_in.at[1], part_send.at[1], hop_sem.at[1], plane(0, -1)),
        ]

    def fin_msgs():
        return [
            remote(part.at[1 + n, pl.ds(h * half, half)], fin.at[n, pl.ds(h * half, half)], part_send.at[2 + 2 * n + h], fin_sem.at[n, h], plane(0, 1 - 2 * n))
            for n in range(2)
            for h in range(2)
        ]

    fins = fin_msgs()
    lax.fori_loop(0, len(LINES), add_rows, 0)
    fins[1].start()
    for what in sends:
        forward_msg(*what).wait_send()
    for what in pairs:
        pair_msg(*what).wait_send()
    fins[2].start()
    landed(hop_in.at[0], hop_sem.at[0])
    part[1, pl.ds(0, half)] += hop_in[0]
    landed(hop_in.at[1], hop_sem.at[1])
    part[2, pl.ds(half, half)] += hop_in[1]

    def tab_done(i, carry):
        tab_msg(i).wait_send()
        return carry

    lax.fori_loop(0, n_dev - 1, tab_done, 0)
    fins[0].start()
    fins[3].start()
    for c in meta_msgs() + hop_msgs():
        c.wait_send()

    def ret_done(k, carry):
        for cc in range(CORES):
            i, home, to, slot, hop, is_local = r_block(k, cc)

            @pl.when(jnp.logical_not(is_local))
            def _():
                remote(rbuf.at[home], ret.at[slot], ret_send.at[home], ret_sem.at[slot], to).wait_send()
        return carry

    lax.fori_loop(0, n_chip, ret_done, 0)
    for j in (0, 1, -1, 2):
        for way in range(2):
            relay_msg(j, way)[1].wait_send()
    for n, h in ((0, 1), (1, 0), (0, 0), (1, 1)):
        rows = pl.ds(h * half, half)
        landed(fin.at[n, rows], fin_sem.at[n, h])
        if (n, h) == (0, 0):
            gx_ref[rows] = (part[3, rows] + fin[0, rows] + fin[1, rows]).astype(gx_ref.dtype)
    rows = pl.ds(half, half)
    gx_ref[rows] = (part[3, rows] + fin[0, rows] + fin[1, rows]).astype(gx_ref.dtype)
    for c in fins:
        c.wait_send()


def write_out(*refs):
    n = len(refs) // 2
    sems = refs[-1]
    copies = [pltpu.make_async_copy(refs[i], refs[n + i], sems.at[i]) for i in range(n)]
    for c in copies:
        c.start()
    for c in copies:
        c.wait()


def solution(mesh):
    n_dev = mesh.shape["ep"]
    side = math.isqrt(n_dev // CORES)
    rows_spec = P(("dp", "ep"), None)
    cube_spec = P(("dp", "ep"), None, None)
    weight_spec = P("ep", None, None)

    def local_step(grad_y, gate_vals, topk_idx, slot_ids, pair_counts, y_routed, x_disp, h_gate, h_up, w_gate, w_up, w_down):
        assert w_gate.shape[0] == 1
        assert side * side * CORES == n_dev and len(ORDER) == side * side
        cap = x_disp.shape[1] // n_dev
        tok_dev, model_dim = grad_y.shape
        ffn = w_gate.shape[2]
        crow = CORES * cap
        n_chip = side * side
        top_k = topk_idx.shape[1]
        vmem = pl.BlockSpec(memory_space=pltpu.VMEM)
        anym = pl.BlockSpec(memory_space=pl.ANY)
        dma = pltpu.SemaphoreType.DMA
        results = pl.pallas_call(
            functools.partial(kernel, n_dev, side),
            out_shape=(
                pltpu.VMEM((tok_dev, model_dim), BF16),
                pltpu.VMEM((top_k, tok_dev), F32),
                pltpu.VMEM((model_dim, ffn), F32),
                pltpu.VMEM((model_dim, ffn), F32),
                pltpu.VMEM((ffn, model_dim), F32),
            ),
            in_specs=[anym] * 12,
            out_specs=(vmem,) * 5,
            scratch_shapes=[
                pltpu.VMEM((n_dev, tok_dev, model_dim), BF16),
                pltpu.VMEM((n_dev, 2, tok_dev), F32),
                pltpu.VMEM((n_dev, 2, tok_dev), F32),
                pltpu.VMEM((side, top_k, tok_dev), jnp.int32),
                pltpu.VMEM((side, top_k, tok_dev), jnp.int32),
                pltpu.VMEM((n_dev, cap, model_dim), BF16),
                pltpu.VMEM((n_dev, cap, model_dim), BF16),
                pltpu.VMEM((2 * side, cap, model_dim), BF16),
                pltpu.VMEM((4, tok_dev, model_dim), F32),
                pltpu.VMEM((2, tok_dev // 2, model_dim), F32),
                pltpu.VMEM((2, tok_dev, model_dim), F32),
                pltpu.VMEM((model_dim, 2 * ffn), BF16),
                pltpu.VMEM((ffn, model_dim), BF16),
                pltpu.VMEM((2, crow, model_dim), BF16),
                pltpu.VMEM((2, crow, ffn), BF16),
                pltpu.VMEM((2, crow, ffn), BF16),
                dma((n_dev, 2)),
                dma((n_dev,)),
                dma((side, 2)),
                dma((n_dev,)),
                dma((2 * side,)),
                dma((2,)),
                dma((2, 2)),
                dma((64,)),
                dma((n_chip,)),
                dma((n_dev,)),
                dma((3, 2)),
                dma((n_dev,)),
                dma((2 * side,)),
                dma((6,)),
                dma((3, 2)),
                dma((3,)),
                pltpu.SemaphoreType.REGULAR((side - 1,)),
                pltpu.VMEM((top_k, tok_dev), F32),
                pltpu.SMEM(pair_counts.shape, jnp.int32),
                dma((5,)),
            ],
            compiler_params=pltpu.CompilerParams(collective_id=0, has_side_effects=True, vmem_limit_bytes=58720256),
            name="moe_bwd",
        )(grad_y, topk_idx.T, slot_ids.T, gate_vals.T, pair_counts, y_routed.reshape(tok_dev * top_k, model_dim), x_disp[0], h_gate[0], h_up[0], w_gate[0], w_up[0], w_down[0])
        gx, gg, gwg, gwu, gwd = pl.pallas_call(
            write_out,
            out_shape=tuple(jax.ShapeDtypeStruct(r.shape, r.dtype) for r in results),
            in_specs=[anym] * len(results),
            out_specs=(anym,) * len(results),
            scratch_shapes=[dma((len(results),))],
            compiler_params=pltpu.CompilerParams(vmem_limit_bytes=1048576),
            name="write_out",
        )(*results)
        return gx, gg.T, gwg[None], gwu[None], gwd[None]

    return jax.shard_map(local_step, mesh=mesh, in_specs=(rows_spec, rows_spec, rows_spec, rows_spec, rows_spec, cube_spec, cube_spec, cube_spec, cube_spec, weight_spec, weight_spec, weight_spec), out_specs=(rows_spec, rows_spec, cube_spec, cube_spec, cube_spec), check_vma=False)
```

```python
import functools
import math

import jax
import jax.numpy as jnp
from jax import lax
from jax.experimental import pallas as pl
from jax.experimental.pallas import tpu as pltpu
from jax.sharding import PartitionSpec as P

MESH = pl.DeviceIdType.MESH
CORES = 2
BF16, F32 = jnp.bfloat16, jnp.float32

ORDER = ((0, -1), (1, 0), (-1, 0), (0, 0), (1, -1), (0, 1), (-1, 1), (1, 1), (2, 0), (-1, -1), (0, 2), (1, 2), (-1, 2), (2, 2), (2, 1), (2, -1))
EVENTS = {
    0: ((-1, 0), (0, -1), (1, 0), (0, 1)),
    2: ((2, 0), (-1, 1)),
    4: ((0, 2), (1, -1), (-1, -1)),
    5: ((1, 1),),
    6: ((2, -1),),
    9: ((2, 1),),
    10: ((1, 2),),
    12: ((2, 2), (-1, 2)),
}
FLIP = 0
RELAY = {15: (11,)}
TAIL_RELAY = (13, 10, 8, 14), (15, 12)

LINES = (2, 0, -1, 1)
PART = {2: 0, 1: 1, -1: 2, 0: 3}

NN = (((1,), (0,)), ((), ()))
NT = (((1,), (1,)), ((), ()))
TN = (((0,), (0,)), ((), ()))


def dot(a, b, dims):
    return lax.dot_general(a, b, dims, preferred_element_type=F32)


def lut(k, vals):
    out = vals[0]
    for i, v in enumerate(vals):
        if i:
            out = jnp.where(k == i, v, out)
    return out


def kernel(n_dev, side, gy_ref, ids_ref, slots_ref, gates_ref, pc_ref, y_ref, x_ref, hg_ref, hu_ref, wg_ref, wu_ref, wd_ref,
           gx_ref, gg_ref, gwg_ref, gwu_ref, gwd_ref,
           tokens, stab, tabs, mids, mslots, rbuf, ret, relay, part, hop_in, fin, wgu, wd, xb, hgb, hub,
           tok_sem, tab_sem, meta_sem, ret_sem, relay_sem, hop_sem, fin_sem,
           ag_send, pair_send, tab_send, meta_send, ret_send, relay_send, part_send, load_sem, w_sem, round_sem, gates, counts, in_sem):
    me = lax.axis_index("ep")
    core = me % CORES
    mx = (me // CORES) % side
    my = me // (CORES * side)
    turn = 1 - core if FLIP else core
    my_a = (1 - turn) * mx + turn * my
    my_b = (1 - turn) * my + turn * mx
    tok_dev, model_dim = gy_ref.shape
    top_k = ids_ref.shape[0]
    ffn = wg_ref.shape[1]
    cap = rbuf.shape[1]
    half = tok_dev // 2
    n_chip = side * side
    crow = CORES * cap
    partner = me + 1 - 2 * core

    def wrap(v):
        return (v + 2 * side) % side

    def device(x, y, c):
        return (wrap(y) * side + wrap(x)) * CORES + c

    def plane(a, b):
        return device(mx + (1 - turn) * a + turn * b, my + turn * a + (1 - turn) * b, core)

    def remote(src, dst, send_sem, recv_sem, to):
        return pltpu.make_async_remote_copy(src_ref=src, dst_ref=dst, send_sem=send_sem, recv_sem=recv_sem, device_id={"ep": to}, device_id_type=MESH)

    def landed(ref, sem):
        pltpu.make_async_copy(ref, ref, sem).wait()

    peers = [partner] + [device(mx + dx, my + dy, c) for dx, dy in ((1, 0), (-1, 0), (0, 1), (0, -1)) for c in range(CORES)]

    def tell(sem):
        for to in peers:
            pl.semaphore_signal(sem, inc=1, device_id={"ep": to}, device_id_type=MESH)

    barrier = pltpu.get_barrier_semaphore()
    tell(barrier)

    own_copies = [
        pltpu.make_async_copy(gy_ref, tokens.at[me], in_sem.at[0]),
        pltpu.make_async_copy(ids_ref, mids.at[my_b], in_sem.at[1]),
        pltpu.make_async_copy(slots_ref, mslots.at[my_b], in_sem.at[2]),
        pltpu.make_async_copy(gates_ref, gates, in_sem.at[3]),
        pltpu.make_async_copy(pc_ref, counts, in_sem.at[4]),
    ]
    for c in own_copies:
        c.start()
    wcopies = [
        pltpu.make_async_copy(wd_ref, wd, w_sem.at[0]),
        pltpu.make_async_copy(wg_ref, wgu.at[:, pl.ds(0, ffn)], w_sem.at[1]),
        pltpu.make_async_copy(wu_ref, wgu.at[:, pl.ds(ffn, ffn)], w_sem.at[2]),
    ]
    for c in wcopies:
        c.start()

    def offset(k, axis):
        return lut(k, [o[axis] for o in ORDER])

    def chip_at(k):
        return wrap(my + offset(k, 1)) * side + wrap(mx + offset(k, 0))

    def loads(k):
        q = chip_at(k)
        slot = k % 2
        rows = pl.ds(pl.multiple_of(q * crow, crow), crow)
        return [
            pltpu.make_async_copy(x_ref.at[rows], xb.at[slot], load_sem.at[0, slot]),
            pltpu.make_async_copy(hg_ref.at[rows], hgb.at[slot], load_sem.at[1, slot]),
            pltpu.make_async_copy(hu_ref.at[rows], hub.at[slot], load_sem.at[2, slot]),
        ]

    pl.semaphore_wait(barrier, len(peers))
    own_copies[0].wait()

    sends, pairs = [], []

    def block(src, h):
        return tokens.at[src, pl.ds(h * half, half)]

    def forward_msg(n, i, j, h, a, b):
        src = plane(i, j)
        return remote(block(src, h), block(src, h), ag_send.at[n], tok_sem.at[src, h], plane(a, b))

    def forward(*what):
        what = (len(sends), *what)
        sends.append(what)
        forward_msg(*what).start()

    def pair_msg(n, i, j):
        src = plane(i, j)
        return remote(tokens.at[src], tokens.at[src], pair_send.at[n], tok_sem.at[src, 0], partner)

    def to_partner(i, j):
        what = (len(pairs), i, j)
        pairs.append(what)
        pair_msg(*what).start()

    def arrived(src, h):
        landed(block(src, h), tok_sem.at[src, h])

    to_partner(0, 0)

    def tab_msg(i):
        to = (me + 1 + i) % n_dev
        return remote(stab.at[to], tabs.at[me], tab_send.at[i], tab_sem.at[me], to)

    def tab_start(i, carry):
        tab_msg(i).start()
        return carry

    for n in range(2):
        for a, b, h in ((1, 0, n), (-1, 0, 1 - n), (0, 1, n), (0, -1, 1 - n)):
            forward(0, 0, h, a, b)

    tell(round_sem.at[0])
    for c in loads(0):
        c.start()

    for c in own_copies[1:]:
        c.wait()
    ids = mids[my_b]
    slots = mslots[my_b]

    def table(e, carry):
        hit = ids == e
        slot = jnp.max(jnp.where(hit, slots, -1), axis=0, keepdims=True)
        slot = jnp.where(slot < counts[0, e], slot, -1)
        gate = jnp.sum(jnp.where(hit, gates[...], 0.0), axis=0, keepdims=True)
        stab[e] = jnp.concatenate([slot.astype(F32), gate], axis=0)
        return carry

    lax.fori_loop(0, n_dev, table, 0)
    gwg_ref[...] = jnp.zeros_like(gwg_ref)
    gwu_ref[...] = jnp.zeros_like(gwu_ref)
    gwd_ref[...] = jnp.zeros_like(gwd_ref)

    for n in range(side - 1):
        if n:
            tell(round_sem.at[n])
        pl.semaphore_wait(round_sem.at[n], len(peers))
    lax.fori_loop(0, n_dev - 1, tab_start, 0)
    tab_copy = pltpu.make_async_copy(stab.at[me], tabs.at[me], tab_sem.at[me])
    tab_copy.start()
    def meta_msgs():
        out = []
        for n, j in enumerate((1, -1, 2)):
            out.append(remote(mids.at[my_b], mids.at[my_b], meta_send.at[n, 0], meta_sem.at[my_b, 0], plane(0, j)))
            out.append(remote(mslots.at[my_b], mslots.at[my_b], meta_send.at[n, 1], meta_sem.at[my_b, 1], plane(0, j)))
        return out

    for c in meta_msgs():
        c.start()

    def event(i, j):
        src = plane(i, j)
        first = 1 if (i == 1 and j == 0) or j == 1 else 0
        for n, h in enumerate((first, 1 - first)):
            arrived(src, h)
            if j == 0:
                if n == 0 and abs(i) == 1:
                    forward(i, j, h, -i, 0)
                forward(i, j, h, 0, 1)
                forward(i, j, h, 0, -1)
            elif n == 0 and abs(j) == 1:
                forward(i, j, h, 0, -j)
        to_partner(i, j)

    def r_block(k, cc):
        axis = 1 - cc if FLIP else cc
        i, j = offset(k, axis), offset(k, 1 - axis)
        a, b = (mx, my) if axis == 0 else (my, mx)
        hb = wrap(b + j)
        home = chip_at(k) * CORES + cc
        step = jnp.where(i == 2, 1 - 2 * core, i)
        to = device(mx + step, my, cc) if axis == 0 else device(mx, my + step, cc)
        slot = (hb * side + a) * CORES + core
        hop = hb * 2 + core
        is_local = jnp.logical_and(i == 0, core == cc)
        return i, home, to, slot, hop, is_local

    def send_chunk(k):
        for cc in range(CORES):
            i, home, to, slot, hop, is_local = r_block(k, cc)

            @pl.when(is_local)
            def _():
                pltpu.make_async_copy(rbuf.at[home], ret.at[slot], ret_sem.at[slot]).start()

            @pl.when(i == 2)
            def _():
                remote(rbuf.at[home], relay.at[hop], ret_send.at[home], relay_sem.at[hop], to).start()

            @pl.when(jnp.logical_and(i != 2, jnp.logical_not(is_local)))
            def _():
                remote(rbuf.at[home], ret.at[slot], ret_send.at[home], ret_sem.at[slot], to).start()

    def relay_msg(j, way):
        hb = wrap(my_b + j)
        slot = (hb * side + wrap(my_a - 1 + 2 * way)) * CORES + way
        hop = hb * 2 + way
        return hop, remote(relay.at[hop], ret.at[slot], relay_send.at[hop], ret_sem.at[slot], plane(1 - 2 * way, 0))

    def hand_on(k):
        dx, dy = ORDER[k]
        i = jnp.where(turn == 0, dx, dy)
        j = jnp.where(turn == 0, dy, dx)

        @pl.when(i == 2)
        def _():
            for way in range(2):
                hop, msg = relay_msg(j, way)
                landed(relay.at[hop], relay_sem.at[hop])
                msg.start()

    slot_iota = lax.broadcasted_iota(jnp.int32, (cap, tok_dev), 0)
    slot_iota_f = slot_iota.astype(F32)
    for c in wcopies:
        c.wait()

    def chunk(k, carry):
        @pl.when(k > 0)
        def _():
            send_chunk(k - 1)

        for at, evs in EVENTS.items():
            @pl.when(k == at)
            def _(evs=evs):
                for i, j in evs:
                    event(i, j)

        for at, steps in RELAY.items():
            @pl.when(k == at)
            def _(steps=steps):
                for n in steps:
                    hand_on(n)

        slot = k % 2
        for c in loads(k):
            c.wait()

        @pl.when(k + 1 < n_chip)
        def _():
            for c in loads(k + 1):
                c.start()

        q = chip_at(k)
        landed(tokens.at[q * CORES + 1 - core], tok_sem.at[q * CORES + 1 - core, 0])

        d_parts = []
        for cc in range(CORES):
            home = q * CORES + cc
            landed(tabs.at[home], tab_sem.at[home])
            tab = tabs[home]
            pick = tab[0:1, :] == slot_iota_f
            gate = jnp.sum(jnp.where(pick, tab[1:2, :], 0.0), axis=1, keepdims=True)
            rows = dot(pick.astype(F32).astype(BF16), tokens[home], NN)
            d_parts.append((gate * rows).astype(BF16))
        d = jnp.concatenate(d_parts, axis=0)
        da = dot(d, wd[...], NT).astype(BF16).astype(F32)
        h1 = hgb[slot].astype(F32)
        h3 = hub[slot].astype(F32)
        g = jax.nn.sigmoid(h1)
        s = h1 * g
        act = (s * h3).astype(BF16)
        dh1 = (da * h3 * g * (1.0 + h1 * (1.0 - g))).astype(BF16)
        dh3 = (da * s).astype(BF16)
        dh = jnp.concatenate([dh1, dh3], axis=1)
        r = dot(dh, wgu[...], NT).astype(BF16)
        for cc in range(CORES):
            rbuf[q * CORES + cc] = r[cc * cap:(cc + 1) * cap]
        x = xb[slot]
        gwg_ref[...] += dot(x, dh1, TN)
        gwu_ref[...] += dot(x, dh3, TN)
        gwd_ref[...] += dot(act, d, TN)
        return carry

    lax.fori_loop(0, n_chip, chunk, 0)
    send_chunk(jnp.int32(n_chip - 1))

    n_run = crow // top_k
    n_step = tok_dev // n_run

    def y_load(m):
        return pltpu.make_async_copy(y_ref.at[pl.ds(pl.multiple_of(m * crow, crow), crow)], xb.at[m % 2], load_sem.at[0, m % 2])

    y_load(0).start()
    lane = lax.broadcasted_iota(jnp.int32, (crow, tok_dev), 1)
    token_of = lax.broadcasted_iota(jnp.int32, (crow, tok_dev), 0) // top_k
    gg_ref[...] = jnp.zeros_like(gg_ref)

    def gate_grad(m, carry):
        y_load(m).wait()

        @pl.when(m + 1 < n_step)
        def _():
            y_load(m + 1).start()

        gy = tokens[me, pl.ds(pl.multiple_of(m * n_run, n_run), n_run), :].astype(F32)
        gy = jnp.broadcast_to(gy[:, None, :], (n_run, top_k, model_dim)).reshape(crow, model_dim)
        col = jnp.sum(xb[m % 2].astype(F32) * gy, axis=1, keepdims=True)
        put = jnp.where(lane == token_of + m * n_run, col, 0.0)
        gg_ref[...] += jnp.sum(put.reshape(n_run, top_k, tok_dev), axis=0)
        return carry

    for k in TAIL_RELAY[0]:
        hand_on(k)
    lax.fori_loop(0, n_step, gate_grad, 0)
    for k in TAIL_RELAY[1]:
        hand_on(k)

    def add_rows(n, carry):
        j = lut(n, LINES)
        hb = wrap(my_b + j)

        @pl.when(j != 0)
        def _():
            landed(mids.at[hb], meta_sem.at[hb, 0])
            landed(mslots.at[hb], meta_sem.at[hb, 1])

        h_ids = mids[hb]
        h_slots = mslots[hb]
        picks = []
        for sa in range(side):
            for ce in range(CORES):
                slot = (hb * side + sa) * CORES + ce
                landed(ret.at[slot], ret_sem.at[slot])
                x = (1 - turn) * sa + turn * my_b
                y = (1 - turn) * my_b + turn * sa
                row = jnp.max(jnp.where(h_ids == (y * side + x) * CORES + ce, h_slots, -1), axis=0, keepdims=True)
                picks.append((row == slot_iota).astype(F32).astype(BF16))
        pick = jnp.concatenate(picks, axis=0)
        rows = ret[pl.ds(hb * side * CORES, side * CORES)].reshape(side * CORES * cap, model_dim)
        part[lut(n, [PART[v] for v in LINES])] = dot(pick, rows, TN)

        @pl.when(n == 1)
        def _():
            for c in hop_msgs():
                c.start()

        return carry

    def hop_msgs():
        return [
            remote(part.at[0, pl.ds(0, half)], hop_in.at[0], part_send.at[0], hop_sem.at[0], plane(0, 1)),
            remote(part.at[0, pl.ds(half, half)], hop_in.at[1], part_send.at[1], hop_sem.at[1], plane(0, -1)),
        ]

    def fin_msgs():
        return [
            remote(part.at[1 + n, pl.ds(h * half, half)], fin.at[n, pl.ds(h * half, half)], part_send.at[2 + 2 * n + h], fin_sem.at[n, h], plane(0, 1 - 2 * n))
            for n in range(2)
            for h in range(2)
        ]

    fins = fin_msgs()
    lax.fori_loop(0, len(LINES), add_rows, 0)
    fins[2].start()
    for what in sends:
        forward_msg(*what).wait_send()
    for what in pairs:
        pair_msg(*what).wait_send()
    fins[1].start()
    landed(hop_in.at[0], hop_sem.at[0])
    part[1, pl.ds(0, half)] += hop_in[0]
    landed(hop_in.at[1], hop_sem.at[1])
    part[2, pl.ds(half, half)] += hop_in[1]

    def tab_done(i, carry):
        tab_msg(i).wait_send()
        return carry

    lax.fori_loop(0, n_dev - 1, tab_done, 0)
    fins[0].start()
    fins[3].start()
    for c in meta_msgs() + hop_msgs():
        c.wait_send()

    def ret_done(k, carry):
        for cc in range(CORES):
            i, home, to, slot, hop, is_local = r_block(k, cc)

            @pl.when(jnp.logical_not(is_local))
            def _():
                remote(rbuf.at[home], ret.at[slot], ret_send.at[home], ret_sem.at[slot], to).wait_send()
        return carry

    lax.fori_loop(0, n_chip, ret_done, 0)
    for j in (0, 1, -1, 2):
        for way in range(2):
            relay_msg(j, way)[1].wait_send()
    for n, h in ((0, 1), (1, 0), (0, 0), (1, 1)):
        rows = pl.ds(h * half, half)
        landed(fin.at[n, rows], fin_sem.at[n, h])
        if (n, h) == (0, 0):
            gx_ref[rows] = (part[3, rows] + fin[0, rows] + fin[1, rows]).astype(gx_ref.dtype)
    rows = pl.ds(half, half)
    gx_ref[rows] = (part[3, rows] + fin[0, rows] + fin[1, rows]).astype(gx_ref.dtype)
    for c in fins:
        c.wait_send()


def write_out(*refs):
    n = len(refs) // 2
    sems = refs[-1]
    copies = [pltpu.make_async_copy(refs[i], refs[n + i], sems.at[i]) for i in range(n)]
    for c in copies:
        c.start()
    for c in copies:
        c.wait()


def solution(mesh):
    n_dev = mesh.shape["ep"]
    side = math.isqrt(n_dev // CORES)
    rows_spec = P(("dp", "ep"), None)
    cube_spec = P(("dp", "ep"), None, None)
    weight_spec = P("ep", None, None)

    def local_step(grad_y, gate_vals, topk_idx, slot_ids, pair_counts, y_routed, x_disp, h_gate, h_up, w_gate, w_up, w_down):
        assert w_gate.shape[0] == 1
        assert side * side * CORES == n_dev and len(ORDER) == side * side
        cap = x_disp.shape[1] // n_dev
        tok_dev, model_dim = grad_y.shape
        ffn = w_gate.shape[2]
        crow = CORES * cap
        n_chip = side * side
        top_k = topk_idx.shape[1]
        vmem = pl.BlockSpec(memory_space=pltpu.VMEM)
        anym = pl.BlockSpec(memory_space=pl.ANY)
        dma = pltpu.SemaphoreType.DMA
        results = pl.pallas_call(
            functools.partial(kernel, n_dev, side),
            out_shape=(
                pltpu.VMEM((tok_dev, model_dim), BF16),
                pltpu.VMEM((top_k, tok_dev), F32),
                pltpu.VMEM((model_dim, ffn), F32),
                pltpu.VMEM((model_dim, ffn), F32),
                pltpu.VMEM((ffn, model_dim), F32),
            ),
            in_specs=[anym] * 12,
            out_specs=(vmem,) * 5,
            scratch_shapes=[
                pltpu.VMEM((n_dev, tok_dev, model_dim), BF16),
                pltpu.VMEM((n_dev, 2, tok_dev), F32),
                pltpu.VMEM((n_dev, 2, tok_dev), F32),
                pltpu.VMEM((side, top_k, tok_dev), jnp.int32),
                pltpu.VMEM((side, top_k, tok_dev), jnp.int32),
                pltpu.VMEM((n_dev, cap, model_dim), BF16),
                pltpu.VMEM((n_dev, cap, model_dim), BF16),
                pltpu.VMEM((2 * side, cap, model_dim), BF16),
                pltpu.VMEM((4, tok_dev, model_dim), F32),
                pltpu.VMEM((2, tok_dev // 2, model_dim), F32),
                pltpu.VMEM((2, tok_dev, model_dim), F32),
                pltpu.VMEM((model_dim, 2 * ffn), BF16),
                pltpu.VMEM((ffn, model_dim), BF16),
                pltpu.VMEM((2, crow, model_dim), BF16),
                pltpu.VMEM((2, crow, ffn), BF16),
                pltpu.VMEM((2, crow, ffn), BF16),
                dma((n_dev, 2)),
                dma((n_dev,)),
                dma((side, 2)),
                dma((n_dev,)),
                dma((2 * side,)),
                dma((2,)),
                dma((2, 2)),
                dma((64,)),
                dma((n_chip,)),
                dma((n_dev,)),
                dma((3, 2)),
                dma((n_dev,)),
                dma((2 * side,)),
                dma((6,)),
                dma((3, 2)),
                dma((3,)),
                pltpu.SemaphoreType.REGULAR((side - 1,)),
                pltpu.VMEM((top_k, tok_dev), F32),
                pltpu.SMEM(pair_counts.shape, jnp.int32),
                dma((5,)),
            ],
            compiler_params=pltpu.CompilerParams(collective_id=0, has_side_effects=True, vmem_limit_bytes=58720256),
            name="moe_bwd",
        )(grad_y, topk_idx.T, slot_ids.T, gate_vals.T, pair_counts, y_routed.reshape(tok_dev * top_k, model_dim), x_disp[0], h_gate[0], h_up[0], w_gate[0], w_up[0], w_down[0])
        gx, gg, gwg, gwu, gwd = pl.pallas_call(
            write_out,
            out_shape=tuple(jax.ShapeDtypeStruct(r.shape, r.dtype) for r in results),
            in_specs=[anym] * len(results),
            out_specs=(anym,) * len(results),
            scratch_shapes=[dma((len(results),))],
            compiler_params=pltpu.CompilerParams(vmem_limit_bytes=1048576),
            name="write_out",
        )(*results)
        return gx, gg.T, gwg[None], gwu[None], gwd[None]

    return jax.shard_map(local_step, mesh=mesh, in_specs=(rows_spec, rows_spec, rows_spec, rows_spec, rows_spec, cube_spec, cube_spec, cube_spec, cube_spec, weight_spec, weight_spec, weight_spec), out_specs=(rows_spec, rows_spec, cube_spec, cube_spec, cube_spec), check_vma=False)
```

```python
import functools
import math

import jax
import jax.numpy as jnp
from jax import lax
from jax.experimental import pallas as pl
from jax.experimental.pallas import tpu as pltpu
from jax.sharding import PartitionSpec as P

MESH = pl.DeviceIdType.MESH
CORES = 2
BF16, F32 = jnp.bfloat16, jnp.float32

ORDER = ((-1, 0), (0, 1), (0, -1), (0, 0), (-1, 1), (1, 0), (1, -1), (1, 1), (0, 2), (-1, -1), (2, 0), (2, 1), (2, -1), (2, 2), (1, 2), (-1, 2))
EVENTS = {
    0: ((-1, 0), (0, -1), (1, 0), (0, 1)),
    2: ((2, 0), (-1, 1)),
    4: ((0, 2), (1, -1), (-1, -1)),
    5: ((1, 1),),
    6: ((2, -1),),
    9: ((2, 1),),
    10: ((1, 2),),
    12: ((2, 2), (-1, 2)),
}
FLIP = 1
RELAY = {14: (8, 10), 15: (11,)}
TAIL_RELAY = (13, 14), (15, 12)

LINES = (2, 0, -1, 1)
PART = {2: 0, 1: 1, -1: 2, 0: 3}

NN = (((1,), (0,)), ((), ()))
NT = (((1,), (1,)), ((), ()))
TN = (((0,), (0,)), ((), ()))


def dot(a, b, dims):
    return lax.dot_general(a, b, dims, preferred_element_type=F32)


def lut(k, vals):
    out = vals[0]
    for i, v in enumerate(vals):
        if i:
            out = jnp.where(k == i, v, out)
    return out


def kernel(n_dev, side, gy_ref, ids_ref, slots_ref, gates_ref, pc_ref, y_ref, x_ref, hg_ref, hu_ref, wg_ref, wu_ref, wd_ref,
           gx_ref, gg_ref, gwg_ref, gwu_ref, gwd_ref,
           tokens, stab, tabs, mids, mslots, rbuf, ret, relay, part, hop_in, fin, wgu, wd, xb, hgb, hub,
           tok_sem, tab_sem, meta_sem, ret_sem, relay_sem, hop_sem, fin_sem,
           ag_send, pair_send, tab_send, meta_send, ret_send, relay_send, part_send, load_sem, w_sem, round_sem, gates, counts, in_sem):
    me = lax.axis_index("ep")
    core = me % CORES
    mx = (me // CORES) % side
    my = me // (CORES * side)
    turn = 1 - core if FLIP else core
    my_a = (1 - turn) * mx + turn * my
    my_b = (1 - turn) * my + turn * mx
    tok_dev, model_dim = gy_ref.shape
    top_k = ids_ref.shape[0]
    ffn = wg_ref.shape[1]
    cap = rbuf.shape[1]
    half = tok_dev // 2
    n_chip = side * side
    crow = CORES * cap
    partner = me + 1 - 2 * core

    def wrap(v):
        return (v + 2 * side) % side

    def device(x, y, c):
        return (wrap(y) * side + wrap(x)) * CORES + c

    def plane(a, b):
        return device(mx + (1 - turn) * a + turn * b, my + turn * a + (1 - turn) * b, core)

    def remote(src, dst, send_sem, recv_sem, to):
        return pltpu.make_async_remote_copy(src_ref=src, dst_ref=dst, send_sem=send_sem, recv_sem=recv_sem, device_id={"ep": to}, device_id_type=MESH)

    def landed(ref, sem):
        pltpu.make_async_copy(ref, ref, sem).wait()

    peers = [partner] + [device(mx + dx, my + dy, c) for dx, dy in ((1, 0), (-1, 0), (0, 1), (0, -1)) for c in range(CORES)]

    def tell(sem):
        for to in peers:
            pl.semaphore_signal(sem, inc=1, device_id={"ep": to}, device_id_type=MESH)

    barrier = pltpu.get_barrier_semaphore()
    tell(barrier)

    own_copies = [
        pltpu.make_async_copy(gy_ref, tokens.at[me], in_sem.at[0]),
        pltpu.make_async_copy(ids_ref, mids.at[my_b], in_sem.at[1]),
        pltpu.make_async_copy(slots_ref, mslots.at[my_b], in_sem.at[2]),
        pltpu.make_async_copy(gates_ref, gates, in_sem.at[3]),
        pltpu.make_async_copy(pc_ref, counts, in_sem.at[4]),
    ]
    for c in own_copies:
        c.start()
    wcopies = [
        pltpu.make_async_copy(wd_ref, wd, w_sem.at[0]),
        pltpu.make_async_copy(wg_ref, wgu.at[:, pl.ds(0, ffn)], w_sem.at[1]),
        pltpu.make_async_copy(wu_ref, wgu.at[:, pl.ds(ffn, ffn)], w_sem.at[2]),
    ]
    for c in wcopies:
        c.start()

    def offset(k, axis):
        return lut(k, [o[axis] for o in ORDER])

    def chip_at(k):
        return wrap(my + offset(k, 1)) * side + wrap(mx + offset(k, 0))

    def loads(k):
        q = chip_at(k)
        slot = k % 2
        rows = pl.ds(pl.multiple_of(q * crow, crow), crow)
        return [
            pltpu.make_async_copy(x_ref.at[rows], xb.at[slot], load_sem.at[0, slot]),
            pltpu.make_async_copy(hg_ref.at[rows], hgb.at[slot], load_sem.at[1, slot]),
            pltpu.make_async_copy(hu_ref.at[rows], hub.at[slot], load_sem.at[2, slot]),
        ]

    pl.semaphore_wait(barrier, len(peers))
    own_copies[0].wait()

    sends, pairs = [], []

    def block(src, h):
        return tokens.at[src, pl.ds(h * half, half)]

    def forward_msg(n, i, j, h, a, b):
        src = plane(i, j)
        return remote(block(src, h), block(src, h), ag_send.at[n], tok_sem.at[src, h], plane(a, b))

    def forward(*what):
        what = (len(sends), *what)
        sends.append(what)
        forward_msg(*what).start()

    def pair_msg(n, i, j):
        src = plane(i, j)
        return remote(tokens.at[src], tokens.at[src], pair_send.at[n], tok_sem.at[src, 0], partner)

    def to_partner(i, j):
        what = (len(pairs), i, j)
        pairs.append(what)
        pair_msg(*what).start()

    def arrived(src, h):
        landed(block(src, h), tok_sem.at[src, h])

    to_partner(0, 0)

    def tab_msg(i):
        to = (me + 1 + i) % n_dev
        return remote(stab.at[to], tabs.at[me], tab_send.at[i], tab_sem.at[me], to)

    def tab_start(i, carry):
        tab_msg(i).start()
        return carry

    for n in range(2):
        for a, b, h in ((1, 0, n), (-1, 0, 1 - n), (0, 1, n), (0, -1, 1 - n)):
            forward(0, 0, h, a, b)

    tell(round_sem.at[0])
    for c in loads(0):
        c.start()

    for c in own_copies[1:]:
        c.wait()
    ids = mids[my_b]
    slots = mslots[my_b]

    def table(e, carry):
        hit = ids == e
        slot = jnp.max(jnp.where(hit, slots, -1), axis=0, keepdims=True)
        slot = jnp.where(slot < counts[0, e], slot, -1)
        gate = jnp.sum(jnp.where(hit, gates[...], 0.0), axis=0, keepdims=True)
        stab[e] = jnp.concatenate([slot.astype(F32), gate], axis=0)
        return carry

    lax.fori_loop(0, n_dev, table, 0)
    gwg_ref[...] = jnp.zeros_like(gwg_ref)
    gwu_ref[...] = jnp.zeros_like(gwu_ref)
    gwd_ref[...] = jnp.zeros_like(gwd_ref)

    for n in range(side - 1):
        if n:
            tell(round_sem.at[n])
        pl.semaphore_wait(round_sem.at[n], len(peers))
    lax.fori_loop(0, n_dev - 1, tab_start, 0)
    tab_copy = pltpu.make_async_copy(stab.at[me], tabs.at[me], tab_sem.at[me])
    tab_copy.start()
    def meta_msgs():
        out = []
        for n, j in enumerate((1, -1, 2)):
            out.append(remote(mids.at[my_b], mids.at[my_b], meta_send.at[n, 0], meta_sem.at[my_b, 0], plane(0, j)))
            out.append(remote(mslots.at[my_b], mslots.at[my_b], meta_send.at[n, 1], meta_sem.at[my_b, 1], plane(0, j)))
        return out

    for c in meta_msgs():
        c.start()

    def event(i, j):
        src = plane(i, j)
        first = 1 if (i == 1 and j == 0) or j == 1 else 0
        for n, h in enumerate((first, 1 - first)):
            arrived(src, h)
            if j == 0:
                if n == 0 and abs(i) == 1:
                    forward(i, j, h, -i, 0)
                forward(i, j, h, 0, 1)
                forward(i, j, h, 0, -1)
            elif n == 0 and abs(j) == 1:
                forward(i, j, h, 0, -j)
        to_partner(i, j)

    def r_block(k, cc):
        axis = 1 - cc if FLIP else cc
        i, j = offset(k, axis), offset(k, 1 - axis)
        a, b = (mx, my) if axis == 0 else (my, mx)
        hb = wrap(b + j)
        home = chip_at(k) * CORES + cc
        step = jnp.where(i == 2, 1 - 2 * core, i)
        to = device(mx + step, my, cc) if axis == 0 else device(mx, my + step, cc)
        slot = (hb * side + a) * CORES + core
        hop = hb * 2 + core
        is_local = jnp.logical_and(i == 0, core == cc)
        return i, home, to, slot, hop, is_local

    def send_chunk(k):
        for cc in range(CORES):
            i, home, to, slot, hop, is_local = r_block(k, cc)

            @pl.when(is_local)
            def _():
                pltpu.make_async_copy(rbuf.at[home], ret.at[slot], ret_sem.at[slot]).start()

            @pl.when(i == 2)
            def _():
                remote(rbuf.at[home], relay.at[hop], ret_send.at[home], relay_sem.at[hop], to).start()

            @pl.when(jnp.logical_and(i != 2, jnp.logical_not(is_local)))
            def _():
                remote(rbuf.at[home], ret.at[slot], ret_send.at[home], ret_sem.at[slot], to).start()

    def relay_msg(j, way):
        hb = wrap(my_b + j)
        slot = (hb * side + wrap(my_a - 1 + 2 * way)) * CORES + way
        hop = hb * 2 + way
        return hop, remote(relay.at[hop], ret.at[slot], relay_send.at[hop], ret_sem.at[slot], plane(1 - 2 * way, 0))

    def hand_on(k):
        dx, dy = ORDER[k]
        i = jnp.where(turn == 0, dx, dy)
        j = jnp.where(turn == 0, dy, dx)

        @pl.when(i == 2)
        def _():
            for way in range(2):
                hop, msg = relay_msg(j, way)
                landed(relay.at[hop], relay_sem.at[hop])
                msg.start()

    slot_iota = lax.broadcasted_iota(jnp.int32, (cap, tok_dev), 0)
    slot_iota_f = slot_iota.astype(F32)
    for c in wcopies:
        c.wait()

    def chunk(k, carry):
        @pl.when(k > 0)
        def _():
            send_chunk(k - 1)

        for at, evs in EVENTS.items():
            @pl.when(k == at)
            def _(evs=evs):
                for i, j in evs:
                    event(i, j)

        for at, steps in RELAY.items():
            @pl.when(k == at)
            def _(steps=steps):
                for n in steps:
                    hand_on(n)

        slot = k % 2
        for c in loads(k):
            c.wait()

        @pl.when(k + 1 < n_chip)
        def _():
            for c in loads(k + 1):
                c.start()

        q = chip_at(k)
        landed(tokens.at[q * CORES + 1 - core], tok_sem.at[q * CORES + 1 - core, 0])

        d_parts = []
        for cc in range(CORES):
            home = q * CORES + cc
            landed(tabs.at[home], tab_sem.at[home])
            tab = tabs[home]
            pick = tab[0:1, :] == slot_iota_f
            gate = jnp.sum(jnp.where(pick, tab[1:2, :], 0.0), axis=1, keepdims=True)
            rows = dot(pick.astype(F32).astype(BF16), tokens[home], NN)
            d_parts.append((gate * rows).astype(BF16))
        d = jnp.concatenate(d_parts, axis=0)
        da = dot(d, wd[...], NT).astype(BF16).astype(F32)
        h1 = hgb[slot].astype(F32)
        h3 = hub[slot].astype(F32)
        g = jax.nn.sigmoid(h1)
        s = h1 * g
        act = (s * h3).astype(BF16)
        dh1 = (da * h3 * g * (1.0 + h1 * (1.0 - g))).astype(BF16)
        dh3 = (da * s).astype(BF16)
        dh = jnp.concatenate([dh1, dh3], axis=1)
        r = dot(dh, wgu[...], NT).astype(BF16)
        for cc in range(CORES):
            rbuf[q * CORES + cc] = r[cc * cap:(cc + 1) * cap]
        x = xb[slot]
        gwg_ref[...] += dot(x, dh1, TN)
        gwu_ref[...] += dot(x, dh3, TN)
        gwd_ref[...] += dot(act, d, TN)
        return carry

    lax.fori_loop(0, n_chip, chunk, 0)
    send_chunk(jnp.int32(n_chip - 1))

    n_run = crow // top_k
    n_step = tok_dev // n_run

    def y_load(m):
        return pltpu.make_async_copy(y_ref.at[pl.ds(pl.multiple_of(m * crow, crow), crow)], xb.at[m % 2], load_sem.at[0, m % 2])

    y_load(0).start()
    lane = lax.broadcasted_iota(jnp.int32, (crow, tok_dev), 1)
    token_of = lax.broadcasted_iota(jnp.int32, (crow, tok_dev), 0) // top_k
    gg_ref[...] = jnp.zeros_like(gg_ref)

    def gate_grad(m, carry):
        y_load(m).wait()

        @pl.when(m + 1 < n_step)
        def _():
            y_load(m + 1).start()

        gy = tokens[me, pl.ds(pl.multiple_of(m * n_run, n_run), n_run), :].astype(F32)
        gy = jnp.broadcast_to(gy[:, None, :], (n_run, top_k, model_dim)).reshape(crow, model_dim)
        col = jnp.sum(xb[m % 2].astype(F32) * gy, axis=1, keepdims=True)
        put = jnp.where(lane == token_of + m * n_run, col, 0.0)
        gg_ref[...] += jnp.sum(put.reshape(n_run, top_k, tok_dev), axis=0)
        return carry

    for k in TAIL_RELAY[0]:
        hand_on(k)
    lax.fori_loop(0, n_step, gate_grad, 0)
    for k in TAIL_RELAY[1]:
        hand_on(k)

    def add_rows(n, carry):
        j = lut(n, LINES)
        hb = wrap(my_b + j)

        @pl.when(j != 0)
        def _():
            landed(mids.at[hb], meta_sem.at[hb, 0])
            landed(mslots.at[hb], meta_sem.at[hb, 1])

        h_ids = mids[hb]
        h_slots = mslots[hb]
        picks = []
        for sa in range(side):
            for ce in range(CORES):
                slot = (hb * side + sa) * CORES + ce
                landed(ret.at[slot], ret_sem.at[slot])
                x = (1 - turn) * sa + turn * my_b
                y = (1 - turn) * my_b + turn * sa
                row = jnp.max(jnp.where(h_ids == (y * side + x) * CORES + ce, h_slots, -1), axis=0, keepdims=True)
                picks.append((row == slot_iota).astype(F32).astype(BF16))
        pick = jnp.concatenate(picks, axis=0)
        rows = ret[pl.ds(hb * side * CORES, side * CORES)].reshape(side * CORES * cap, model_dim)
        part[lut(n, [PART[v] for v in LINES])] = dot(pick, rows, TN)

        @pl.when(n == 1)
        def _():
            for c in hop_msgs():
                c.start()

        return carry

    def hop_msgs():
        return [
            remote(part.at[0, pl.ds(0, half)], hop_in.at[0], part_send.at[0], hop_sem.at[0], plane(0, 1)),
            remote(part.at[0, pl.ds(half, half)], hop_in.at[1], part_send.at[1], hop_sem.at[1], plane(0, -1)),
        ]

    def fin_msgs():
        return [
            remote(part.at[1 + n, pl.ds(h * half, half)], fin.at[n, pl.ds(h * half, half)], part_send.at[2 + 2 * n + h], fin_sem.at[n, h], plane(0, 1 - 2 * n))
            for n in range(2)
            for h in range(2)
        ]

    fins = fin_msgs()
    lax.fori_loop(0, len(LINES), add_rows, 0)
    fins[2].start()
    for what in sends:
        forward_msg(*what).wait_send()
    for what in pairs:
        pair_msg(*what).wait_send()
    fins[1].start()
    landed(hop_in.at[0], hop_sem.at[0])
    part[1, pl.ds(0, half)] += hop_in[0]
    landed(hop_in.at[1], hop_sem.at[1])
    part[2, pl.ds(half, half)] += hop_in[1]

    def tab_done(i, carry):
        tab_msg(i).wait_send()
        return carry

    lax.fori_loop(0, n_dev - 1, tab_done, 0)
    fins[0].start()
    fins[3].start()
    for c in meta_msgs() + hop_msgs():
        c.wait_send()

    def ret_done(k, carry):
        for cc in range(CORES):
            i, home, to, slot, hop, is_local = r_block(k, cc)

            @pl.when(jnp.logical_not(is_local))
            def _():
                remote(rbuf.at[home], ret.at[slot], ret_send.at[home], ret_sem.at[slot], to).wait_send()
        return carry

    lax.fori_loop(0, n_chip, ret_done, 0)
    for j in (0, 1, -1, 2):
        for way in range(2):
            relay_msg(j, way)[1].wait_send()
    for n, h in ((0, 1), (1, 0), (0, 0), (1, 1)):
        rows = pl.ds(h * half, half)
        landed(fin.at[n, rows], fin_sem.at[n, h])
        if (n, h) == (0, 0):
            gx_ref[rows] = (part[3, rows] + fin[0, rows] + fin[1, rows]).astype(gx_ref.dtype)
    rows = pl.ds(half, half)
    gx_ref[rows] = (part[3, rows] + fin[0, rows] + fin[1, rows]).astype(gx_ref.dtype)
    for c in fins:
        c.wait_send()


def write_out(*refs):
    n = len(refs) // 2
    sems = refs[-1]
    copies = [pltpu.make_async_copy(refs[i], refs[n + i], sems.at[i]) for i in range(n)]
    for c in copies:
        c.start()
    for c in copies:
        c.wait()


def solution(mesh):
    n_dev = mesh.shape["ep"]
    side = math.isqrt(n_dev // CORES)
    rows_spec = P(("dp", "ep"), None)
    cube_spec = P(("dp", "ep"), None, None)
    weight_spec = P("ep", None, None)

    def local_step(grad_y, gate_vals, topk_idx, slot_ids, pair_counts, y_routed, x_disp, h_gate, h_up, w_gate, w_up, w_down):
        assert w_gate.shape[0] == 1
        assert side * side * CORES == n_dev and len(ORDER) == side * side
        cap = x_disp.shape[1] // n_dev
        tok_dev, model_dim = grad_y.shape
        ffn = w_gate.shape[2]
        crow = CORES * cap
        n_chip = side * side
        top_k = topk_idx.shape[1]
        vmem = pl.BlockSpec(memory_space=pltpu.VMEM)
        anym = pl.BlockSpec(memory_space=pl.ANY)
        dma = pltpu.SemaphoreType.DMA
        results = pl.pallas_call(
            functools.partial(kernel, n_dev, side),
            out_shape=(
                pltpu.VMEM((tok_dev, model_dim), BF16),
                pltpu.VMEM((top_k, tok_dev), F32),
                pltpu.VMEM((model_dim, ffn), F32),
                pltpu.VMEM((model_dim, ffn), F32),
                pltpu.VMEM((ffn, model_dim), F32),
            ),
            in_specs=[anym] * 12,
            out_specs=(vmem,) * 5,
            scratch_shapes=[
                pltpu.VMEM((n_dev, tok_dev, model_dim), BF16),
                pltpu.VMEM((n_dev, 2, tok_dev), F32),
                pltpu.VMEM((n_dev, 2, tok_dev), F32),
                pltpu.VMEM((side, top_k, tok_dev), jnp.int32),
                pltpu.VMEM((side, top_k, tok_dev), jnp.int32),
                pltpu.VMEM((n_dev, cap, model_dim), BF16),
                pltpu.VMEM((n_dev, cap, model_dim), BF16),
                pltpu.VMEM((2 * side, cap, model_dim), BF16),
                pltpu.VMEM((4, tok_dev, model_dim), F32),
                pltpu.VMEM((2, tok_dev // 2, model_dim), F32),
                pltpu.VMEM((2, tok_dev, model_dim), F32),
                pltpu.VMEM((model_dim, 2 * ffn), BF16),
                pltpu.VMEM((ffn, model_dim), BF16),
                pltpu.VMEM((2, crow, model_dim), BF16),
                pltpu.VMEM((2, crow, ffn), BF16),
                pltpu.VMEM((2, crow, ffn), BF16),
                dma((n_dev, 2)),
                dma((n_dev,)),
                dma((side, 2)),
                dma((n_dev,)),
                dma((2 * side,)),
                dma((2,)),
                dma((2, 2)),
                dma((64,)),
                dma((n_chip,)),
                dma((n_dev,)),
                dma((3, 2)),
                dma((n_dev,)),
                dma((2 * side,)),
                dma((6,)),
                dma((3, 2)),
                dma((3,)),
                pltpu.SemaphoreType.REGULAR((side - 1,)),
                pltpu.VMEM((top_k, tok_dev), F32),
                pltpu.SMEM(pair_counts.shape, jnp.int32),
                dma((5,)),
            ],
            compiler_params=pltpu.CompilerParams(collective_id=0, has_side_effects=True, vmem_limit_bytes=58720256),
            name="moe_bwd",
        )(grad_y, topk_idx.T, slot_ids.T, gate_vals.T, pair_counts, y_routed.reshape(tok_dev * top_k, model_dim), x_disp[0], h_gate[0], h_up[0], w_gate[0], w_up[0], w_down[0])
        gx, gg, gwg, gwu, gwd = pl.pallas_call(
            write_out,
            out_shape=tuple(jax.ShapeDtypeStruct(r.shape, r.dtype) for r in results),
            in_specs=[anym] * len(results),
            out_specs=(anym,) * len(results),
            scratch_shapes=[dma((len(results),))],
            compiler_params=pltpu.CompilerParams(vmem_limit_bytes=1048576),
            name="write_out",
        )(*results)
        return gx, gg.T, gwg[None], gwu[None], gwd[None]

    return jax.shard_map(local_step, mesh=mesh, in_specs=(rows_spec, rows_spec, rows_spec, rows_spec, rows_spec, cube_spec, cube_spec, cube_spec, cube_spec, weight_spec, weight_spec, weight_spec), out_specs=(rows_spec, rows_spec, cube_spec, cube_spec, cube_spec), check_vma=False)
```

```python
import functools
import math

import jax
import jax.numpy as jnp
from jax import lax
from jax.experimental import pallas as pl
from jax.experimental.pallas import tpu as pltpu
from jax.sharding import PartitionSpec as P

MESH = pl.DeviceIdType.MESH
CORES = 2
BF16, F32 = jnp.bfloat16, jnp.float32

ORDER = ((-1, 0), (0, 1), (0, -1), (0, 0), (-1, 1), (1, 0), (1, -1), (1, 1), (0, 2), (-1, -1), (2, 0), (2, 1), (2, -1), (2, 2), (1, 2), (-1, 2))
EVENTS = {
    0: ((-1, 0), (0, -1), (1, 0), (0, 1)),
    2: ((2, 0), (-1, 1)),
    4: ((0, 2), (1, -1), (-1, -1)),
    5: ((1, 1),),
    6: ((2, -1),),
    9: ((2, 1),),
    10: ((1, 2),),
    12: ((2, 2), (-1, 2)),
}
FLIP = 1
RELAY = {}
TAIL_RELAY = (11, 13, 10, 8, 14), (15, 12)

LINES = (2, 0, -1, 1)
PART = {2: 0, 1: 1, -1: 2, 0: 3}

NN = (((1,), (0,)), ((), ()))
NT = (((1,), (1,)), ((), ()))
TN = (((0,), (0,)), ((), ()))


def dot(a, b, dims):
    return lax.dot_general(a, b, dims, preferred_element_type=F32)


def lut(k, vals):
    out = vals[0]
    for i, v in enumerate(vals):
        if i:
            out = jnp.where(k == i, v, out)
    return out


def kernel(n_dev, side, gy_ref, ids_ref, slots_ref, gates_ref, pc_ref, y_ref, x_ref, hg_ref, hu_ref, wg_ref, wu_ref, wd_ref,
           gx_ref, gg_ref, gwg_ref, gwu_ref, gwd_ref,
           tokens, stab, tabs, mids, mslots, rbuf, ret, relay, part, hop_in, fin, wgu, wd, xb, hgb, hub,
           tok_sem, tab_sem, meta_sem, ret_sem, relay_sem, hop_sem, fin_sem,
           ag_send, pair_send, tab_send, meta_send, ret_send, relay_send, part_send, load_sem, w_sem, round_sem, gates, counts, in_sem):
    me = lax.axis_index("ep")
    core = me % CORES
    mx = (me // CORES) % side
    my = me // (CORES * side)
    turn = 1 - core if FLIP else core
    my_a = (1 - turn) * mx + turn * my
    my_b = (1 - turn) * my + turn * mx
    tok_dev, model_dim = gy_ref.shape
    top_k = ids_ref.shape[0]
    ffn = wg_ref.shape[1]
    cap = rbuf.shape[1]
    half = tok_dev // 2
    n_chip = side * side
    crow = CORES * cap
    partner = me + 1 - 2 * core

    def wrap(v):
        return (v + 2 * side) % side

    def device(x, y, c):
        return (wrap(y) * side + wrap(x)) * CORES + c

    def plane(a, b):
        return device(mx + (1 - turn) * a + turn * b, my + turn * a + (1 - turn) * b, core)

    def remote(src, dst, send_sem, recv_sem, to):
        return pltpu.make_async_remote_copy(src_ref=src, dst_ref=dst, send_sem=send_sem, recv_sem=recv_sem, device_id={"ep": to}, device_id_type=MESH)

    def landed(ref, sem):
        pltpu.make_async_copy(ref, ref, sem).wait()

    peers = [partner] + [device(mx + dx, my + dy, c) for dx, dy in ((1, 0), (-1, 0), (0, 1), (0, -1)) for c in range(CORES)]

    def tell(sem):
        for to in peers:
            pl.semaphore_signal(sem, inc=1, device_id={"ep": to}, device_id_type=MESH)

    barrier = pltpu.get_barrier_semaphore()
    tell(barrier)

    own_copies = [
        pltpu.make_async_copy(gy_ref, tokens.at[me], in_sem.at[0]),
        pltpu.make_async_copy(ids_ref, mids.at[my_b], in_sem.at[1]),
        pltpu.make_async_copy(slots_ref, mslots.at[my_b], in_sem.at[2]),
        pltpu.make_async_copy(gates_ref, gates, in_sem.at[3]),
        pltpu.make_async_copy(pc_ref, counts, in_sem.at[4]),
    ]
    for c in own_copies:
        c.start()
    wcopies = [
        pltpu.make_async_copy(wd_ref, wd, w_sem.at[0]),
        pltpu.make_async_copy(wg_ref, wgu.at[:, pl.ds(0, ffn)], w_sem.at[1]),
        pltpu.make_async_copy(wu_ref, wgu.at[:, pl.ds(ffn, ffn)], w_sem.at[2]),
    ]
    for c in wcopies:
        c.start()

    def offset(k, axis):
        return lut(k, [o[axis] for o in ORDER])

    def chip_at(k):
        return wrap(my + offset(k, 1)) * side + wrap(mx + offset(k, 0))

    def loads(k):
        q = chip_at(k)
        slot = k % 2
        rows = pl.ds(pl.multiple_of(q * crow, crow), crow)
        return [
            pltpu.make_async_copy(x_ref.at[rows], xb.at[slot], load_sem.at[0, slot]),
            pltpu.make_async_copy(hg_ref.at[rows], hgb.at[slot], load_sem.at[1, slot]),
            pltpu.make_async_copy(hu_ref.at[rows], hub.at[slot], load_sem.at[2, slot]),
        ]

    pl.semaphore_wait(barrier, len(peers))
    own_copies[0].wait()

    sends, pairs = [], []

    def block(src, h):
        return tokens.at[src, pl.ds(h * half, half)]

    def forward_msg(n, i, j, h, a, b):
        src = plane(i, j)
        return remote(block(src, h), block(src, h), ag_send.at[n], tok_sem.at[src, h], plane(a, b))

    def forward(*what):
        what = (len(sends), *what)
        sends.append(what)
        forward_msg(*what).start()

    def pair_msg(n, i, j):
        src = plane(i, j)
        return remote(tokens.at[src], tokens.at[src], pair_send.at[n], tok_sem.at[src, 0], partner)

    def to_partner(i, j):
        what = (len(pairs), i, j)
        pairs.append(what)
        pair_msg(*what).start()

    def arrived(src, h):
        landed(block(src, h), tok_sem.at[src, h])

    to_partner(0, 0)

    def tab_msg(i):
        to = (me + 1 + i) % n_dev
        return remote(stab.at[to], tabs.at[me], tab_send.at[i], tab_sem.at[me], to)

    def tab_start(i, carry):
        tab_msg(i).start()
        return carry

    for n in range(2):
        for a, b, h in ((1, 0, n), (-1, 0, 1 - n), (0, 1, n), (0, -1, 1 - n)):
            forward(0, 0, h, a, b)

    tell(round_sem.at[0])
    for c in loads(0):
        c.start()

    for c in own_copies[1:]:
        c.wait()
    ids = mids[my_b]
    slots = mslots[my_b]

    def table(e, carry):
        hit = ids == e
        slot = jnp.max(jnp.where(hit, slots, -1), axis=0, keepdims=True)
        slot = jnp.where(slot < counts[0, e], slot, -1)
        gate = jnp.sum(jnp.where(hit, gates[...], 0.0), axis=0, keepdims=True)
        stab[e] = jnp.concatenate([slot.astype(F32), gate], axis=0)
        return carry

    lax.fori_loop(0, n_dev, table, 0)
    gwg_ref[...] = jnp.zeros_like(gwg_ref)
    gwu_ref[...] = jnp.zeros_like(gwu_ref)
    gwd_ref[...] = jnp.zeros_like(gwd_ref)

    for n in range(side - 1):
        if n:
            tell(round_sem.at[n])
        pl.semaphore_wait(round_sem.at[n], len(peers))
    lax.fori_loop(0, n_dev - 1, tab_start, 0)
    tab_copy = pltpu.make_async_copy(stab.at[me], tabs.at[me], tab_sem.at[me])
    tab_copy.start()
    def meta_msgs():
        out = []
        for n, j in enumerate((1, -1, 2)):
            out.append(remote(mids.at[my_b], mids.at[my_b], meta_send.at[n, 0], meta_sem.at[my_b, 0], plane(0, j)))
            out.append(remote(mslots.at[my_b], mslots.at[my_b], meta_send.at[n, 1], meta_sem.at[my_b, 1], plane(0, j)))
        return out

    for c in meta_msgs():
        c.start()

    def event(i, j):
        src = plane(i, j)
        first = 1 if (i == 1 and j == 0) or j == 1 else 0
        for n, h in enumerate((first, 1 - first)):
            arrived(src, h)
            if j == 0:
                if n == 0 and abs(i) == 1:
                    forward(i, j, h, -i, 0)
                forward(i, j, h, 0, 1)
                forward(i, j, h, 0, -1)
            elif n == 0 and abs(j) == 1:
                forward(i, j, h, 0, -j)
        to_partner(i, j)

    def r_block(k, cc):
        axis = 1 - cc if FLIP else cc
        i, j = offset(k, axis), offset(k, 1 - axis)
        a, b = (mx, my) if axis == 0 else (my, mx)
        hb = wrap(b + j)
        home = chip_at(k) * CORES + cc
        step = jnp.where(i == 2, 1 - 2 * core, i)
        to = device(mx + step, my, cc) if axis == 0 else device(mx, my + step, cc)
        slot = (hb * side + a) * CORES + core
        hop = hb * 2 + core
        is_local = jnp.logical_and(i == 0, core == cc)
        return i, home, to, slot, hop, is_local

    def send_chunk(k):
        for cc in range(CORES):
            i, home, to, slot, hop, is_local = r_block(k, cc)

            @pl.when(is_local)
            def _():
                pltpu.make_async_copy(rbuf.at[home], ret.at[slot], ret_sem.at[slot]).start()

            @pl.when(i == 2)
            def _():
                remote(rbuf.at[home], relay.at[hop], ret_send.at[home], relay_sem.at[hop], to).start()

            @pl.when(jnp.logical_and(i != 2, jnp.logical_not(is_local)))
            def _():
                remote(rbuf.at[home], ret.at[slot], ret_send.at[home], ret_sem.at[slot], to).start()

    def relay_msg(j, way):
        hb = wrap(my_b + j)
        slot = (hb * side + wrap(my_a - 1 + 2 * way)) * CORES + way
        hop = hb * 2 + way
        return hop, remote(relay.at[hop], ret.at[slot], relay_send.at[hop], ret_sem.at[slot], plane(1 - 2 * way, 0))

    def hand_on(k):
        dx, dy = ORDER[k]
        i = jnp.where(turn == 0, dx, dy)
        j = jnp.where(turn == 0, dy, dx)

        @pl.when(i == 2)
        def _():
            for way in range(2):
                hop, msg = relay_msg(j, way)
                landed(relay.at[hop], relay_sem.at[hop])
                msg.start()

    slot_iota = lax.broadcasted_iota(jnp.int32, (cap, tok_dev), 0)
    slot_iota_f = slot_iota.astype(F32)
    for c in wcopies:
        c.wait()

    def chunk(k, carry):
        @pl.when(k > 0)
        def _():
            send_chunk(k - 1)

        for at, evs in EVENTS.items():
            @pl.when(k == at)
            def _(evs=evs):
                for i, j in evs:
                    event(i, j)

        for at, steps in RELAY.items():
            @pl.when(k == at)
            def _(steps=steps):
                for n in steps:
                    hand_on(n)

        slot = k % 2
        for c in loads(k):
            c.wait()

        @pl.when(k + 1 < n_chip)
        def _():
            for c in loads(k + 1):
                c.start()

        q = chip_at(k)
        landed(tokens.at[q * CORES + 1 - core], tok_sem.at[q * CORES + 1 - core, 0])

        d_parts = []
        for cc in range(CORES):
            home = q * CORES + cc
            landed(tabs.at[home], tab_sem.at[home])
            tab = tabs[home]
            pick = tab[0:1, :] == slot_iota_f
            gate = jnp.sum(jnp.where(pick, tab[1:2, :], 0.0), axis=1, keepdims=True)
            rows = dot(pick.astype(F32).astype(BF16), tokens[home], NN)
            d_parts.append((gate * rows).astype(BF16))
        d = jnp.concatenate(d_parts, axis=0)
        da = dot(d, wd[...], NT).astype(BF16).astype(F32)
        h1 = hgb[slot].astype(F32)
        h3 = hub[slot].astype(F32)
        g = jax.nn.sigmoid(h1)
        s = h1 * g
        act = (s * h3).astype(BF16)
        dh1 = (da * h3 * g * (1.0 + h1 * (1.0 - g))).astype(BF16)
        dh3 = (da * s).astype(BF16)
        dh = jnp.concatenate([dh1, dh3], axis=1)
        r = dot(dh, wgu[...], NT).astype(BF16)
        for cc in range(CORES):
            rbuf[q * CORES + cc] = r[cc * cap:(cc + 1) * cap]
        x = xb[slot]
        gwg_ref[...] += dot(x, dh1, TN)
        gwu_ref[...] += dot(x, dh3, TN)
        gwd_ref[...] += dot(act, d, TN)
        return carry

    lax.fori_loop(0, n_chip, chunk, 0)
    send_chunk(jnp.int32(n_chip - 1))

    n_run = crow // top_k
    n_step = tok_dev // n_run

    def y_load(m):
        return pltpu.make_async_copy(y_ref.at[pl.ds(pl.multiple_of(m * crow, crow), crow)], xb.at[m % 2], load_sem.at[0, m % 2])

    y_load(0).start()
    lane = lax.broadcasted_iota(jnp.int32, (crow, tok_dev), 1)
    token_of = lax.broadcasted_iota(jnp.int32, (crow, tok_dev), 0) // top_k
    gg_ref[...] = jnp.zeros_like(gg_ref)

    def gate_grad(m, carry):
        y_load(m).wait()

        @pl.when(m + 1 < n_step)
        def _():
            y_load(m + 1).start()

        gy = tokens[me, pl.ds(pl.multiple_of(m * n_run, n_run), n_run), :].astype(F32)
        gy = jnp.broadcast_to(gy[:, None, :], (n_run, top_k, model_dim)).reshape(crow, model_dim)
        col = jnp.sum(xb[m % 2].astype(F32) * gy, axis=1, keepdims=True)
        put = jnp.where(lane == token_of + m * n_run, col, 0.0)
        gg_ref[...] += jnp.sum(put.reshape(n_run, top_k, tok_dev), axis=0)
        return carry

    for k in TAIL_RELAY[0]:
        hand_on(k)
    lax.fori_loop(0, n_step, gate_grad, 0)
    for k in TAIL_RELAY[1]:
        hand_on(k)

    def add_rows(n, carry):
        j = lut(n, LINES)
        hb = wrap(my_b + j)

        @pl.when(j != 0)
        def _():
            landed(mids.at[hb], meta_sem.at[hb, 0])
            landed(mslots.at[hb], meta_sem.at[hb, 1])

        h_ids = mids[hb]
        h_slots = mslots[hb]
        picks = []
        for sa in range(side):
            for ce in range(CORES):
                slot = (hb * side + sa) * CORES + ce
                landed(ret.at[slot], ret_sem.at[slot])
                x = (1 - turn) * sa + turn * my_b
                y = (1 - turn) * my_b + turn * sa
                row = jnp.max(jnp.where(h_ids == (y * side + x) * CORES + ce, h_slots, -1), axis=0, keepdims=True)
                picks.append((row == slot_iota).astype(F32).astype(BF16))
        pick = jnp.concatenate(picks, axis=0)
        rows = ret[pl.ds(hb * side * CORES, side * CORES)].reshape(side * CORES * cap, model_dim)
        part[lut(n, [PART[v] for v in LINES])] = dot(pick, rows, TN)

        @pl.when(n == 1)
        def _():
            for c in hop_msgs():
                c.start()

        return carry

    def hop_msgs():
        return [
            remote(part.at[0, pl.ds(0, half)], hop_in.at[0], part_send.at[0], hop_sem.at[0], plane(0, 1)),
            remote(part.at[0, pl.ds(half, half)], hop_in.at[1], part_send.at[1], hop_sem.at[1], plane(0, -1)),
        ]

    def fin_msgs():
        return [
            remote(part.at[1 + n, pl.ds(h * half, half)], fin.at[n, pl.ds(h * half, half)], part_send.at[2 + 2 * n + h], fin_sem.at[n, h], plane(0, 1 - 2 * n))
            for n in range(2)
            for h in range(2)
        ]

    fins = fin_msgs()
    lax.fori_loop(0, len(LINES), add_rows, 0)
    fins[2].start()
    for what in sends:
        forward_msg(*what).wait_send()
    for what in pairs:
        pair_msg(*what).wait_send()
    fins[1].start()
    landed(hop_in.at[0], hop_sem.at[0])
    part[1, pl.ds(0, half)] += hop_in[0]
    landed(hop_in.at[1], hop_sem.at[1])
    part[2, pl.ds(half, half)] += hop_in[1]

    def tab_done(i, carry):
        tab_msg(i).wait_send()
        return carry

    lax.fori_loop(0, n_dev - 1, tab_done, 0)
    fins[0].start()
    fins[3].start()
    for c in meta_msgs() + hop_msgs():
        c.wait_send()

    def ret_done(k, carry):
        for cc in range(CORES):
            i, home, to, slot, hop, is_local = r_block(k, cc)

            @pl.when(jnp.logical_not(is_local))
            def _():
                remote(rbuf.at[home], ret.at[slot], ret_send.at[home], ret_sem.at[slot], to).wait_send()
        return carry

    lax.fori_loop(0, n_chip, ret_done, 0)
    for j in (0, 1, -1, 2):
        for way in range(2):
            relay_msg(j, way)[1].wait_send()
    for n, h in ((0, 1), (1, 0), (0, 0), (1, 1)):
        rows = pl.ds(h * half, half)
        landed(fin.at[n, rows], fin_sem.at[n, h])
        if (n, h) == (0, 0):
            gx_ref[rows] = (part[3, rows] + fin[0, rows] + fin[1, rows]).astype(gx_ref.dtype)
    rows = pl.ds(half, half)
    gx_ref[rows] = (part[3, rows] + fin[0, rows] + fin[1, rows]).astype(gx_ref.dtype)
    for c in fins:
        c.wait_send()


def write_out(*refs):
    n = len(refs) // 2
    sems = refs[-1]
    copies = [pltpu.make_async_copy(refs[i], refs[n + i], sems.at[i]) for i in range(n)]
    for c in copies:
        c.start()
    for c in copies:
        c.wait()


def solution(mesh):
    n_dev = mesh.shape["ep"]
    side = math.isqrt(n_dev // CORES)
    rows_spec = P(("dp", "ep"), None)
    cube_spec = P(("dp", "ep"), None, None)
    weight_spec = P("ep", None, None)

    def local_step(grad_y, gate_vals, topk_idx, slot_ids, pair_counts, y_routed, x_disp, h_gate, h_up, w_gate, w_up, w_down):
        assert w_gate.shape[0] == 1
        assert side * side * CORES == n_dev and len(ORDER) == side * side
        cap = x_disp.shape[1] // n_dev
        tok_dev, model_dim = grad_y.shape
        ffn = w_gate.shape[2]
        crow = CORES * cap
        n_chip = side * side
        top_k = topk_idx.shape[1]
        vmem = pl.BlockSpec(memory_space=pltpu.VMEM)
        anym = pl.BlockSpec(memory_space=pl.ANY)
        dma = pltpu.SemaphoreType.DMA
        results = pl.pallas_call(
            functools.partial(kernel, n_dev, side),
            out_shape=(
                pltpu.VMEM((tok_dev, model_dim), BF16),
                pltpu.VMEM((top_k, tok_dev), F32),
                pltpu.VMEM((model_dim, ffn), F32),
                pltpu.VMEM((model_dim, ffn), F32),
                pltpu.VMEM((ffn, model_dim), F32),
            ),
            in_specs=[anym] * 12,
            out_specs=(vmem,) * 5,
            scratch_shapes=[
                pltpu.VMEM((n_dev, tok_dev, model_dim), BF16),
                pltpu.VMEM((n_dev, 2, tok_dev), F32),
                pltpu.VMEM((n_dev, 2, tok_dev), F32),
                pltpu.VMEM((side, top_k, tok_dev), jnp.int32),
                pltpu.VMEM((side, top_k, tok_dev), jnp.int32),
                pltpu.VMEM((n_dev, cap, model_dim), BF16),
                pltpu.VMEM((n_dev, cap, model_dim), BF16),
                pltpu.VMEM((2 * side, cap, model_dim), BF16),
                pltpu.VMEM((4, tok_dev, model_dim), F32),
                pltpu.VMEM((2, tok_dev // 2, model_dim), F32),
                pltpu.VMEM((2, tok_dev, model_dim), F32),
                pltpu.VMEM((model_dim, 2 * ffn), BF16),
                pltpu.VMEM((ffn, model_dim), BF16),
                pltpu.VMEM((2, crow, model_dim), BF16),
                pltpu.VMEM((2, crow, ffn), BF16),
                pltpu.VMEM((2, crow, ffn), BF16),
                dma((n_dev, 2)),
                dma((n_dev,)),
                dma((side, 2)),
                dma((n_dev,)),
                dma((2 * side,)),
                dma((2,)),
                dma((2, 2)),
                dma((64,)),
                dma((n_chip,)),
                dma((n_dev,)),
                dma((3, 2)),
                dma((n_dev,)),
                dma((2 * side,)),
                dma((6,)),
                dma((3, 2)),
                dma((3,)),
                pltpu.SemaphoreType.REGULAR((side - 1,)),
                pltpu.VMEM((top_k, tok_dev), F32),
                pltpu.SMEM(pair_counts.shape, jnp.int32),
                dma((5,)),
            ],
            compiler_params=pltpu.CompilerParams(collective_id=0, has_side_effects=True, vmem_limit_bytes=58720256),
            name="moe_bwd",
        )(grad_y, topk_idx.T, slot_ids.T, gate_vals.T, pair_counts, y_routed.reshape(tok_dev * top_k, model_dim), x_disp[0], h_gate[0], h_up[0], w_gate[0], w_up[0], w_down[0])
        gx, gg, gwg, gwu, gwd = pl.pallas_call(
            write_out,
            out_shape=tuple(jax.ShapeDtypeStruct(r.shape, r.dtype) for r in results),
            in_specs=[anym] * len(results),
            out_specs=(anym,) * len(results),
            scratch_shapes=[dma((len(results),))],
            compiler_params=pltpu.CompilerParams(vmem_limit_bytes=1048576),
            name="write_out",
        )(*results)
        return gx, gg.T, gwg[None], gwu[None], gwd[None]

    return jax.shard_map(local_step, mesh=mesh, in_specs=(rows_spec, rows_spec, rows_spec, rows_spec, rows_spec, cube_spec, cube_spec, cube_spec, cube_spec, weight_spec, weight_spec, weight_spec), out_specs=(rows_spec, rows_spec, cube_spec, cube_spec, cube_spec), check_vma=False)
```
